512 devices in a mesh: lat: 16 (over y, z_lo), lon: 32 (over x, z_hi, core).
Axes of the slice: x: 4, y: 4, z: 16 (z_hi: 4, z_lo: 4; z = z_hi * 4 + z_lo), core: 2. Of those that a mesh axis runs over, the one named last changes fastest.
Arguments:
- atmos_patch_tokens: bfloat16 [256, 768, 512], P('lat', 'lon'), may hold values from -6 to 6
- atmos_norm_gain: float32 [512], replicated, may hold values from 0.5 to 1.5
- query_key_value_weight: bfloat16 [512, 1536], replicated, may hold values from -0.25 to 0.25
- query_key_value_bias: float32 [1536], replicated, may hold values from -3 to 3
- relative_bias_grid: float32 [16, 225], replicated, may hold values from -260 to 260
- attention_output_weight: bfloat16 [512, 512], replicated, may hold values from -0.25 to 0.25
- flux_projector: bfloat16 [512, 16], replicated, may hold values from -0.25 to 0.25
- surface_encoder: float32 [4, 512], replicated, may hold values from -1.5 to 1.5
- ocean_cell_state: bfloat16 [256, 1024, 256], P('lat', 'lon'), may hold values from -6 to 6
- land_sea_mask: int32 [256, 1024], P('lat', 'lon'), may hold values 0 or 1
- depthwise_conv_kernel: float32 [7, 7, 256], replicated, may hold values from -0.875 to 0.875
- depthwise_conv_bias: float32 [256], replicated, may hold values from -3 to 3
- ocean_norm_gain: float32 [256], replicated, may hold values from 0.5 to 1.5
- pointwise_expand: bfloat16 [256, 1024], replicated, may hold values from -0.375 to 0.375
- pointwise_contract: bfloat16 [1024, 256], replicated, may hold values from -0.1875 to 0.1875
- layer_update_scale: float32 [256], replicated, may hold values from 0.3 to 1.5
- forcing_encoder: float32 [16, 256], replicated, may hold values from -1.5 to 1.5
- surface_projector: float32 [256, 4], replicated, may hold values from -0.375 to 0.375
- overlay_area_weight: bfloat16 [16, 32, 3, 64, 512], P('lat', 'lon'), may hold values from 0 to 1, as said below
- owners: int32 [16, 32, 3], P('lat', 'lon'), may hold values from 0 to 31, as said below
- owner_tile_blocks: int32 [16, 32, 3], P('lat', 'lon'), may hold values from 0 to 5
- counts: int32 [16, 32], P('lat', 'lon'), may hold values from 1 to 3
Outputs:
- atm_out: bfloat16 [256, 768, 512], P('lat', 'lon')
- ocean_out: bfloat16 [256, 1024, 256], P('lat', 'lon')
The draws below stay inside these ranges and needn't reach their ends.
Inputs may be any that keep to these rules, and one draw needn't show every extreme that they name: `overlay_area_weight`: nonnegative. `owners`: each slot's owner is the ocean tile's own longitude strip or one of the two beside it, cyclically. `owner_tile_blocks`: values of unused slots are arbitrary within the range.
All inputs are finite; a program needn't handle non-finite values. No bound on the sum of `land_sea_mask` on one device may be relied on, other than what follows from the above.
Results may differ from the reference program's by a relative error of at most 0.008.
Values may be sent and summed in bfloat16 or wider, within the bound.
A program may use at most 64 MiB of HBM per device.

```python
import math
import jax
import jax.numpy as jnp
from jax import lax

ATMOS_WIDTH = 512
HEADS = 16
WIN = 8
SHIFT = 4
ATMOS_PATCH_ROWS = 16
ATMOS_PATCH_COLS = 24
BLK = 64
OCEAN_WIDTH = 256
HID = 1024
KER = 7
OH = 16
OW = 32
FLUX = 16
SURFACE_FIELDS = 4
SLOTS = 3
NLAT_P = 256
NLON_P = 768
NOLAT = 256
NOLON = 1024
N_LAT = 16
N_LON = 32


def draw_relative_bias_grid(key, part):
    entries = (2 * WIN - 1) ** 2
    lookup = jnp.clip(jax.random.normal(key, (HEADS, entries), jnp.float32), -4.0, 4.0)
    return lookup


def draw_overlay_area_weight(key, part):
    cells = OH * OW
    shape = (N_LAT, N_LON, SLOTS, BLK, cells)
    links = (jax.random.randint(jax.random.fold_in(key, 21), shape, 0, cells) < 6).astype(jnp.float32)
    values = jax.random.uniform(jax.random.fold_in(key, 22), shape, jnp.float32, 0.25, 0.75)
    return (links * values).astype(jnp.bfloat16)


def draw_owners(key, part):
    offsets = jax.random.randint(jax.random.fold_in(key, 31), (N_LAT, N_LON, SLOTS), -1, 2)
    strips = jnp.arange(N_LON, dtype=jnp.int32)[None, :, None]
    return ((strips + offsets + N_LON) % N_LON).astype(jnp.int32)


def set_ends(result, stream_key, low, high):
    dims = result.shape
    index_at = [jax.random.randint(jax.random.fold_in(stream_key, axis), (), 0, dims[axis]) for axis in range(len(dims))]
    result = result.at[tuple(index_at)].set(low)
    longest = dims.index(max(dims))
    index_at[longest] = (index_at[longest] + 1) % dims[longest]
    return result.at[tuple(index_at)].set(high)


def shard_levels(own_key, extent, split, low, high):
    level = 1.0
    for axis_at, parts in split:
        heights = jax.random.uniform(jax.random.fold_in(jax.random.fold_in(own_key, 6), axis_at), (parts,), jnp.float32, low / len(split), high / len(split))
        level = level * jnp.repeat(jnp.exp(heights), extent[axis_at] // parts).reshape((-1,) + (1,) * (len(extent) - 1 - axis_at))
    return level


def scatter_about(key, shape, scale, limit, cuts=(), kind=jnp.bfloat16):
    gain = shard_levels(key, shape, cuts, -0.22, 0.18) if cuts else 1.0
    values = jax.random.normal(key, shape, jnp.float32) * scale * gain
    return jnp.minimum(jnp.maximum(values, -limit), limit).astype(kind)


def setup_inputs(seed: int = 0) -> dict:
    keys = jax.random.split(jax.random.key(seed), 23)
    return {
        "atmos_patch_tokens": scatter_about(keys[0], (NLAT_P, NLON_P, ATMOS_WIDTH), 1.0, 6.0, ((0, 16), (1, 32))),
        "atmos_norm_gain": jnp.clip(1.0 + 0.1 * jax.random.normal(keys[1], (ATMOS_WIDTH,), jnp.float32), 0.5, 1.5),
        "query_key_value_weight": scatter_about(keys[2], (ATMOS_WIDTH, 3 * ATMOS_WIDTH), ATMOS_WIDTH ** -0.5, 0.25),
        "query_key_value_bias": scatter_about(keys[3], (3 * ATMOS_WIDTH,), 0.5, 3.0, (), jnp.float32),
        "relative_bias_grid": draw_relative_bias_grid(jax.random.fold_in(keys[22], 71), 0),
        "attention_output_weight": scatter_about(keys[5], (ATMOS_WIDTH, ATMOS_WIDTH), ATMOS_WIDTH ** -0.5, 0.25),
        "flux_projector": scatter_about(keys[6], (ATMOS_WIDTH, FLUX), ATMOS_WIDTH ** -0.5, 0.25),
        "surface_encoder": scatter_about(keys[7], (SURFACE_FIELDS, ATMOS_WIDTH), (4 * SURFACE_FIELDS) ** -0.5, 1.5, (), jnp.float32),
        "ocean_cell_state": scatter_about(keys[8], (NOLAT, NOLON, OCEAN_WIDTH), 1.0, 6.0, ((0, 16), (1, 32))),
        "land_sea_mask": set_ends((jax.random.randint(keys[9], (NOLAT, NOLON), 0, 4) < 3).astype(jnp.int32), jax.random.fold_in(keys[9], 1), 0, 1),
        "depthwise_conv_kernel": scatter_about(keys[10], (KER, KER, OCEAN_WIDTH), (KER * KER) ** -0.5, 0.875, (), jnp.float32),
        "depthwise_conv_bias": scatter_about(keys[11], (OCEAN_WIDTH,), 0.5, 3.0, (), jnp.float32),
        "ocean_norm_gain": jnp.clip(1.0 + 0.1 * jax.random.normal(keys[12], (OCEAN_WIDTH,), jnp.float32), 0.5, 1.5),
        "pointwise_expand": scatter_about(keys[13], (OCEAN_WIDTH, HID), OCEAN_WIDTH ** -0.5, 0.375),
        "pointwise_contract": scatter_about(keys[14], (HID, OCEAN_WIDTH), HID ** -0.5, 0.1875),
        "layer_update_scale": jnp.clip(jnp.exp(jax.random.uniform(keys[15], (OCEAN_WIDTH,), jnp.float32, math.log(0.3), math.log(1.5))), 0.3, 1.5),
        "forcing_encoder": scatter_about(keys[16], (FLUX, OCEAN_WIDTH), FLUX ** -0.5, 1.5, (), jnp.float32),
        "surface_projector": scatter_about(keys[17], (OCEAN_WIDTH, SURFACE_FIELDS), OCEAN_WIDTH ** -0.5, 0.375, (), jnp.float32),
        "overlay_area_weight": draw_overlay_area_weight(jax.random.fold_in(keys[22], 71), 0),
        "owners": draw_owners(jax.random.fold_in(keys[22], 71), 0),
        "owner_tile_blocks": set_ends(jax.random.randint(keys[20], (N_LAT, N_LON, SLOTS), 0, ATMOS_PATCH_ROWS * ATMOS_PATCH_COLS // BLK), jax.random.fold_in(keys[20], 1), 0, (ATMOS_PATCH_ROWS * ATMOS_PATCH_COLS // BLK) - 1).astype(jnp.int32),
        "counts": set_ends(jax.random.randint(keys[21], (N_LAT, N_LON), 1, SLOTS + 1), jax.random.fold_in(keys[21], 1), 1, SLOTS).astype(jnp.int32),
    }


FULL_PRECISION = lax.Precision.HIGHEST

def layer_norm(values, gain_vector, epsilon):
    average = lax.optimization_barrier(jnp.mean(values, axis=-1, keepdims=True))
    centred = values - average
    spread = lax.optimization_barrier(jnp.mean(centred * centred, axis=-1, keepdims=True))
    return centred * lax.rsqrt(spread + epsilon) * gain_vector

def to_windows(values, window):
    row_count, col_count, channel_total = values.shape
    pieces = values.reshape(row_count // window, window, col_count // window, window, channel_total).transpose(0, 2, 1, 3, 4)
    return pieces.reshape(-1, window * window, channel_total)

def from_windows(values, row_count, col_count, window):
    channel_total = values.shape[-1]
    pieces = values.reshape(row_count // window, col_count // window, window, window, channel_total).transpose(0, 2, 1, 3, 4)
    return pieces.reshape(row_count, col_count, channel_total)

def position_bias(lookup, window):
    places = jnp.arange(window * window, dtype=jnp.int32)
    row_place = places // window
    col_place = places % window
    offsets = (row_place[:, None] - row_place[None, :] + window - 1) * (2 * window - 1) + (col_place[:, None] - col_place[None, :] + window - 1)
    onehot = (offsets[:, :, None] == jnp.arange((2 * window - 1) ** 2, dtype=jnp.int32)[None, None, :]).astype(jnp.float32)
    return jnp.einsum('hp,abp->hab', lookup, onehot, precision=FULL_PRECISION)

def window_attention(normed, region, query_key_value_weight, query_key_value_bias, pos_bias, attention_output_weight, head_count, window):
    row_count, col_count, feature_width = normed.shape
    head_size = feature_width // head_count
    qkv = jnp.dot(normed.reshape(row_count * col_count, feature_width), query_key_value_weight, preferred_element_type=jnp.float32) + query_key_value_bias
    queries = (qkv[:, :feature_width] * head_size ** (-0.5)).astype(jnp.bfloat16)
    key_rows = qkv[:, feature_width:2 * feature_width].astype(jnp.bfloat16)
    value_rows = qkv[:, 2 * feature_width:].astype(jnp.bfloat16)

    def split_heads(matrix):
        return to_windows(matrix.reshape(row_count, col_count, feature_width), window).reshape(-1, window * window, head_count, head_size)
    queries = split_heads(queries)
    key_rows = split_heads(key_rows)
    value_rows = split_heads(value_rows)
    labels = to_windows(region.reshape(row_count, col_count, 1), window)[:, :, 0]
    scores = jnp.einsum('wahd,wbhd->whab', queries.astype(jnp.float32), key_rows.astype(jnp.float32)) + pos_bias[None]
    same_region = labels[:, None, :, None] == labels[:, None, None, :]
    scores = jnp.where(same_region, scores, -1000000000.0)
    largest = lax.optimization_barrier(jnp.max(scores, axis=-1, keepdims=True))
    expo = jnp.exp(scores - largest)
    weights = (expo / lax.optimization_barrier(jnp.sum(expo, axis=-1, keepdims=True))).astype(jnp.bfloat16)
    attended = jnp.einsum('whab,wbhd->wahd', weights.astype(jnp.float32), value_rows.astype(jnp.float32)).astype(jnp.bfloat16)
    attended = from_windows(attended.reshape(-1, window * window, feature_width), row_count, col_count, window)
    attended = attended.reshape(row_count * col_count, feature_width)
    projected = jnp.dot(attended, attention_output_weight, preferred_element_type=jnp.float32).astype(jnp.bfloat16)
    return projected.reshape(row_count, col_count, feature_width)

def reference(atmos_patch_tokens, atmos_norm_gain, query_key_value_weight, query_key_value_bias, relative_bias_grid, attention_output_weight, flux_projector, surface_encoder, ocean_cell_state, land_sea_mask, depthwise_conv_kernel, depthwise_conv_bias, ocean_norm_gain, pointwise_expand, pointwise_contract, layer_update_scale, forcing_encoder, surface_projector, overlay_area_weight, owners, owner_tile_blocks, counts):
    latitude_count = N_LAT
    longitude_count = N_LON
    ocean_cell_grid = OH * OW
    block_count = ATMOS_PATCH_ROWS * ATMOS_PATCH_COLS // BLK
    latitude_rows = ATMOS_PATCH_ROWS * latitude_count
    longitude_columns = ATMOS_PATCH_COLS * longitude_count
    ocean_rows = OH * latitude_count
    ocean_cols = OW * longitude_count
    wet_cell_mask = land_sea_mask.astype(jnp.float32)
    in_use = (jnp.arange(SLOTS, dtype=jnp.int32)[None, None, :] < counts[:, :, None]).astype(jnp.float32)
    owner_hot = (owners[..., None] == jnp.arange(longitude_count, dtype=jnp.int32)).astype(jnp.float32) * in_use[..., None]
    block_hot = (owner_tile_blocks[..., None] == jnp.arange(block_count, dtype=jnp.int32)).astype(jnp.float32)
    ocean_mask_float = ocean_cell_state.astype(jnp.float32)
    surface_values = jnp.einsum('jev,vh->jeh', ocean_mask_float, surface_projector, precision=FULL_PRECISION) * wet_cell_mask[:, :, None]
    surface_values = surface_values.astype(jnp.bfloat16)
    surface_tiles = surface_values.reshape(latitude_count, OH, longitude_count, OW, SURFACE_FIELDS).transpose(0, 2, 1, 3, 4).reshape(latitude_count, longitude_count, ocean_cell_grid, SURFACE_FIELDS)
    regrid_float = overlay_area_weight.astype(jnp.float32)
    contrib = jnp.einsum('ijktc,ijcs->ijkts', regrid_float, surface_tiles.astype(jnp.float32), precision=FULL_PRECISION)
    toward_atmosphere = jnp.einsum('ijkm,ijkb,ijkts->imbts', owner_hot, block_hot, contrib, precision=FULL_PRECISION)
    sea_surface_atmos = toward_atmosphere.reshape(latitude_count, longitude_count, ATMOS_PATCH_ROWS, ATMOS_PATCH_COLS, SURFACE_FIELDS).transpose(0, 2, 1, 3, 4).reshape(latitude_rows, longitude_columns, SURFACE_FIELDS)
    spatial_mixed = (atmos_patch_tokens.astype(jnp.float32) + jnp.einsum('fnw,wl->fnl', sea_surface_atmos, surface_encoder, precision=FULL_PRECISION)).astype(jnp.bfloat16)
    normed = layer_norm(spatial_mixed.astype(jnp.float32), atmos_norm_gain, 1e-05).astype(jnp.bfloat16)
    rolled = jnp.roll(normed, (-SHIFT, -SHIFT), (0, 1))
    region = (jnp.arange(latitude_rows, dtype=jnp.int32) >= latitude_rows - SHIFT).astype(jnp.int32)
    region = jnp.broadcast_to(region[:, None], (latitude_rows, longitude_columns))
    pos_bias = position_bias(relative_bias_grid, WIN)
    band_count = latitude_rows // WIN

    def one_band(pieces):
        return window_attention(pieces[0], pieces[1], query_key_value_weight, query_key_value_bias, pos_bias, attention_output_weight, HEADS, WIN)
    projected = lax.map(one_band, (rolled.reshape(band_count, WIN, longitude_columns, ATMOS_WIDTH), region.reshape(band_count, WIN, longitude_columns)))
    projected = projected.reshape(latitude_rows, longitude_columns, ATMOS_WIDTH)
    back = jnp.roll(projected, (SHIFT, SHIFT), (0, 1))
    atm_out = (spatial_mixed.astype(jnp.float32) + back.astype(jnp.float32)).astype(jnp.bfloat16)
    flux = jnp.dot(atm_out.reshape(latitude_rows * longitude_columns, ATMOS_WIDTH), flux_projector, preferred_element_type=jnp.float32).astype(jnp.bfloat16)
    flux_tiles = flux.reshape(latitude_count, ATMOS_PATCH_ROWS, longitude_count, ATMOS_PATCH_COLS, FLUX).transpose(0, 2, 1, 3, 4).reshape(latitude_count, longitude_count, block_count, BLK, FLUX)
    picked = jnp.einsum('ijkm,ijkb,imbtf->ijktf', owner_hot, block_hot, flux_tiles.astype(jnp.float32), precision=FULL_PRECISION)
    forcing = jnp.einsum('ijktc,ijktf->ijcf', regrid_float, picked, precision=FULL_PRECISION)
    forcing = forcing.reshape(latitude_count, longitude_count, OH, OW, FLUX).transpose(0, 2, 1, 3, 4).reshape(ocean_rows, ocean_cols, FLUX)
    half = KER // 2
    padded = jnp.pad(ocean_mask_float, ((half, half), (0, 0), (0, 0)))
    padded = jnp.concatenate([padded[:, ocean_cols - half:], padded, padded[:, :half]], axis=1)
    conv = jnp.zeros_like(ocean_mask_float) + depthwise_conv_bias
    for row_off in range(KER):
        for col_off in range(KER):
            conv = conv + depthwise_conv_kernel[row_off, col_off] * padded[row_off:row_off + ocean_rows, col_off:col_off + ocean_cols]
    pre = conv + jnp.einsum('rcf,fx->rcx', forcing, forcing_encoder, precision=FULL_PRECISION)

    def pointwise(pieces):
        pre_band, state_band, mask_band = pieces
        ocean_normed = layer_norm(pre_band, ocean_norm_gain, 1e-06).astype(jnp.bfloat16)
        hidden = jax.nn.gelu(jnp.dot(ocean_normed, pointwise_expand, preferred_element_type=jnp.float32), approximate=False).astype(jnp.bfloat16)
        update = jnp.dot(hidden, pointwise_contract, preferred_element_type=jnp.float32)
        return (state_band + mask_band[:, None] * layer_update_scale * update).astype(jnp.bfloat16)
    band_cells = OH * ocean_cols
    ocean_out = lax.map(pointwise, (pre.reshape(latitude_count, band_cells, OCEAN_WIDTH), ocean_mask_float.reshape(latitude_count, band_cells, OCEAN_WIDTH), wet_cell_mask.reshape(latitude_count, band_cells)))
    ocean_out = ocean_out.reshape(ocean_rows, ocean_cols, OCEAN_WIDTH)
    return (atm_out, ocean_out)
```

```python
import functools

import jax
import jax.numpy as jnp
from jax import lax
from jax.experimental import pallas as pl
from jax.experimental.pallas import tpu as pltpu
from jax.sharding import PartitionSpec as P

F32 = jnp.float32
BF16 = jnp.bfloat16
MESH = pl.DeviceIdType.MESH
HEADS = 16
HALF = 8
WIN = 8
NT = (((1,), (1,)), ((), ()))
TN = (((0,), (0,)), ((), ()))
NN = (((1,), (0,)), ((), ()))


def dot(a, b, dims):
    return lax.dot_general(a, b, dims, preferred_element_type=F32)


def iota(shape, dim):
    return lax.broadcasted_iota(jnp.int32, shape, dim)


def low_half(shape):
    return iota(shape, len(shape) - 2) % 8 < 4


def turn(x):
    return pltpu.roll(x, 4, x.ndim - 2)


def pack(x, high):
    n, _, lanes = x.shape
    x = x.reshape(n // 2, 2, 8, lanes)
    even, odd = x[:, 0], x[:, 1]
    if high:
        even = turn(even)
    else:
        odd = turn(odd)
    return jnp.where(low_half(even.shape), even, odd)


def unpack(x, high):
    n, _, lanes = x.shape
    other = turn(x)
    pair = (other, x) if high else (x, other)
    return jnp.stack(pair, axis=1).reshape(2 * n, 8, lanes)


def split2(x):
    top = x.astype(BF16).astype(F32)
    return top, x - top


def split3(x):
    top, rest = split2(x)
    middle, last = split2(rest)
    return top, middle, last


def greet(partners):
    barrier = pltpu.get_barrier_semaphore()
    for device in partners:
        pl.semaphore_signal(barrier, inc=1, device_id=device, device_id_type=MESH)
    return lambda: pl.semaphore_wait(barrier, len(partners))


def place():
    la, lo = lax.axis_index("lat"), lax.axis_index("lon")
    nla, nlo = lax.axis_size("lat"), lax.axis_size("lon")
    return lambda di, dj: (lax.rem(la + di + nla, nla), lax.rem(lo + dj + nlo, nlo))


SURFACE_PARTNERS = [
    (di, dj) for di in (-1, 0, 1) for dj in (-2, -1, 0, 1, 2)
    if (di, dj) not in ((0, 0), (-1, 2), (1, -2))
]
AROUND = [(di, dj) for di in (-1, 0, 1) for dj in (-1, 0, 1) if (di, dj) != (0, 0)]


def first_kernel(
    owner_ref, block_ref, count_ref, tok_ref, ocean_ref, mask_ref, overlay_ref, proj_ref, grid_ref,
    msgs_ref, east_ref, south_ref, corner_ref, above_ref, below_ref, left_ref, right_ref, oc_ref, bias_ref,
    msg_s, east_s, corner_s, left_s, right_s, oc_s, table_s, send_sem, recv_sem,
):
    at = place()
    lo = lax.axis_index("lon")
    nlo = lax.axis_size("lon")
    wait_barrier = greet([at(*o) for o in SURFACE_PARTNERS])

    top, middle, last = split3(proj_ref[...])
    parts = jnp.concatenate([top, middle, last], axis=0).astype(BF16)
    state = ocean_ref[...].reshape(512, 256)
    surf = dot(parts, state, NT)
    surf = ((surf[0:8] + surf[8:16] + surf[16:24]) * mask_ref[...]).astype(BF16)
    row = iota((8, 128), 0)
    twice = []
    codes = jnp.full((8, 128), -1.0, F32)
    for k in range(3):
        block = overlay_ref[k]
        twice.append(dot(surf, jnp.concatenate([block, block], axis=0), NT))
        side = lax.rem(owner_ref[0, k] - lo + 1 + nlo, nlo)
        code = jnp.where(k < count_ref[0, 0], side * 8 + block_ref[0, k], -1).astype(F32)
        codes = jnp.where(row == 4 + k, code, codes)
    msg_s[0:8] = jnp.where(row < 4, twice[0], twice[1])
    msg_s[8:16] = jnp.where(row < 4, twice[2], codes)

    side = pack(tok_ref[4:16, 0:8, :].astype(F32), False)
    east_s[...] = side.reshape(48, 512).astype(BF16)
    side = pack(tok_ref[0:4, 0:8, :].astype(F32), False)
    corner_s[...] = side.reshape(16, 512).astype(BF16)
    west_cols = pack(ocean_ref[:, 0:8, :].astype(F32), False)
    east_cols = pack(ocean_ref[:, 24:32, :].astype(F32), True)
    left_s[...] = east_cols.reshape(64, 256).astype(BF16)
    right_s[...] = west_cols.reshape(64, 256).astype(BF16)
    oc_s[0] = west_cols[0:2].reshape(16, 256).astype(BF16)
    oc_s[1] = east_cols[0:2].reshape(16, 256).astype(BF16)
    oc_s[2] = west_cols[6:8].reshape(16, 256).astype(BF16)
    oc_s[3] = east_cols[6:8].reshape(16, 256).astype(BF16)

    copies = []

    def send(src, dst, offset):
        n = len(copies)
        copy = pltpu.make_async_remote_copy(
            src_ref=src, dst_ref=dst, send_sem=send_sem.at[n], recv_sem=recv_sem.at[n],
            device_id=at(*offset), device_id_type=MESH,
        )
        copies.append(copy)
        copy.start()

    wait_barrier()
    for below in range(2):
        for dj in (1, 2, -1, 0):
            if (below, dj) != (0, 0):
                send(msg_s, msgs_ref.at[below * 4 + dj + 1], (-below, -dj))
    send(east_s, east_ref, (0, -1))
    send(tok_ref.at[pl.ds(0, 4)], south_ref, (-1, 0))
    send(corner_s, corner_ref, (-1, -1))
    send(ocean_ref.at[pl.ds(0, 4)], below_ref, (-1, 0))
    send(ocean_ref.at[pl.ds(12, 4)], above_ref, (1, 0))
    send(left_s, left_ref, (0, 1))
    send(right_s, right_ref, (0, -1))
    send(oc_s.at[0], oc_ref.at[0], (-1, -1))
    send(oc_s.at[1], oc_ref.at[1], (-1, 1))
    send(oc_s.at[2], oc_ref.at[2], (1, -1))
    send(oc_s.at[3], oc_ref.at[3], (1, 1))
    msgs_ref[1] = msg_s[...]

    grid = jnp.concatenate([grid_ref[...], jnp.zeros((16, 31), F32)], axis=1)
    for ra in range(8):
        rolled = grid if ra == 0 else pltpu.roll(grid, 256 - 15 * ra, 1)
        table_s[:, ra, :] = rolled[:, 0:128]
    parts = [x.astype(BF16) for x in split3(table_s[...].reshape(128, 128))]
    entry = iota((128, 64), 0)
    lane = iota((128, 64), 1)
    for ca in range(8):
        chosen = (entry == (7 - lane // 8) * 15 + ca - lane % 8 + 7).astype(BF16)
        found = (dot(parts[0], chosen, NN) + dot(parts[1], chosen, NN)) + dot(parts[2], chosen, NN)
        bias_ref[:, ca, :] = found

    for copy in copies:
        copy.wait()


def vmem(n):
    return [pl.BlockSpec(memory_space=pltpu.VMEM)] * n


def smem(n):
    return [pl.BlockSpec(memory_space=pltpu.SMEM)] * n


def first(owners, blocks, counts, tok, ocean, mask_row, overlay, proj8, grid):
    shapes = [
        ((8, 16, 128), F32), ((48, 512), BF16), ((4, 24, 512), BF16), ((16, 512), BF16),
        ((4, 32, 256), BF16), ((4, 32, 256), BF16), ((64, 256), BF16), ((64, 256), BF16),
        ((4, 16, 256), BF16), ((128, 8, 64), F32),
    ]
    return pl.pallas_call(
        first_kernel,
        out_shape=[jax.ShapeDtypeStruct(*s) for s in shapes],
        in_specs=smem(3) + vmem(6),
        out_specs=vmem(len(shapes)),
        scratch_shapes=[
            pltpu.VMEM((16, 128), F32), pltpu.VMEM((48, 512), BF16), pltpu.VMEM((16, 512), BF16),
            pltpu.VMEM((64, 256), BF16), pltpu.VMEM((64, 256), BF16), pltpu.VMEM((4, 16, 256), BF16),
            pltpu.VMEM((16, 8, 128), F32),
            pltpu.SemaphoreType.DMA((18,)), pltpu.SemaphoreType.DMA((18,)),
        ],
        compiler_params=pltpu.CompilerParams(collective_id=0, has_side_effects=True),
        name="first",
    )(owners, blocks, counts, tok, ocean, mask_row, overlay, proj8, grid)


def layer_norm(x, gain, epsilon):
    average = jnp.mean(x, axis=-1, keepdims=True)
    centred = x - average
    spread = jnp.mean(centred * centred, axis=-1, keepdims=True)
    return centred * lax.rsqrt(spread + epsilon) * gain


def gather_surface(msgs_ref):
    row = iota((8, 128), 0)
    upper = row < 4
    right = iota((8, 128), 1) >= 64
    tiles = {}
    for below in range(2):
        for tile in range(2):
            sums = [jnp.zeros((8, 128), F32)] * 3
            for side in range(3):
                dj = tile - side + 1
                a = msgs_ref[below * 4 + dj + 1, 0:8, :]
                b = msgs_ref[below * 4 + dj + 1, 8:16, :]
                code_a = jnp.where(upper, b[4:5], b[5:6])
                code_b = jnp.where(upper, b[6:7], -1.0)
                for j in range(3):
                    target = jnp.where(right, side * 8.0 + 2 * j + 1, side * 8.0 + 2 * j)
                    sums[j] += jnp.where(code_a == target, a, 0.0) + jnp.where(code_b == target, b, 0.0)
            tiles[below, tile] = sums
    out = []
    for j in range(3):
        patch = iota((8, 128), 1) + 128 * j
        east = column_of(patch) < 4
        south = patch < 96
        here = jnp.where(east, tiles[0, 1][j], tiles[0, 0][j])
        under = jnp.where(east, tiles[1, 1][j], tiles[1, 0][j])
        out.append(jnp.where(south, under, here))
    return jnp.concatenate(out, axis=1)


def column_of(patch):
    p = patch.astype(F32)
    return p - 24.0 * jnp.floor((p + 0.5) * (1.0 / 24.0))


def atmosphere_kernel(
    tok_ref, east_ref, south_ref, corner_ref, msgs_ref, enc_ref, gain_ref, wqkv_ref, bqkv_ref, bias_ref, wo_ref, fp_ref,
    cyc_ref, flux_ref, pe_ref, pc_ref,
    mixed_s, norm_s, q_s, k_s, v_s, att_s, last_s,
):
    sst = gather_surface(msgs_ref)
    s_hi, s_lo = split2(sst)
    e_hi, e_lo = split2(enc_ref[...])
    left = jnp.concatenate([s_hi, s_lo, s_hi], axis=0).astype(BF16)
    right = jnp.concatenate([e_hi, e_hi, e_lo], axis=0).astype(BF16)
    mixed_s[...] = dot(left, right, TN).reshape(16, 24, 512)
    gain = gain_ref[...].reshape(1, 1, 512)
    for g in range(4):
        rows = slice(4 * g, 4 * g + 4)
        if g == 0:
            tokens = south_ref[...].astype(F32)
            side = unpack(corner_ref[...].astype(F32).reshape(2, 8, 512), False)
        else:
            tokens = tok_ref[rows].astype(F32)
            side = unpack(east_ref[16 * (g - 1) : 16 * g].astype(F32).reshape(2, 8, 512), False)
        head = jnp.where(low_half((4, 8, 512)), side, tokens[:, 0:8])
        tokens = jnp.concatenate([head, tokens[:, 8:24]], axis=1)
        mixed = (tokens + mixed_s[rows]).astype(BF16).astype(F32)
        mixed_s[rows] = mixed
        normed = layer_norm(mixed, gain, 1e-05)
        turned = [turn(normed[:, 8 * b : 8 * b + 8]) for b in range(3)]
        low = low_half((4, 8, 512))
        w_row, w_start = ((1, 4), (0, 0), (0, 4), (1, 0))[g]
        for b in range(3):
            norm_s[w_row * 3 + b, w_start : w_start + 4] = jnp.where(low, turned[b], turned[(b + 1) % 3])

    rows = norm_s[...].reshape(384, 512).astype(BF16)
    bq = bqkv_ref[...]
    q_s[...] = ((dot(rows, wqkv_ref[:, 0:512], NN) + bq[:, 0:512]) * 32 ** (-0.5)).astype(BF16)
    k_s[...] = (dot(rows, wqkv_ref[:, 512:1024], NN) + bq[:, 512:1024]).astype(BF16)
    v_s[...] = (dot(rows, wqkv_ref[:, 1024:1536], NN) + bq[:, 1024:1536]).astype(BF16)

    edge = lax.axis_index("lat") == lax.axis_size("lat") - 1
    a_row = (iota((512, 64), 0) % 64) >= 32
    b_row = iota((512, 64), 1) >= 32
    apart = jnp.where(a_row != b_row, -1e9, 0.0)
    last_s[...] = jnp.where(edge, apart, 0.0)
    own = (iota((8, 1, 256), 2) // 32) == iota((8, 1, 256), 0)

    def window(w, carry):
        lower = (w >= 3).astype(F32)
        at = pl.ds(pl.multiple_of(w * 64, 64), 64)
        for g in range(2):
            lanes = slice(256 * g, 256 * g + 256)
            queries = jnp.where(own, q_s[at, lanes][None], jnp.zeros((), BF16)).reshape(512, 256)
            scores = dot(queries, k_s[at, lanes], NT)
            scores = scores + bias_ref[64 * g : 64 * g + 64].reshape(512, 64) + lower * last_s[...]
            scores = scores - jnp.max(scores, axis=-1, keepdims=True)
            weights = jnp.exp(scores)
            weights = (weights / jnp.sum(weights, axis=-1, keepdims=True)).astype(BF16)
            found = dot(weights, v_s[at, lanes], NN).reshape(8, 64, 256)
            att_s[at, lanes] = jnp.sum(jnp.where(own, found, 0.0), axis=0).astype(BF16)
        return carry

    lax.fori_loop(0, 6, window, 0)

    norm_s[...] = dot(att_s[...], wo_ref[...], NN).astype(BF16).astype(F32).reshape(6, 8, 8, 512)
    for g in range(4):
        w_row, w_start = ((1, 4), (0, 0), (0, 4), (1, 0))[g]
        turned = [turn(norm_s[w_row * 3 + b, w_start : w_start + 4]) for b in range(3)]
        low = low_half((4, 8, 512))
        back = jnp.concatenate([jnp.where(low, turned[b - 1], turned[b]) for b in range(3)], axis=1)
        rows = slice(4 * g, 4 * g + 4)
        result = (mixed_s[rows] + back).astype(BF16)
        mixed_s[rows] = result.astype(F32)
        cyc_ref[rows] = result
        side = pack(result.astype(F32)[:, 0:8], False).reshape(16, 512).astype(BF16)
        if g == 0:
            pc_ref[...] = side
        else:
            pe_ref[16 * (g - 1) : 16 * g] = side
    flux_ref[...] = dot(fp_ref[...], mixed_s[...].reshape(384, 512).astype(BF16), NT).astype(BF16)


def atmosphere(tok, east, south, corner, msgs, enc8, gain, wqkv, bqkv, bias, wo, fp):
    shapes = [((16, 24, 512), BF16), ((16, 384), BF16), ((48, 512), BF16), ((16, 512), BF16)]
    return pl.pallas_call(
        atmosphere_kernel,
        out_shape=[jax.ShapeDtypeStruct(*s) for s in shapes],
        in_specs=vmem(12),
        out_specs=vmem(len(shapes)),
        scratch_shapes=[
            pltpu.VMEM((16, 24, 512), F32), pltpu.VMEM((6, 8, 8, 512), F32),
            pltpu.VMEM((384, 512), BF16), pltpu.VMEM((384, 512), BF16), pltpu.VMEM((384, 512), BF16),
            pltpu.VMEM((384, 512), BF16), pltpu.VMEM((512, 64), F32),
        ],
        name="atmosphere",
    )(tok, east, south, corner, msgs, enc8, gain, wqkv, bqkv, bias, wo, fp)


FLUX_TO = [(below, 0 - dj) for below in range(2) for dj in (-2, -1, 0, 1) if (below, dj) != (0, 0)]
FLUX_PARTNERS = FLUX_TO + [(-di, -dj) for di, dj in FLUX_TO if (-di, -dj) not in FLUX_TO]


def second_kernel(
    cyc_ref, flux_ref, pe_ref, pc_ref, ocean_ref, above_ref, below_ref, left_ref, right_ref, oc_ref, kernel_ref, cbias_ref,
    fluxes_ref, west_ref, north_ref, nw_ref, conv_ref,
    pad_s, send_sem, recv_sem,
):
    at = place()
    wait_barrier = greet([at(*o) for o in FLUX_PARTNERS])
    copies = []

    def send(src, dst, offset):
        n = len(copies)
        copy = pltpu.make_async_remote_copy(
            src_ref=src, dst_ref=dst, send_sem=send_sem.at[n], recv_sem=recv_sem.at[n],
            device_id=at(*offset), device_id_type=MESH,
        )
        copies.append(copy)
        copy.start()

    wait_barrier()
    for below in range(2):
        for dj in (-1, -2, 1, 0):
            if (below, dj) != (0, 0):
                send(flux_ref, fluxes_ref.at[below * 4 + dj + 2], (below, -dj))
    send(pe_ref, west_ref, (0, 1))
    send(cyc_ref.at[pl.ds(0, 4)], north_ref, (1, 0))
    send(pc_ref, nw_ref, (1, 1))
    fluxes_ref[2] = flux_ref[...]

    la = lax.axis_index("lat")
    has_above = (la > 0).astype(F32)
    has_below = (la < lax.axis_size("lat") - 1).astype(F32)

    def put(rows, cols, values):
        for h in range(2):
            pad_s[h, rows, cols, :] = values[:, :, 128 * h : 128 * h + 128]

    def wide(values, high):
        return unpack(values.astype(F32).reshape(values.shape[0] // 8, 8, 256), high)

    put(slice(3, 19), slice(8, 40), ocean_ref[...].astype(F32))
    put(slice(3, 19), slice(0, 8), wide(left_ref[...], True))
    put(slice(3, 19), slice(40, 48), wide(right_ref[...], False))
    put(slice(0, 3), slice(8, 40), above_ref[...].astype(F32)[1:4] * has_above)
    put(slice(19, 22), slice(8, 40), below_ref[...].astype(F32)[0:3] * has_below)
    put(slice(0, 3), slice(0, 8), wide(oc_ref[3], True)[1:4] * has_above)
    put(slice(0, 3), slice(40, 48), wide(oc_ref[2], False)[1:4] * has_above)
    put(slice(19, 22), slice(0, 8), wide(oc_ref[1], True)[0:3] * has_below)
    put(slice(19, 22), slice(40, 48), wide(oc_ref[0], False)[0:3] * has_below)

    def band(i, carry):
        start = i * 8
        for h in range(2):
            lanes = slice(128 * h, 128 * h + 128)
            first_term = jnp.broadcast_to(cbias_ref[:, lanes], (8, 128))
            for b in range(4):
                sums = [first_term] * 8
                for v in range(7):
                    col = 8 * b + v + 5
                    cells = [pad_s[h, start + r, col : col + 8, :] for r in range(14)]
                    for u in range(7):
                        tap = kernel_ref[u, v : v + 1, lanes]
                        for r in range(8):
                            sums[r] = sums[r] + tap * cells[r + u]
                for r in range(8):
                    conv_ref[start + r, 8 * b : 8 * b + 8, lanes] = sums[r]
        return carry

    lax.fori_loop(0, 2, band, 0)
    for copy in copies:
        copy.wait()


def second(cyc, flux, pe, pc, ocean, above, below, left, right, oc, kernel, cbias):
    shapes = [
        ((8, 16, 384), BF16), ((48, 512), BF16), ((4, 24, 512), BF16), ((16, 512), BF16), ((16, 32, 256), F32),
    ]
    return pl.pallas_call(
        second_kernel,
        out_shape=[jax.ShapeDtypeStruct(*s) for s in shapes],
        in_specs=vmem(12),
        out_specs=vmem(len(shapes)),
        scratch_shapes=[
            pltpu.VMEM((2, 22, 48, 128), F32),
            pltpu.SemaphoreType.DMA((10,)), pltpu.SemaphoreType.DMA((10,)),
        ],
        compiler_params=pltpu.CompilerParams(collective_id=1, has_side_effects=True),
        name="second",
    )(cyc, flux, pe, pc, ocean, above, below, left, right, oc, kernel, cbias)


def ocean_kernel(
    owner_ref, block_ref, count_ref, fluxes_ref, conv_ref, overlay_ref, fenc_ref, gain_ref, w1_ref, w2_ref, ocean_ref,
    mask_ref, scale_ref, cyc_ref, west_ref, north_ref, nw_ref,
    atm_ref, out_ref,
    pre_s, rate_s,
):
    lo = lax.axis_index("lon")
    nlo = lax.axis_size("lon")
    lane = iota((16, 128), 1)
    right = lane >= 64
    picked = [jnp.zeros((16, 128), F32)] * 3
    codes = []
    for k in range(3):
        side = lax.rem(owner_ref[0, k] - lo + 1 + nlo, nlo)
        codes.append(jnp.where(k < count_ref[0, 0], side * 8 + block_ref[0, k], -1))
    for j in range(3):
        patch = lane + 128 * j
        east = column_of(patch) < 4
        south = patch < 96
        at = slice(128 * j, 128 * j + 128)
        for side in range(3):
            here = jnp.where(east, fluxes_ref[side, :, at].astype(F32), fluxes_ref[side + 1, :, at].astype(F32))
            under = jnp.where(east, fluxes_ref[4 + side, :, at].astype(F32), fluxes_ref[5 + side, :, at].astype(F32))
            tile = jnp.where(south, under, here)
            target = jnp.where(right, side * 8 + 2 * j + 1, side * 8 + 2 * j)
            for k in range(3):
                picked[k] += jnp.where(target == codes[k], tile, 0.0)
    picked = [x + pltpu.roll(x, 64, 1) for x in picked]
    columns = jnp.concatenate([jnp.where(right, picked[1], picked[0]), picked[2][:, 0:64]], axis=1)
    forcing = dot(columns.astype(BF16), overlay_ref[...].reshape(192, 512), NN)
    f_hi, f_lo = split2(forcing)
    e_hi, e_lo = split2(fenc_ref[...])
    pre_s[...] = conv_ref[...].reshape(512, 256) + dot(
        jnp.concatenate([f_hi, f_lo, f_hi], axis=0).astype(BF16),
        jnp.concatenate([e_hi, e_hi, e_lo], axis=0).astype(BF16),
        TN,
    )
    mask = jnp.broadcast_to(mask_ref[...], (16, 512)).astype(BF16)
    parts = [jnp.broadcast_to(x, (16, 256)) for x in split3(scale_ref[...])]
    row = iota((16, 256), 0)
    scale = jnp.where(row == 0, parts[0], jnp.where(row == 1, parts[1], jnp.where(row == 2, parts[2], 0.0)))
    rate_s[...] = dot(mask, scale.astype(BF16), TN)

    def cells(i, carry):
        at = pl.ds(pl.multiple_of(i * 128, 128), 128)
        normed = layer_norm(pre_s[at], gain_ref[...], 1e-06).astype(BF16)
        update = jnp.zeros((128, 256), F32)
        for c in range(4):
            cols = slice(256 * c, 256 * c + 256)
            x = dot(normed, w1_ref[:, cols], NN)
            hidden = (0.5 * x * (1.0 + lax.erf(x * (0.5**0.5)))).astype(BF16)
            update = update + dot(hidden, w2_ref[cols], NN)
        rows = pl.ds(i * 4, 4)
        state = ocean_ref[rows].astype(F32).reshape(128, 256)
        out_ref[rows] = (state + rate_s[at] * update).astype(BF16).reshape(4, 32, 256)
        return carry

    lax.fori_loop(0, 4, cells, 0)

    low = low_half((4, 8, 512))
    for g in range(4):
        rows = slice(4 * g, 4 * g + 4)
        if g == 0:
            body = north_ref[...]
            side = nw_ref[...]
        else:
            body = cyc_ref[rows]
            side = west_ref[16 * (g - 1) : 16 * g]
        side = unpack(side.astype(F32).reshape(2, 8, 512), False)
        body = body.astype(F32)
        head = jnp.where(low, side, body[:, 0:8])
        atm_ref[rows] = jnp.concatenate([head, body[:, 8:24]], axis=1).astype(BF16)


def ocean_step(owners, blocks, counts, fluxes, conv, overlay, fenc, gain, w1, w2, ocean, mask_row, scale, cyc, west, north, nw):
    shapes = [((16, 24, 512), BF16), ((16, 32, 256), BF16)]
    return pl.pallas_call(
        ocean_kernel,
        out_shape=[jax.ShapeDtypeStruct(*s) for s in shapes],
        in_specs=smem(3) + vmem(14),
        out_specs=vmem(len(shapes)),
        scratch_shapes=[pltpu.VMEM((512, 256), F32), pltpu.VMEM((512, 256), F32)],
        name="ocean",
    )(owners, blocks, counts, fluxes, conv, overlay, fenc, gain, w1, w2, ocean, mask_row, scale, cyc, west, north, nw)


def local(
    atmos_patch_tokens,
    atmos_norm_gain,
    query_key_value_weight,
    query_key_value_bias,
    relative_bias_grid,
    attention_output_weight,
    flux_projector,
    surface_encoder,
    ocean_cell_state,
    land_sea_mask,
    depthwise_conv_kernel,
    depthwise_conv_bias,
    ocean_norm_gain,
    pointwise_expand,
    pointwise_contract,
    layer_update_scale,
    forcing_encoder,
    surface_projector,
    overlay_area_weight,
    owners,
    owner_tile_blocks,
    counts,
):
    owners = owners.reshape(1, 3)
    blocks = owner_tile_blocks.reshape(1, 3)
    overlay = overlay_area_weight.reshape(3, 64, 512)
    mask_row = land_sea_mask.reshape(1, 512).astype(F32)
    proj = surface_projector.T
    proj8 = jnp.concatenate([proj, proj], axis=0)
    enc8 = jnp.concatenate([surface_encoder, surface_encoder], axis=0)
    msgs, east, south, corner, above, below, left, right, oc, bias = first(
        owners, blocks, counts, atmos_patch_tokens, ocean_cell_state, mask_row, overlay, proj8, relative_bias_grid
    )
    cyc, flux, pe, pc = atmosphere(
        atmos_patch_tokens, east, south, corner, msgs, enc8, atmos_norm_gain.reshape(1, 512), query_key_value_weight,
        query_key_value_bias.reshape(1, 1536), bias, attention_output_weight, flux_projector.T,
    )
    fluxes, west, north, nw, conv = second(
        cyc, flux, pe, pc, ocean_cell_state, above, below, left, right, oc, depthwise_conv_kernel,
        depthwise_conv_bias.reshape(1, 256),
    )
    atm_out, ocean_out = ocean_step(
        owners, blocks, counts, fluxes, conv, overlay, forcing_encoder, ocean_norm_gain.reshape(1, 256), pointwise_expand,
        pointwise_contract, ocean_cell_state, mask_row, layer_update_scale.reshape(1, 256), cyc, west, north, nw,
    )
    return atm_out, ocean_out


def solution(mesh):
    rep = P()
    placed = (
        P("lat", "lon", None), rep, rep, rep, rep, rep, rep, rep, P("lat", "lon", None), P("lat", "lon"),
        rep, rep, rep, rep, rep, rep, rep, rep, P("lat", "lon", None, None, None),
        P("lat", "lon", None), P("lat", "lon", None), P("lat", "lon"),
    )
    return jax.shard_map(
        local,
        mesh=mesh,
        in_specs=placed,
        out_specs=(P("lat", "lon", None), P("lat", "lon", None)),
        check_vma=False,
    )
```

```python
import functools

import jax
import jax.numpy as jnp
from jax import lax
from jax.experimental import pallas as pl
from jax.experimental.pallas import tpu as pltpu
from jax.sharding import PartitionSpec as P

F32 = jnp.float32
BF16 = jnp.bfloat16
MESH = pl.DeviceIdType.MESH
HEADS = 16
HALF = 8
WIN = 8
NT = (((1,), (1,)), ((), ()))
TN = (((0,), (0,)), ((), ()))
NN = (((1,), (0,)), ((), ()))


def dot(a, b, dims):
    return lax.dot_general(a, b, dims, preferred_element_type=F32)


def iota(shape, dim):
    return lax.broadcasted_iota(jnp.int32, shape, dim)


def low_half(shape):
    return iota(shape, len(shape) - 2) % 8 < 4


def turn(x):
    return pltpu.roll(x, 4, x.ndim - 2)


def pack(x, high):
    n, _, lanes = x.shape
    x = x.reshape(n // 2, 2, 8, lanes)
    even, odd = x[:, 0], x[:, 1]
    if high:
        even = turn(even)
    else:
        odd = turn(odd)
    return jnp.where(low_half(even.shape), even, odd)


def unpack(x, high):
    n, _, lanes = x.shape
    other = turn(x)
    pair = (other, x) if high else (x, other)
    return jnp.stack(pair, axis=1).reshape(2 * n, 8, lanes)


def split2(x):
    top = x.astype(BF16).astype(F32)
    return top, x - top


def split3(x):
    top, rest = split2(x)
    middle, last = split2(rest)
    return top, middle, last


def greet(partners):
    barrier = pltpu.get_barrier_semaphore()
    for device in partners:
        pl.semaphore_signal(barrier, inc=1, device_id=device, device_id_type=MESH)
    return lambda: pl.semaphore_wait(barrier, len(partners))


def place():
    la, lo = lax.axis_index("lat"), lax.axis_index("lon")
    nla, nlo = lax.axis_size("lat"), lax.axis_size("lon")
    return lambda di, dj: (lax.rem(la + di + nla, nla), lax.rem(lo + dj + nlo, nlo))


def vmem(n):
    return [pl.BlockSpec(memory_space=pltpu.VMEM)] * n


def smem(n):
    return [pl.BlockSpec(memory_space=pltpu.SMEM)] * n


def anywhere(n):
    return [pl.BlockSpec(memory_space=pl.ANY)] * n


def layer_norm(x, gain, epsilon):
    average = jnp.mean(x, axis=-1, keepdims=True)
    centred = x - average
    spread = jnp.mean(centred * centred, axis=-1, keepdims=True)
    return centred * lax.rsqrt(spread + epsilon) * gain


def column_of(patch):
    p = patch.astype(F32)
    return p - 24.0 * jnp.floor((p + 0.5) * (1.0 / 24.0))


def mask_row(mask):
    wide = jnp.concatenate([mask.astype(F32), jnp.zeros((16, 96), F32)], axis=1)
    moved = [wide if q == 0 else pltpu.roll(wide, 32 * q, 1) for q in range(4)]
    parts = [sum(moved[q][4 * j + q : 4 * j + q + 1] for q in range(4)) for j in range(4)]
    return jnp.concatenate(parts, axis=1)


PARTNERS = [(0, 1), (0, -1), (0, 2), (0, -2), (1, 0), (-1, 0)]
COPIES = 32


def surface_message(owner_ref, block_ref, count_ref, ocean_ref, mask_ref, overlay_ref, proj_s, msg_s):
    lo = lax.axis_index("lon")
    nlo = lax.axis_size("lon")
    parts = jnp.concatenate(split3(proj_s[...]), axis=0).astype(BF16)
    surf = dot(parts, ocean_ref[...].reshape(512, 256), NT)
    surf = ((surf[0:8] + surf[8:16] + surf[16:24]) * mask_row(mask_ref[...])).astype(BF16)
    row = iota((8, 128), 0)
    twice = []
    codes = jnp.full((8, 128), -1.0, F32)
    for k in range(3):
        block = overlay_ref[k]
        twice.append(dot(surf, jnp.concatenate([block, block], axis=0), NT))
        side = lax.rem(owner_ref[0, k] - lo + 1 + nlo, nlo)
        code = jnp.where(k < count_ref[0, 0], side * 8 + block_ref[0, k], -1).astype(F32)
        codes = jnp.where(row == 4 + k, code, codes)
    msg_s[0:8] = jnp.where(row < 4, twice[0], twice[1])
    msg_s[8:16] = jnp.where(row < 4, twice[2], codes)


def gather_surface(msgs_ref):
    upper = iota((8, 128), 0) < 4
    right = iota((8, 128), 1) >= 64
    tiles = []
    for tile in range(2):
        sums = [jnp.zeros((8, 128), F32)] * 3
        for side in range(3):
            slot = tile - side + 2
            a = msgs_ref[slot, 0:8, :]
            b = msgs_ref[slot, 8:16, :]
            code_a = jnp.where(upper, b[4:5], b[5:6])
            code_b = jnp.where(upper, b[6:7], -1.0)
            for j in range(3):
                target = jnp.where(right, side * 8.0 + 2 * j + 1, side * 8.0 + 2 * j)
                sums[j] += jnp.where(code_a == target, a, 0.0) + jnp.where(code_b == target, b, 0.0)
        tiles.append(sums)
    return [
        jnp.where(column_of(iota((8, 128), 1) + 128 * j) < 4, tiles[1][j], tiles[0][j]) for j in range(3)
    ]


def bias_table(grid_ref, table_s, bias_s):
    grid = jnp.concatenate([grid_ref[...], jnp.zeros((16, 31), F32)], axis=1)
    for ra in range(8):
        rolled = grid if ra == 0 else pltpu.roll(grid, 256 - 15 * ra, 1)
        table_s[:, ra, :] = rolled[:, 0:128]
    parts = [x.astype(BF16) for x in split3(table_s[...].reshape(128, 128))]
    entry = iota((128, 64), 0)
    lane = iota((128, 64), 1)
    for ca in range(8):
        chosen = (entry == (7 - lane // 8) * 15 + ca - lane % 8 + 7).astype(BF16)
        found = (dot(parts[0], chosen, NN) + dot(parts[1], chosen, NN)) + dot(parts[2], chosen, NN)
        bias_s[:, ca, :] = found


def add_surface(sst, enc_s):
    s_hi, s_lo = split2(sst)
    e_hi, e_lo = split2(enc_s[...])
    left = jnp.concatenate([s_hi, s_lo, s_hi], axis=0).astype(BF16)
    right = jnp.concatenate([e_hi, e_hi, e_lo], axis=0).astype(BF16)
    return dot(left, right, TN)


def normalise(g, tokens, side, gain, mixed_s, norm_s):
    low = low_half((4, 8, 512))
    rows = slice(4 * g, 4 * g + 4)
    tokens = tokens.astype(F32)
    side = unpack(side.astype(F32).reshape(2, 8, 512), False)
    head = jnp.where(low, side, tokens[:, 0:8])
    tokens = jnp.concatenate([head, tokens[:, 8:24]], axis=1)
    mixed = (tokens + mixed_s[rows]).astype(BF16).astype(F32)
    mixed_s[rows] = mixed
    normed = layer_norm(mixed, gain, 1e-05)
    turned = [turn(normed[:, 8 * b : 8 * b + 8]) for b in range(3)]
    w_row, w_start = WINDOW_OF[g]
    for b in range(3):
        norm_s[w_row * 3 + b, w_start : w_start + 4] = jnp.where(low, turned[b], turned[(b + 1) % 3])


WINDOW_OF = ((1, 4), (0, 0), (0, 4), (1, 0))


def attend(w_row, norm_s, wqkv_s, bqkv_ref, wo_s, bias_s, last_s, q_s, k_s, v_s, att_s):
    rows = norm_s[3 * w_row : 3 * w_row + 3].reshape(192, 512).astype(BF16)
    for part, ref in enumerate((q_s, k_s, v_s)):
        cols = slice(512 * part, 512 * part + 512)
        value = dot(rows, wqkv_s[:, cols], NN) + bqkv_ref[cols].reshape(1, 512)
        if part == 0:
            value = value * 32 ** (-0.5)
        ref[...] = value.astype(BF16)
    own = (iota((8, 1, 256), 2) // 32) == iota((8, 1, 256), 0)

    def window(w, carry):
        at = pl.ds(pl.multiple_of(w * 64, 64), 64)
        for g in range(2):
            lanes = slice(256 * g, 256 * g + 256)
            queries = jnp.where(own, q_s[at, lanes][None], jnp.zeros((), BF16)).reshape(512, 256)
            scores = dot(queries, k_s[at, lanes], NT)
            scores = scores + bias_s[64 * g : 64 * g + 64].reshape(512, 64)
            if w_row == 1:
                scores = scores + last_s[...]
            scores = scores - jnp.max(scores, axis=-1, keepdims=True)
            weights = jnp.exp(scores)
            weights = (weights / jnp.sum(weights, axis=-1, keepdims=True)).astype(BF16)
            found = dot(weights, v_s[at, lanes], NN).reshape(8, 64, 256)
            att_s[at, lanes] = jnp.sum(jnp.where(own, found, 0.0), axis=0).astype(BF16)
        return carry

    lax.fori_loop(0, 3, window, 0)
    projected = dot(att_s[...], wo_s[...], NN).astype(BF16).astype(F32)
    norm_s[3 * w_row : 3 * w_row + 3] = projected.reshape(3, 8, 8, 512)


def finish(g, norm_s, mixed_s, cyc_ref, side_ref):
    w_row, w_start = WINDOW_OF[g]
    turned = [turn(norm_s[w_row * 3 + b, w_start : w_start + 4]) for b in range(3)]
    low = low_half((4, 8, 512))
    back = jnp.concatenate([jnp.where(low, turned[b - 1], turned[b]) for b in range(3)], axis=1)
    rows = slice(4 * g, 4 * g + 4)
    result = (mixed_s[rows] + back).astype(BF16)
    mixed_s[rows] = result.astype(F32)
    cyc_ref[rows] = result
    side_ref[...] = pack(result.astype(F32)[:, 0:8], False).reshape(16, 512).astype(BF16)


def convolve(pad_s, kernel_ref, cbias_ref, conv_ref):
    def band(i, carry):
        start = i * 8
        for h in range(2):
            lanes = slice(128 * h, 128 * h + 128)
            first_term = jnp.broadcast_to(cbias_ref[:, lanes], (8, 128))
            for b in range(4):
                sums = [first_term] * 8
                for v in range(7):
                    col = 8 * b + v + 5
                    cells = [pad_s[h, start + r, col : col + 8, :] for r in range(14)]
                    for u in range(7):
                        tap = kernel_ref[u, v : v + 1, lanes]
                        for r in range(8):
                            sums[r] = sums[r] + tap * cells[r + u]
                for r in range(8):
                    conv_ref[start + r, 8 * b : 8 * b + 8, lanes] = sums[r]
        return carry

    lax.fori_loop(0, 2, band, 0)


def step_kernel(
    owner_ref, block_ref, count_ref, tok_ref, ocean_ref, mask_ref, overlay_ref, proj_ref, grid_ref, enc_ref, gain_ref, bqkv_ref,
    fp_ref, kernel_ref, cbias_ref, wqkv_ref, wo_ref,
    cyc_ref, fluxes_ref, west_ref, north_ref, nw_ref, conv_ref,
    wqkv_s, wo_s, proj_s, enc_s, msg_s, msgs_s, side_s, east_s, south_s, corner_s, sst_s, under_s, table_s, bias_s, last_s,
    mixed_s, norm_s, q_s, k_s, v_s, att_s, above_s, below_s, leave_s, cols_s, pad_s, pe_s, flux_s,
    load_sem, send_sem, recv_sem,
):
    at = place()
    la = lax.axis_index("lat")
    nla = lax.axis_size("lat")
    wait_barrier = greet([at(*o) for o in PARTNERS])
    loads = [
        pltpu.make_async_copy(wqkv_ref, wqkv_s, load_sem.at[0]),
        pltpu.make_async_copy(wo_ref, wo_s, load_sem.at[1]),
    ]
    for load in loads:
        load.start()
    copies = []

    def send(src, dst, offset):
        n = len(copies)
        copy = pltpu.make_async_remote_copy(
            src_ref=src, dst_ref=dst, send_sem=send_sem.at[n], recv_sem=recv_sem.at[n],
            device_id=at(*offset), device_id_type=MESH,
        )
        copies.append(copy)
        copy.start()
        return copy

    for half in range(2):
        proj_s[4 * half : 4 * half + 4] = proj_ref[...]
        enc_s[4 * half : 4 * half + 4] = enc_ref[...]
    surface_message(owner_ref, block_ref, count_ref, ocean_ref, mask_ref, overlay_ref, proj_s, msg_s)
    side_s[...] = pack(tok_ref[:, 0:8, :].astype(F32), False).reshape(64, 512).astype(BF16)

    wait_barrier()
    messages = [send(msg_s, msgs_s.at[dj + 1], (0, -dj)) for dj in (2, 1, -1)]
    msgs_s[1] = msg_s[...]
    east = send(side_s, east_s, (0, -1))

    bias_table(grid_ref, table_s, bias_s)
    edge = la == nla - 1
    a_row = (iota((512, 64), 0) % 64) >= 32
    b_row = iota((512, 64), 1) >= 32
    last_s[...] = jnp.where(edge, jnp.where(a_row != b_row, -1e9, 0.0), 0.0)

    for copy in messages:
        copy.wait_recv()
    sst = gather_surface(msgs_s)
    sst_s[...] = sst[0]
    under = send(sst_s, under_s, (-1, 0))
    south = send(tok_ref.at[pl.ds(0, 4)], south_s, (-1, 0))
    below = send(ocean_ref.at[pl.ds(0, 3)], below_s, (-1, 0))
    above = send(ocean_ref.at[pl.ds(13, 3)], above_s, (1, 0))
    mixed_s[...] = add_surface(jnp.concatenate(sst, axis=1), enc_s).reshape(16, 24, 512)
    gain = gain_ref[...].reshape(1, 1, 512)
    east.wait_recv()
    corner = send(east_s.at[pl.ds(0, 16)], corner_s, (-1, 0))
    for g in (1, 2, 3):
        normalise(g, tok_ref[4 * g : 4 * g + 4], east_s[16 * g : 16 * g + 16], gain, mixed_s, norm_s)
    for load in loads:
        load.wait()
    attend(0, norm_s, wqkv_s, bqkv_ref, wo_s, bias_s, last_s, q_s, k_s, v_s, att_s)
    for g in (1, 2):
        finish(g, norm_s, mixed_s, cyc_ref, pe_s.at[pl.ds(16 * g, 16)])
    send(pe_s.at[pl.ds(16, 32)], west_ref.at[pl.ds(16, 32)], (0, 1))

    def put(rows, cols, values):
        for h in range(2):
            pad_s[h, rows, cols, :] = values[:, :, 128 * h : 128 * h + 128]

    below.wait_recv()
    above.wait_recv()
    put(slice(3, 19), slice(8, 40), ocean_ref[...].astype(F32))
    put(slice(0, 3), slice(8, 40), above_s[...].astype(F32) * (la > 0).astype(F32))
    put(slice(19, 22), slice(8, 40), below_s[...].astype(F32) * (la < nla - 1).astype(F32))
    for h in range(2):
        lanes = slice(128 * h, 128 * h + 128)
        leave_s[0, :, lanes] = pack(pad_s[h, :, 32:40, :], True).reshape(88, 128).astype(BF16)
        leave_s[1, :, lanes] = pack(pad_s[h, :, 8:16, :], False).reshape(88, 128).astype(BF16)
    sides = [send(leave_s.at[0], cols_s.at[0], (0, 1)), send(leave_s.at[1], cols_s.at[1], (0, -1))]

    for copy in (under, south, corner):
        copy.wait_recv()
    mixed_s[0:4] = add_surface(under_s[...], enc_s)[0:96].reshape(4, 24, 512)
    normalise(0, south_s[...], corner_s[...], gain, mixed_s, norm_s)
    attend(1, norm_s, wqkv_s, bqkv_ref, wo_s, bias_s, last_s, q_s, k_s, v_s, att_s)
    for g in (3, 0):
        finish(g, norm_s, mixed_s, cyc_ref, pe_s.at[pl.ds(16 * g, 16)])
    flux_s[...] = dot(fp_ref[...], mixed_s[...].reshape(384, 512).astype(BF16), NT).astype(BF16)
    for down in (1, 0):
        for dj in (1, -2, -1, 0):
            if (down, dj) != (0, 0):
                send(flux_s, fluxes_ref.at[down * 4 + dj + 2], (down, -dj))
    send(cyc_ref.at[pl.ds(0, 4)], north_ref, (1, 0))
    send(pe_s.at[pl.ds(48, 16)], west_ref.at[pl.ds(48, 16)], (0, 1))
    send(pe_s.at[pl.ds(0, 16)], nw_ref, (1, 1))
    fluxes_ref[2] = flux_s[...]

    for copy in sides:
        copy.wait_recv()
    for n, high in ((0, True), (1, False)):
        values = unpack(cols_s[n].astype(F32).reshape(11, 8, 256), high)
        put(slice(0, 22), slice(40 * n, 40 * n + 8), values)
    convolve(pad_s, kernel_ref, cbias_ref, conv_ref)

    early = [*messages, east, under, south, below, above, corner, *sides]
    for copy in copies:
        copy.wait_send()
        if not any(copy is other for other in early):
            copy.wait_recv()


def step(owners, blocks, counts, tok, ocean, mask, overlay, proj, grid, enc, gain, bqkv, fp, kernel, cbias, wqkv, wo):
    shapes = [
        ((16, 24, 512), BF16), ((8, 16, 384), BF16), ((64, 512), BF16), ((4, 24, 512), BF16), ((16, 512), BF16),
        ((16, 32, 256), F32),
    ]
    return pl.pallas_call(
        step_kernel,
        out_shape=[jax.ShapeDtypeStruct(*s) for s in shapes],
        in_specs=smem(3) + vmem(12) + anywhere(2),
        out_specs=vmem(len(shapes)),
        scratch_shapes=[
            pltpu.VMEM((512, 1536), BF16), pltpu.VMEM((512, 512), BF16), pltpu.VMEM((8, 256), F32), pltpu.VMEM((8, 512), F32),
            pltpu.VMEM((16, 128), F32), pltpu.VMEM((4, 16, 128), F32), pltpu.VMEM((64, 512), BF16), pltpu.VMEM((64, 512), BF16),
            pltpu.VMEM((4, 24, 512), BF16), pltpu.VMEM((16, 512), BF16), pltpu.VMEM((8, 128), F32), pltpu.VMEM((8, 128), F32),
            pltpu.VMEM((16, 8, 128), F32), pltpu.VMEM((128, 8, 64), F32), pltpu.VMEM((512, 64), F32),
            pltpu.VMEM((16, 24, 512), F32), pltpu.VMEM((6, 8, 8, 512), F32),
            pltpu.VMEM((192, 512), BF16), pltpu.VMEM((192, 512), BF16), pltpu.VMEM((192, 512), BF16), pltpu.VMEM((192, 512), BF16),
            pltpu.VMEM((3, 32, 256), BF16), pltpu.VMEM((3, 32, 256), BF16), pltpu.VMEM((2, 88, 256), BF16),
            pltpu.VMEM((2, 88, 256), BF16), pltpu.VMEM((2, 22, 48, 128), F32), pltpu.VMEM((64, 512), BF16),
            pltpu.VMEM((16, 384), BF16),
            pltpu.SemaphoreType.DMA((2,)), pltpu.SemaphoreType.DMA((COPIES,)), pltpu.SemaphoreType.DMA((COPIES,)),
        ],
        compiler_params=pltpu.CompilerParams(collective_id=0, has_side_effects=True),
        name="step",
    )(owners, blocks, counts, tok, ocean, mask, overlay, proj, grid, enc, gain, bqkv, fp, kernel, cbias, wqkv, wo)


def ocean_kernel(
    owner_ref, block_ref, count_ref, fluxes_ref, conv_ref, overlay_ref, fenc_ref, gain_ref, w1_ref, w2_ref, ocean_ref,
    mask_ref, scale_ref, cyc_ref, west_ref, north_ref, nw_ref,
    atm_ref, out_ref,
    pre_s, rate_s,
):
    lo = lax.axis_index("lon")
    nlo = lax.axis_size("lon")
    lane = iota((16, 128), 1)
    right = lane >= 64
    picked = [jnp.zeros((16, 128), F32)] * 3
    codes = []
    for k in range(3):
        side = lax.rem(owner_ref[0, k] - lo + 1 + nlo, nlo)
        codes.append(jnp.where(k < count_ref[0, 0], side * 8 + block_ref[0, k], -1))
    for j in range(3):
        patch = lane + 128 * j
        east = column_of(patch) < 4
        south = patch < 96
        at = slice(128 * j, 128 * j + 128)
        for side in range(3):
            here = jnp.where(east, fluxes_ref[side, :, at].astype(F32), fluxes_ref[side + 1, :, at].astype(F32))
            under = jnp.where(east, fluxes_ref[4 + side, :, at].astype(F32), fluxes_ref[5 + side, :, at].astype(F32))
            tile = jnp.where(south, under, here)
            target = jnp.where(right, side * 8 + 2 * j + 1, side * 8 + 2 * j)
            for k in range(3):
                picked[k] += jnp.where(target == codes[k], tile, 0.0)
    picked = [x + pltpu.roll(x, 64, 1) for x in picked]
    columns = jnp.concatenate([jnp.where(right, picked[1], picked[0]), picked[2][:, 0:64]], axis=1)
    forcing = dot(columns.astype(BF16), overlay_ref[...].reshape(192, 512), NN)
    f_hi, f_lo = split2(forcing)
    e_hi, e_lo = split2(fenc_ref[...])
    pre_s[...] = conv_ref[...].reshape(512, 256) + dot(
        jnp.concatenate([f_hi, f_lo, f_hi], axis=0).astype(BF16),
        jnp.concatenate([e_hi, e_hi, e_lo], axis=0).astype(BF16),
        TN,
    )
    mask = jnp.broadcast_to(mask_row(mask_ref[...]), (16, 512)).astype(BF16)
    parts = [jnp.broadcast_to(x, (16, 256)) for x in split3(scale_ref[...])]
    row = iota((16, 256), 0)
    scale = jnp.where(row == 0, parts[0], jnp.where(row == 1, parts[1], jnp.where(row == 2, parts[2], 0.0)))
    rate_s[...] = dot(mask, scale.astype(BF16), TN)

    def cells(i, carry):
        at = pl.ds(pl.multiple_of(i * 128, 128), 128)
        normed = layer_norm(pre_s[at], gain_ref[...], 1e-06).astype(BF16)
        update = jnp.zeros((128, 256), F32)
        for c in range(4):
            cols = slice(256 * c, 256 * c + 256)
            x = dot(normed, w1_ref[:, cols], NN)
            hidden = (0.5 * x * (1.0 + lax.erf(x * (0.5**0.5)))).astype(BF16)
            update = update + dot(hidden, w2_ref[cols], NN)
        rows = pl.ds(i * 4, 4)
        state = ocean_ref[rows].astype(F32).reshape(128, 256)
        out_ref[rows] = (state + rate_s[at] * update).astype(BF16).reshape(4, 32, 256)
        return carry

    lax.fori_loop(0, 4, cells, 0)

    low = low_half((4, 8, 512))
    for g in range(4):
        rows = slice(4 * g, 4 * g + 4)
        if g == 0:
            body = north_ref[...]
            side = nw_ref[...]
        else:
            body = cyc_ref[rows]
            side = west_ref[16 * g : 16 * g + 16]
        side = unpack(side.astype(F32).reshape(2, 8, 512), False)
        body = body.astype(F32)
        head = jnp.where(low, side, body[:, 0:8])
        atm_ref[rows] = jnp.concatenate([head, body[:, 8:24]], axis=1).astype(BF16)


def ocean_step(owners, blocks, counts, fluxes, conv, overlay, fenc, gain, w1, w2, ocean, mask, scale, cyc, west, north, nw):
    shapes = [((16, 24, 512), BF16), ((16, 32, 256), BF16)]
    return pl.pallas_call(
        ocean_kernel,
        out_shape=[jax.ShapeDtypeStruct(*s) for s in shapes],
        in_specs=smem(3) + vmem(14),
        out_specs=vmem(len(shapes)),
        scratch_shapes=[pltpu.VMEM((512, 256), F32), pltpu.VMEM((512, 256), F32)],
        name="ocean",
    )(owners, blocks, counts, fluxes, conv, overlay, fenc, gain, w1, w2, ocean, mask, scale, cyc, west, north, nw)


def local(
    atmos_patch_tokens,
    atmos_norm_gain,
    query_key_value_weight,
    query_key_value_bias,
    relative_bias_grid,
    attention_output_weight,
    flux_projector,
    surface_encoder,
    ocean_cell_state,
    land_sea_mask,
    depthwise_conv_kernel,
    depthwise_conv_bias,
    ocean_norm_gain,
    pointwise_expand,
    pointwise_contract,
    layer_update_scale,
    forcing_encoder,
    surface_projector,
    overlay_area_weight,
    owners,
    owner_tile_blocks,
    counts,
):
    owners = owners.reshape(1, 3)
    blocks = owner_tile_blocks.reshape(1, 3)
    overlay = overlay_area_weight.reshape(3, 64, 512)
    cyc, fluxes, west, north, nw, conv = step(
        owners, blocks, counts, atmos_patch_tokens, ocean_cell_state, land_sea_mask, overlay, surface_projector.T,
        relative_bias_grid, surface_encoder, atmos_norm_gain.reshape(1, 512), query_key_value_bias, flux_projector.T,
        depthwise_conv_kernel, depthwise_conv_bias.reshape(1, 256), query_key_value_weight, attention_output_weight,
    )
    atm_out, ocean_out = ocean_step(
        owners, blocks, counts, fluxes, conv, overlay, forcing_encoder, ocean_norm_gain.reshape(1, 256), pointwise_expand,
        pointwise_contract, ocean_cell_state, land_sea_mask, layer_update_scale.reshape(1, 256), cyc, west, north, nw,
    )
    return atm_out, ocean_out


def solution(mesh):
    rep = P()
    placed = (
        P("lat", "lon", None), rep, rep, rep, rep, rep, rep, rep, P("lat", "lon", None), P("lat", "lon"),
        rep, rep, rep, rep, rep, rep, rep, rep, P("lat", "lon", None, None, None),
        P("lat", "lon", None), P("lat", "lon", None), P("lat", "lon"),
    )
    return jax.shard_map(
        local,
        mesh=mesh,
        in_specs=placed,
        out_specs=(P("lat", "lon", None), P("lat", "lon", None)),
        check_vma=False,
    )
```

```python
import types

import jax
import jax.numpy as jnp
from jax import lax
from jax.experimental import pallas as pl
from jax.experimental.pallas import tpu as pltpu
from jax.sharding import PartitionSpec as P

F32 = jnp.float32
BF16 = jnp.bfloat16
MESH = pl.DeviceIdType.MESH
HEADS = 16
HALF = 8
WIN = 8
NT = (((1,), (1,)), ((), ()))
TN = (((0,), (0,)), ((), ()))
NN = (((1,), (0,)), ((), ()))


def dot(a, b, dims):
    return lax.dot_general(a, b, dims, preferred_element_type=F32)


def iota(shape, dim):
    return lax.broadcasted_iota(jnp.int32, shape, dim)


def low_half(shape):
    return iota(shape, len(shape) - 2) % 8 < 4


def turn(x):
    return pltpu.roll(x, 4, x.ndim - 2)


def pack(x, high):
    n, _, lanes = x.shape
    x = x.reshape(n // 2, 2, 8, lanes)
    even, odd = x[:, 0], x[:, 1]
    if high:
        even = turn(even)
    else:
        odd = turn(odd)
    return jnp.where(low_half(even.shape), even, odd)


def unpack(x, high):
    n, _, lanes = x.shape
    other = turn(x)
    pair = (other, x) if high else (x, other)
    return jnp.stack(pair, axis=1).reshape(2 * n, 8, lanes)


def split2(x):
    top = x.astype(BF16).astype(F32)
    return top, x - top


def split3(x):
    top, rest = split2(x)
    middle, last = split2(rest)
    return top, middle, last


def greet(partners):
    barrier = pltpu.get_barrier_semaphore()
    for device in partners:
        pl.semaphore_signal(barrier, inc=1, device_id=device, device_id_type=MESH)
    return lambda: pl.semaphore_wait(barrier, len(partners))


def place():
    la, lo = lax.axis_index("lat"), lax.axis_index("lon")
    nla, nlo = lax.axis_size("lat"), lax.axis_size("lon")
    return lambda di, dj: (lax.rem(la + di + nla, nla), lax.rem(lo + dj + nlo, nlo))


def vmem(n):
    return [pl.BlockSpec(memory_space=pltpu.VMEM)] * n


def smem(n):
    return [pl.BlockSpec(memory_space=pltpu.SMEM)] * n


def anywhere(n):
    return [pl.BlockSpec(memory_space=pl.ANY)] * n


def layer_norm(x, gain, epsilon):
    average = jnp.mean(x, axis=-1, keepdims=True)
    centred = x - average
    spread = jnp.mean(centred * centred, axis=-1, keepdims=True)
    return centred * lax.rsqrt(spread + epsilon) * gain


def column_of(patch):
    p = patch.astype(F32)
    return p - 24.0 * jnp.floor((p + 0.5) * (1.0 / 24.0))


def mask_row(mask):
    wide = jnp.concatenate([mask.astype(F32), jnp.zeros((16, 96), F32)], axis=1)
    moved = [wide if q == 0 else pltpu.roll(wide, 32 * q, 1) for q in range(4)]
    parts = [sum(moved[q][4 * j + q : 4 * j + q + 1] for q in range(4)) for j in range(4)]
    return jnp.concatenate(parts, axis=1)


PARTNERS = [(0, 1), (0, -1), (0, 2), (0, -2), (1, 0), (-1, 0)]
COPIES = 32


def surface_message(owner_ref, block_ref, count_ref, ocean_ref, mask_ref, overlay_ref, proj_s, msg_s):
    lo = lax.axis_index("lon")
    nlo = lax.axis_size("lon")
    parts = jnp.concatenate(split3(proj_s[...]), axis=0).astype(BF16)
    surf = dot(parts, ocean_ref[...].reshape(512, 256), NT)
    surf = ((surf[0:8] + surf[8:16] + surf[16:24]) * mask_row(mask_ref[...])).astype(BF16)
    row = iota((8, 128), 0)
    twice = []
    codes = jnp.full((8, 128), -1.0, F32)
    for k in range(3):
        block = overlay_ref[k]
        twice.append(dot(surf, jnp.concatenate([block, block], axis=0), NT))
        side = lax.rem(owner_ref[0, k] - lo + 1 + nlo, nlo)
        code = jnp.where(k < count_ref[0, 0], side * 8 + block_ref[0, k], -1).astype(F32)
        codes = jnp.where(row == 4 + k, code, codes)
    msg_s[0:8] = jnp.where(row < 4, twice[0], twice[1])
    msg_s[8:16] = jnp.where(row < 4, twice[2], codes)


def gather_surface(msgs_ref):
    upper = iota((8, 128), 0) < 4
    right = iota((8, 128), 1) >= 64
    tiles = []
    for tile in range(2):
        sums = [jnp.zeros((8, 128), F32)] * 3
        for side in range(3):
            slot = tile - side + 2
            a = msgs_ref[slot, 0:8, :]
            b = msgs_ref[slot, 8:16, :]
            code_a = jnp.where(upper, b[4:5], b[5:6])
            code_b = jnp.where(upper, b[6:7], -1.0)
            for j in range(3):
                target = jnp.where(right, side * 8.0 + 2 * j + 1, side * 8.0 + 2 * j)
                sums[j] += jnp.where(code_a == target, a, 0.0) + jnp.where(code_b == target, b, 0.0)
        tiles.append(sums)
    return [
        jnp.where(column_of(iota((8, 128), 1) + 128 * j) < 4, tiles[1][j], tiles[0][j]) for j in range(3)
    ]


def bias_table(grid_ref, table_s, bias_s):
    grid = jnp.concatenate([grid_ref[...], jnp.zeros((16, 31), F32)], axis=1)
    for ra in range(8):
        rolled = grid if ra == 0 else pltpu.roll(grid, 256 - 15 * ra, 1)
        table_s[:, ra, :] = rolled[:, 0:128]
    parts = [x.astype(BF16) for x in split3(table_s[...].reshape(128, 128))]
    entry = iota((128, 64), 0)
    lane = iota((128, 64), 1)
    for ca in range(8):
        chosen = (entry == (7 - lane // 8) * 15 + ca - lane % 8 + 7).astype(BF16)
        found = (dot(parts[0], chosen, NN) + dot(parts[1], chosen, NN)) + dot(parts[2], chosen, NN)
        bias_s[:, ca, :] = found


def add_surface(sst, enc_s):
    s_hi, s_lo = split2(sst)
    e_hi, e_lo = split2(enc_s[...])
    left = jnp.concatenate([s_hi, s_lo, s_hi], axis=0).astype(BF16)
    right = jnp.concatenate([e_hi, e_hi, e_lo], axis=0).astype(BF16)
    return dot(left, right, TN)


def normalise(g, tokens, side, gain, mixed_s, norm_s):
    low = low_half((4, 8, 512))
    rows = slice(4 * g, 4 * g + 4)
    tokens = tokens.astype(F32)
    side = unpack(side.astype(F32).reshape(2, 8, 512), False)
    head = jnp.where(low, side, tokens[:, 0:8])
    tokens = jnp.concatenate([head, tokens[:, 8:24]], axis=1)
    mixed = (tokens + mixed_s[rows]).astype(BF16).astype(F32)
    mixed_s[rows] = mixed
    normed = layer_norm(mixed, gain, 1e-05)
    turned = [turn(normed[:, 8 * b : 8 * b + 8]) for b in range(3)]
    w_row, w_start = WINDOW_OF[g]
    for b in range(3):
        norm_s[w_row * 3 + b, w_start : w_start + 4] = jnp.where(low, turned[b], turned[(b + 1) % 3])


WINDOW_OF = ((1, 4), (0, 0), (0, 4), (1, 0))


def attend(w_row, norm_s, wqkv_s, bqkv_ref, wo_s, bias_s, last_s, q_s, k_s, v_s, att_s):
    rows = norm_s[3 * w_row : 3 * w_row + 3].reshape(192, 512).astype(BF16)
    for part, ref in enumerate((q_s, k_s, v_s)):
        cols = slice(512 * part, 512 * part + 512)
        value = dot(rows, wqkv_s[:, cols], NN) + bqkv_ref[cols].reshape(1, 512)
        if part == 0:
            value = value * 32 ** (-0.5)
        ref[...] = value.astype(BF16)
    own = (iota((8, 1, 256), 2) // 32) == iota((8, 1, 256), 0)

    def window(w, carry):
        at = pl.ds(pl.multiple_of(w * 64, 64), 64)
        for g in range(2):
            lanes = slice(256 * g, 256 * g + 256)
            queries = jnp.where(own, q_s[at, lanes][None], jnp.zeros((), BF16)).reshape(512, 256)
            scores = dot(queries, k_s[at, lanes], NT)
            scores = scores + bias_s[64 * g : 64 * g + 64].reshape(512, 64)
            if w_row == 1:
                scores = scores + last_s[...]
            scores = scores - jnp.max(scores, axis=-1, keepdims=True)
            weights = jnp.exp(scores)
            weights = (weights / jnp.sum(weights, axis=-1, keepdims=True)).astype(BF16)
            found = dot(weights, v_s[at, lanes], NN).reshape(8, 64, 256)
            att_s[at, lanes] = jnp.sum(jnp.where(own, found, 0.0), axis=0).astype(BF16)
        return carry

    lax.fori_loop(0, 3, window, 0)
    projected = dot(att_s[...], wo_s[...], NN).astype(BF16).astype(F32)
    norm_s[3 * w_row : 3 * w_row + 3] = projected.reshape(3, 8, 8, 512)


def finish(g, norm_s, mixed_s, cyc_ref, side_ref):
    w_row, w_start = WINDOW_OF[g]
    turned = [turn(norm_s[w_row * 3 + b, w_start : w_start + 4]) for b in range(3)]
    low = low_half((4, 8, 512))
    back = jnp.concatenate([jnp.where(low, turned[b - 1], turned[b]) for b in range(3)], axis=1)
    rows = slice(4 * g, 4 * g + 4)
    result = (mixed_s[rows] + back).astype(BF16)
    mixed_s[rows] = result.astype(F32)
    cyc_ref[rows] = result
    side_ref[...] = pack(result.astype(F32)[:, 0:8], False).reshape(16, 512).astype(BF16)


def convolve(pad_s, kernel_ref, cbias_ref, conv_ref):
    def band(i, carry):
        start = i * 8
        for h in range(2):
            lanes = slice(128 * h, 128 * h + 128)
            first_term = jnp.broadcast_to(cbias_ref[:, lanes], (8, 128))
            for b in range(4):
                sums = [first_term] * 8
                for v in range(7):
                    col = 8 * b + v + 5
                    cells = [pad_s[h, start + r, col : col + 8, :] for r in range(14)]
                    for u in range(7):
                        tap = kernel_ref[u, v : v + 1, lanes]
                        for r in range(8):
                            sums[r] = sums[r] + tap * cells[r + u]
                for r in range(8):
                    conv_ref[start + r, 8 * b : 8 * b + 8, lanes] = sums[r]
        return carry

    lax.fori_loop(0, 2, band, 0)


OPERANDS = (
    ("ocean", (16, 32, 256), BF16), ("proj", (4, 256), F32), ("mask", (16, 32), jnp.int32), ("overlay", (3, 64, 512), BF16),
    ("owner", (1, 3), jnp.int32), ("block", (1, 3), jnp.int32), ("count", (1, 1), jnp.int32), ("tok", (16, 24, 512), BF16),
    ("grid", (16, 225), F32), ("enc", (4, 512), F32), ("gain", (1, 512), F32), ("wqkv", (512, 1536), BF16),
    ("bqkv", (1536,), F32), ("wo", (512, 512), BF16), ("fp", (16, 512), BF16), ("kernel", (7, 7, 256), F32),
    ("cbias", (1, 256), F32), ("fenc", (16, 256), F32), ("ogain", (1, 256), F32), ("w1", (256, 1024), BF16),
    ("w2", (1024, 256), BF16), ("scale", (1, 256), F32),
)
SCALARS = ("owner", "block", "count")
SCRATCH = (
    ("proj8", (8, 256), F32), ("enc8", (8, 512), F32), ("msg", (16, 128), F32), ("msgs", (4, 16, 128), F32),
    ("side", (64, 512), BF16), ("east", (64, 512), BF16), ("south", (4, 24, 512), BF16), ("corner", (16, 512), BF16),
    ("sst", (8, 128), F32), ("under", (8, 128), F32), ("table", (16, 8, 128), F32), ("bias", (128, 8, 64), F32),
    ("last", (512, 64), F32), ("mixed", (16, 24, 512), F32), ("norm", (6, 8, 8, 512), F32), ("q", (192, 512), BF16),
    ("k", (192, 512), BF16), ("v", (192, 512), BF16), ("att", (192, 512), BF16), ("above", (3, 32, 256), BF16),
    ("below", (3, 32, 256), BF16), ("leave", (2, 88, 256), BF16), ("cols", (2, 88, 256), BF16),
    ("pad", (2, 22, 48, 128), F32), ("pe", (64, 512), BF16), ("flux", (16, 384), BF16), ("cyc", (16, 24, 512), BF16),
    ("fluxes", (8, 16, 384), BF16), ("west", (64, 512), BF16), ("north", (4, 24, 512), BF16), ("nw", (16, 512), BF16),
    ("conv", (16, 32, 256), F32), ("pre", (512, 256), F32), ("rate", (512, 256), F32), ("atm", (16, 24, 512), BF16),
    ("out", (16, 32, 256), BF16),
)


def pick_flux(x, codes):
    lane = iota((16, 128), 1)
    right = lane >= 64
    picked = [jnp.zeros((16, 128), F32)] * 3
    for j in range(3):
        patch = lane + 128 * j
        east = column_of(patch) < 4
        south = patch < 96
        at = slice(128 * j, 128 * j + 128)
        for side in range(3):
            here = jnp.where(east, x.fluxes[side, :, at].astype(F32), x.fluxes[side + 1, :, at].astype(F32))
            under = jnp.where(east, x.fluxes[4 + side, :, at].astype(F32), x.fluxes[5 + side, :, at].astype(F32))
            tile = jnp.where(south, under, here)
            target = jnp.where(right, side * 8 + 2 * j + 1, side * 8 + 2 * j)
            for k in range(3):
                picked[k] += jnp.where(target == codes[k], tile, 0.0)
    picked = [y + pltpu.roll(y, 64, 1) for y in picked]
    return jnp.concatenate([jnp.where(right, picked[1], picked[0]), picked[2][:, 0:64]], axis=1)


def slot_codes(x):
    lo = lax.axis_index("lon")
    nlo = lax.axis_size("lon")
    codes = []
    for k in range(3):
        side = lax.rem(x.owner[0, k] - lo + 1 + nlo, nlo)
        codes.append(jnp.where(k < x.count[0, 0], side * 8 + x.block[0, k], -1))
    return codes


def ocean_rate(x):
    mask = jnp.broadcast_to(mask_row(x.mask[...]), (16, 512)).astype(BF16)
    parts = [jnp.broadcast_to(y, (16, 256)) for y in split3(x.scale[...])]
    row = iota((16, 256), 0)
    scale = jnp.where(row == 0, parts[0], jnp.where(row == 1, parts[1], jnp.where(row == 2, parts[2], 0.0)))
    x.rate[...] = dot(mask, scale.astype(BF16), TN)


def ocean_update(x):
    forcing = dot(pick_flux(x, slot_codes(x)).astype(BF16), x.overlay[...].reshape(192, 512), NN)
    f_hi, f_lo = split2(forcing)
    e_hi, e_lo = split2(x.fenc[...])
    x.pre[...] = x.conv[...].reshape(512, 256) + dot(
        jnp.concatenate([f_hi, f_lo, f_hi], axis=0).astype(BF16),
        jnp.concatenate([e_hi, e_hi, e_lo], axis=0).astype(BF16),
        TN,
    )

    def cells(i, carry):
        at = pl.ds(pl.multiple_of(i * 128, 128), 128)
        normed = layer_norm(x.pre[at], x.ogain[...], 1e-06).astype(BF16)
        update = jnp.zeros((128, 256), F32)
        for c in range(4):
            cols = slice(256 * c, 256 * c + 256)
            y = dot(normed, x.w1[:, cols], NN)
            hidden = (0.5 * y * (1.0 + lax.erf(y * (0.5**0.5)))).astype(BF16)
            update = update + dot(hidden, x.w2[cols], NN)
        rows = pl.ds(i * 4, 4)
        state = x.ocean[rows].astype(F32).reshape(128, 256)
        x.out[rows] = (state + x.rate[at] * update).astype(BF16).reshape(4, 32, 256)
        return carry

    lax.fori_loop(0, 4, cells, 0)


def assemble(g, x):
    low = low_half((4, 8, 512))
    rows = slice(4 * g, 4 * g + 4)
    body, side = (x.north, x.nw[...]) if g == 0 else (x.cyc.at[rows], x.west[16 * g : 16 * g + 16])
    body = body[...].astype(F32)
    side = unpack(side.astype(F32).reshape(2, 8, 512), False)
    head = jnp.where(low, side, body[:, 0:8])
    x.atm[rows] = jnp.concatenate([head, body[:, 8:24]], axis=1).astype(BF16)


def step_kernel(*refs):
    n = len(OPERANDS)
    given = dict(zip([o[0] for o in OPERANDS], refs[:n]))
    atm_ref, out_ref = refs[n : n + 2]
    refs = refs[n + 2 :]
    x = types.SimpleNamespace(**dict(zip([o[0] for o in (*OPERANDS, *SCRATCH)], refs)))
    load_sem, store_sem, send_sem, recv_sem = refs[n + len(SCRATCH) :]

    at = place()
    la = lax.axis_index("lat")
    nla = lax.axis_size("lat")
    wait_barrier = greet([at(*o) for o in PARTNERS])
    loads = {}
    for i, (name, *_) in enumerate(OPERANDS):
        loads[name] = pltpu.make_async_copy(given[name], getattr(x, name), load_sem.at[i])
        loads[name].start()

    def loaded(*names):
        for name in names:
            loads[name].wait()

    copies = []

    def send(src, dst, offset):
        i = len(copies)
        copy = pltpu.make_async_remote_copy(
            src_ref=src, dst_ref=dst, send_sem=send_sem.at[i], recv_sem=recv_sem.at[i],
            device_id=at(*offset), device_id_type=MESH,
        )
        copies.append(copy)
        copy.start()
        return copy

    loaded("ocean", "proj", "mask", "overlay", "owner", "block", "count")
    for half in range(2):
        x.proj8[4 * half : 4 * half + 4] = x.proj[...]
    surface_message(x.owner, x.block, x.count, x.ocean, x.mask, x.overlay, x.proj8, x.msg)
    loaded("tok")
    x.side[...] = pack(x.tok[:, 0:8, :].astype(F32), False).reshape(64, 512).astype(BF16)

    wait_barrier()
    messages = [send(x.msg, x.msgs.at[dj + 1], (0, -dj)) for dj in (2, 1, -1)]
    x.msgs[1] = x.msg[...]
    east_top = send(x.side.at[pl.ds(0, 16)], x.east.at[pl.ds(0, 16)], (0, -1))
    east = send(x.side.at[pl.ds(16, 48)], x.east.at[pl.ds(16, 48)], (0, -1))
    south = send(x.tok.at[pl.ds(0, 4)], x.south, (-1, 0))

    loaded("grid", "enc", "gain")
    for half in range(2):
        x.enc8[4 * half : 4 * half + 4] = x.enc[...]
    bias_table(x.grid, x.table, x.bias)
    edge = la == nla - 1
    a_row = (iota((512, 64), 0) % 64) >= 32
    b_row = iota((512, 64), 1) >= 32
    x.last[...] = jnp.where(edge, jnp.where(a_row != b_row, -1e9, 0.0), 0.0)

    for copy in messages:
        copy.wait_recv()
    sst = gather_surface(x.msgs)
    x.sst[...] = sst[0]
    under = send(x.sst, x.under, (-1, 0))
    east_top.wait_recv()
    corner = send(x.east.at[pl.ds(0, 16)], x.corner, (-1, 0))
    below = send(x.ocean.at[pl.ds(0, 3)], x.below, (-1, 0))
    above = send(x.ocean.at[pl.ds(13, 3)], x.above, (1, 0))
    x.mixed[...] = add_surface(jnp.concatenate(sst, axis=1), x.enc8).reshape(16, 24, 512)
    gain = x.gain[...].reshape(1, 1, 512)
    east.wait_recv()
    for g in (1, 2, 3):
        normalise(g, x.tok[4 * g : 4 * g + 4], x.east[16 * g : 16 * g + 16], gain, x.mixed, x.norm)
    loaded("wqkv", "bqkv", "wo")
    windows = (x.norm, x.wqkv, x.bqkv, x.wo, x.bias, x.last, x.q, x.k, x.v, x.att)
    attend(0, *windows)
    for g in (1, 2):
        finish(g, x.norm, x.mixed, x.cyc, x.pe.at[pl.ds(16 * g, 16)])
    pieces = [send(x.pe.at[pl.ds(16, 32)], x.west.at[pl.ds(16, 32)], (0, 1))]

    def put(rows, cols, values):
        for h in range(2):
            x.pad[h, rows, cols, :] = values[:, :, 128 * h : 128 * h + 128]

    below.wait_recv()
    above.wait_recv()
    put(slice(3, 19), slice(8, 40), x.ocean[...].astype(F32))
    put(slice(0, 3), slice(8, 40), x.above[...].astype(F32) * (la > 0).astype(F32))
    put(slice(19, 22), slice(8, 40), x.below[...].astype(F32) * (la < nla - 1).astype(F32))
    for h in range(2):
        lanes = slice(128 * h, 128 * h + 128)
        x.leave[0, :, lanes] = pack(x.pad[h, :, 32:40, :], True).reshape(88, 128).astype(BF16)
        x.leave[1, :, lanes] = pack(x.pad[h, :, 8:16, :], False).reshape(88, 128).astype(BF16)
    sides = [send(x.leave.at[0], x.cols.at[0], (0, 1)), send(x.leave.at[1], x.cols.at[1], (0, -1))]
    loaded("scale")
    ocean_rate(x)

    for copy in (under, south, corner):
        copy.wait_recv()
    x.mixed[0:4] = add_surface(x.under[...], x.enc8)[0:96].reshape(4, 24, 512)
    normalise(0, x.south[...], x.corner[...], gain, x.mixed, x.norm)
    attend(1, *windows)
    for g in (3, 0):
        finish(g, x.norm, x.mixed, x.cyc, x.pe.at[pl.ds(16 * g, 16)])
    loaded("fp")
    x.flux[...] = dot(x.fp[...], x.mixed[...].reshape(384, 512).astype(BF16), NT).astype(BF16)
    fluxes = [
        send(x.flux, x.fluxes.at[down * 4 + dj + 2], (down, -dj))
        for down in (1, 0) for dj in (1, -2, -1, 0) if (down, dj) != (0, 0)
    ]
    pieces += [
        send(x.pe.at[pl.ds(48, 16)], x.west.at[pl.ds(48, 16)], (0, 1)),
        send(x.pe.at[pl.ds(0, 16)], x.nw, (1, 1)),
        send(x.cyc.at[pl.ds(0, 4)], x.north, (1, 0)),
    ]
    x.fluxes[2] = x.flux[...]

    for copy in sides:
        copy.wait_recv()
    for side, high in ((0, True), (1, False)):
        values = unpack(x.cols[side].astype(F32).reshape(11, 8, 256), high)
        put(slice(0, 22), slice(40 * side, 40 * side + 8), values)
    loaded("kernel", "cbias")
    convolve(x.pad, x.kernel, x.cbias, x.conv)

    loaded("fenc", "ogain", "w1", "w2")
    for copy in fluxes:
        copy.wait_recv()
    ocean_update(x)
    stores = [pltpu.make_async_copy(x.out, out_ref, store_sem.at[0])]
    stores[0].start()
    for copy in pieces:
        copy.wait_recv()
    for g in range(4):
        assemble(g, x)
    stores.append(pltpu.make_async_copy(x.atm, atm_ref, store_sem.at[1]))
    stores[1].start()
    for copy in copies:
        copy.wait_send()
    for copy in stores:
        copy.wait()


def step(*operands):
    def copy_of(name, shape, kind):
        return pltpu.SMEM(shape, kind) if name in SCALARS else pltpu.VMEM(shape, kind)

    shapes = [((16, 24, 512), BF16), ((16, 32, 256), BF16)]
    return pl.pallas_call(
        step_kernel,
        out_shape=[jax.ShapeDtypeStruct(*s) for s in shapes],
        in_specs=anywhere(len(OPERANDS)),
        out_specs=anywhere(len(shapes)),
        scratch_shapes=[
            *[copy_of(*o) for o in (*OPERANDS, *SCRATCH)],
            pltpu.SemaphoreType.DMA((len(OPERANDS),)), pltpu.SemaphoreType.DMA((2,)),
            pltpu.SemaphoreType.DMA((COPIES,)), pltpu.SemaphoreType.DMA((COPIES,)),
        ],
        compiler_params=pltpu.CompilerParams(collective_id=0, has_side_effects=True),
        name="step",
    )(*operands)


def local(
    atmos_patch_tokens,
    atmos_norm_gain,
    query_key_value_weight,
    query_key_value_bias,
    relative_bias_grid,
    attention_output_weight,
    flux_projector,
    surface_encoder,
    ocean_cell_state,
    land_sea_mask,
    depthwise_conv_kernel,
    depthwise_conv_bias,
    ocean_norm_gain,
    pointwise_expand,
    pointwise_contract,
    layer_update_scale,
    forcing_encoder,
    surface_projector,
    overlay_area_weight,
    owners,
    owner_tile_blocks,
    counts,
):
    owners = owners.reshape(1, 3)
    blocks = owner_tile_blocks.reshape(1, 3)
    overlay = overlay_area_weight.reshape(3, 64, 512)
    atm_out, ocean_out = step(
        ocean_cell_state, surface_projector.T, land_sea_mask, overlay, owners, blocks, counts, atmos_patch_tokens,
        relative_bias_grid, surface_encoder, atmos_norm_gain.reshape(1, 512), query_key_value_weight, query_key_value_bias,
        attention_output_weight, flux_projector.T, depthwise_conv_kernel, depthwise_conv_bias.reshape(1, 256), forcing_encoder,
        ocean_norm_gain.reshape(1, 256), pointwise_expand, pointwise_contract, layer_update_scale.reshape(1, 256),
    )
    return atm_out, ocean_out


def solution(mesh):
    rep = P()
    placed = (
        P("lat", "lon", None), rep, rep, rep, rep, rep, rep, rep, P("lat", "lon", None), P("lat", "lon"),
        rep, rep, rep, rep, rep, rep, rep, rep, P("lat", "lon", None, None, None),
        P("lat", "lon", None), P("lat", "lon", None), P("lat", "lon"),
    )
    return jax.shard_map(
        local,
        mesh=mesh,
        in_specs=placed,
        out_specs=(P("lat", "lon", None), P("lat", "lon", None)),
        check_vma=False,
    )
```

```python
import types

import jax
import jax.numpy as jnp
from jax import lax
from jax.experimental import pallas as pl
from jax.experimental.pallas import tpu as pltpu
from jax.sharding import PartitionSpec as P

F32 = jnp.float32
BF16 = jnp.bfloat16
MESH = pl.DeviceIdType.MESH
HEADS = 16
HALF = 8
WIN = 8
NT = (((1,), (1,)), ((), ()))
TN = (((0,), (0,)), ((), ()))
NN = (((1,), (0,)), ((), ()))


def dot(a, b, dims):
    return lax.dot_general(a, b, dims, preferred_element_type=F32)


def iota(shape, dim):
    return lax.broadcasted_iota(jnp.int32, shape, dim)


def low_half(shape):
    return iota(shape, len(shape) - 2) % 8 < 4


def turn(x):
    return pltpu.roll(x, 4, x.ndim - 2)


def pack(x, high):
    n, _, lanes = x.shape
    x = x.reshape(n // 2, 2, 8, lanes)
    even, odd = x[:, 0], x[:, 1]
    if high:
        even = turn(even)
    else:
        odd = turn(odd)
    return jnp.where(low_half(even.shape), even, odd)


def unpack(x, high):
    n, _, lanes = x.shape
    other = turn(x)
    pair = (other, x) if high else (x, other)
    return jnp.stack(pair, axis=1).reshape(2 * n, 8, lanes)


def split2(x):
    top = x.astype(BF16).astype(F32)
    return top, x - top


def split3(x):
    top, rest = split2(x)
    middle, last = split2(rest)
    return top, middle, last


def greet(partners):
    barrier = pltpu.get_barrier_semaphore()
    for device in partners:
        pl.semaphore_signal(barrier, inc=1, device_id=device, device_id_type=MESH)
    return lambda: pl.semaphore_wait(barrier, len(partners))


def place():
    la, lo = lax.axis_index("lat"), lax.axis_index("lon")
    nla, nlo = lax.axis_size("lat"), lax.axis_size("lon")
    return lambda di, dj: (lax.rem(la + di + nla, nla), lax.rem(lo + dj + nlo, nlo))


def vmem(n):
    return [pl.BlockSpec(memory_space=pltpu.VMEM)] * n


def smem(n):
    return [pl.BlockSpec(memory_space=pltpu.SMEM)] * n


def anywhere(n):
    return [pl.BlockSpec(memory_space=pl.ANY)] * n


def layer_norm(x, gain, epsilon):
    average = jnp.mean(x, axis=-1, keepdims=True)
    centred = x - average
    spread = jnp.mean(centred * centred, axis=-1, keepdims=True)
    return centred * lax.rsqrt(spread + epsilon) * gain


def column_of(patch):
    p = patch.astype(F32)
    return p - 24.0 * jnp.floor((p + 0.5) * (1.0 / 24.0))


def mask_row(mask):
    wide = jnp.concatenate([mask.astype(F32), jnp.zeros((16, 96), F32)], axis=1)
    moved = [wide if q == 0 else pltpu.roll(wide, 32 * q, 1) for q in range(4)]
    parts = [sum(moved[q][4 * j + q : 4 * j + q + 1] for q in range(4)) for j in range(4)]
    return jnp.concatenate(parts, axis=1)


PARTNERS = [(0, 1), (0, -1), (0, 2), (0, -2), (1, 0), (-1, 0)]
COPIES = 32


def surface_message(owner_ref, block_ref, count_ref, ocean_ref, mask_ref, overlay_ref, proj_s, msg_s):
    lo = lax.axis_index("lon")
    nlo = lax.axis_size("lon")
    parts = jnp.concatenate(split3(proj_s[...]), axis=0).astype(BF16)
    surf = dot(parts, ocean_ref[...].reshape(512, 256), NT)
    surf = ((surf[0:8] + surf[8:16] + surf[16:24]) * mask_row(mask_ref[...])).astype(BF16)
    row = iota((8, 128), 0)
    twice = []
    codes = jnp.full((8, 128), -1.0, F32)
    for k in range(3):
        block = overlay_ref[k]
        twice.append(dot(surf, jnp.concatenate([block, block], axis=0), NT))
        side = lax.rem(owner_ref[0, k] - lo + 1 + nlo, nlo)
        code = jnp.where(k < count_ref[0, 0], side * 8 + block_ref[0, k], -1).astype(F32)
        codes = jnp.where(row == 4 + k, code, codes)
    msg_s[0:8] = jnp.where(row < 4, twice[0], twice[1])
    msg_s[8:16] = jnp.where(row < 4, twice[2], codes)


def gather_surface(msgs_ref):
    upper = iota((8, 128), 0) < 4
    right = iota((8, 128), 1) >= 64
    tiles = []
    for tile in range(2):
        sums = [jnp.zeros((8, 128), F32)] * 3
        for side in range(3):
            slot = tile - side + 2
            a = msgs_ref[slot, 0:8, :]
            b = msgs_ref[slot, 8:16, :]
            code_a = jnp.where(upper, b[4:5], b[5:6])
            code_b = jnp.where(upper, b[6:7], -1.0)
            for j in range(3):
                target = jnp.where(right, side * 8.0 + 2 * j + 1, side * 8.0 + 2 * j)
                sums[j] += jnp.where(code_a == target, a, 0.0) + jnp.where(code_b == target, b, 0.0)
        tiles.append(sums)
    return [
        jnp.where(column_of(iota((8, 128), 1) + 128 * j) < 4, tiles[1][j], tiles[0][j]) for j in range(3)
    ]


def bias_table(grid_ref, table_s, bias_s):
    grid = jnp.concatenate([grid_ref[...], jnp.zeros((16, 31), F32)], axis=1)
    for ra in range(8):
        rolled = grid if ra == 0 else pltpu.roll(grid, 256 - 15 * ra, 1)
        table_s[:, ra, :] = rolled[:, 0:128]
    parts = [x.astype(BF16) for x in split3(table_s[...].reshape(128, 128))]
    entry = iota((128, 64), 0)
    lane = iota((128, 64), 1)
    for ca in range(8):
        chosen = (entry == (7 - lane // 8) * 15 + ca - lane % 8 + 7).astype(BF16)
        found = (dot(parts[0], chosen, NN) + dot(parts[1], chosen, NN)) + dot(parts[2], chosen, NN)
        bias_s[:, ca, :] = found


def add_surface(sst, enc_s):
    s_hi, s_lo = split2(sst)
    e_hi, e_lo = split2(enc_s[...])
    left = jnp.concatenate([s_hi, s_lo, s_hi], axis=0).astype(BF16)
    right = jnp.concatenate([e_hi, e_hi, e_lo], axis=0).astype(BF16)
    return dot(left, right, TN)


def normalise(g, tokens, side, gain, mixed_s, norm_s):
    low = low_half((4, 8, 512))
    rows = slice(4 * g, 4 * g + 4)
    tokens = tokens.astype(F32)
    side = unpack(side.astype(F32).reshape(2, 8, 512), False)
    head = jnp.where(low, side, tokens[:, 0:8])
    tokens = jnp.concatenate([head, tokens[:, 8:24]], axis=1)
    mixed = (tokens + mixed_s[rows]).astype(BF16).astype(F32)
    mixed_s[rows] = mixed
    normed = layer_norm(mixed, gain, 1e-05)
    turned = [turn(normed[:, 8 * b : 8 * b + 8]) for b in range(3)]
    w_row, w_start = WINDOW_OF[g]
    for b in range(3):
        norm_s[w_row * 3 + b, w_start : w_start + 4] = jnp.where(low, turned[b], turned[(b + 1) % 3])


WINDOW_OF = ((1, 4), (0, 0), (0, 4), (1, 0))


def attend(w_row, norm_s, wqkv_s, bqkv_ref, wo_s, bias_s, last_s, q_s, k_s, v_s, att_s):
    rows = norm_s[3 * w_row : 3 * w_row + 3].reshape(192, 512).astype(BF16)
    for part, ref in enumerate((q_s, k_s, v_s)):
        cols = slice(512 * part, 512 * part + 512)
        value = dot(rows, wqkv_s[:, cols], NN) + bqkv_ref[cols].reshape(1, 512)
        if part == 0:
            value = value * 32 ** (-0.5)
        ref[...] = value.astype(BF16)
    own = (iota((8, 1, 256), 2) // 32) == iota((8, 1, 256), 0)

    def window(w, carry):
        at = pl.ds(pl.multiple_of(w * 64, 64), 64)
        for g in range(2):
            lanes = slice(256 * g, 256 * g + 256)
            queries = jnp.where(own, q_s[at, lanes][None], jnp.zeros((), BF16)).reshape(512, 256)
            scores = dot(queries, k_s[at, lanes], NT)
            scores = scores + bias_s[64 * g : 64 * g + 64].reshape(512, 64)
            if w_row == 1:
                scores = scores + last_s[...]
            scores = scores - jnp.max(scores, axis=-1, keepdims=True)
            weights = jnp.exp(scores)
            weights = (weights / jnp.sum(weights, axis=-1, keepdims=True)).astype(BF16)
            found = dot(weights, v_s[at, lanes], NN).reshape(8, 64, 256)
            att_s[at, lanes] = jnp.sum(jnp.where(own, found, 0.0), axis=0).astype(BF16)
        return carry

    lax.fori_loop(0, 3, window, 0)
    projected = dot(att_s[...], wo_s[...], NN).astype(BF16).astype(F32)
    norm_s[3 * w_row : 3 * w_row + 3] = projected.reshape(3, 8, 8, 512)


def finish(g, norm_s, mixed_s, cyc_ref, side_ref):
    w_row, w_start = WINDOW_OF[g]
    turned = [turn(norm_s[w_row * 3 + b, w_start : w_start + 4]) for b in range(3)]
    low = low_half((4, 8, 512))
    back = jnp.concatenate([jnp.where(low, turned[b - 1], turned[b]) for b in range(3)], axis=1)
    rows = slice(4 * g, 4 * g + 4)
    result = (mixed_s[rows] + back).astype(BF16)
    mixed_s[rows] = result.astype(F32)
    cyc_ref[rows] = result
    side_ref[...] = pack(result.astype(F32)[:, 0:8], False).reshape(16, 512).astype(BF16)


def convolve(pad_s, kernel_ref, cbias_ref, conv_ref):
    def band(i, carry):
        start = i * 8
        for h in range(2):
            lanes = slice(128 * h, 128 * h + 128)
            first_term = jnp.broadcast_to(cbias_ref[:, lanes], (8, 128))
            for b in range(4):
                sums = [first_term] * 8
                for v in range(7):
                    col = 8 * b + v + 5
                    cells = [pad_s[h, start + r, col : col + 8, :] for r in range(14)]
                    for u in range(7):
                        tap = kernel_ref[u, v : v + 1, lanes]
                        for r in range(8):
                            sums[r] = sums[r] + tap * cells[r + u]
                for r in range(8):
                    conv_ref[start + r, 8 * b : 8 * b + 8, lanes] = sums[r]
        return carry

    lax.fori_loop(0, 2, band, 0)


OPERANDS = (
    ("ocean", (16, 32, 256), BF16), ("proj", (4, 256), F32), ("mask", (16, 32), jnp.int32), ("overlay", (3, 64, 512), BF16),
    ("owner", (1, 3), jnp.int32), ("block", (1, 3), jnp.int32), ("count", (1, 1), jnp.int32), ("tok", (16, 24, 512), BF16),
    ("grid", (16, 225), F32), ("enc", (4, 512), F32), ("gain", (1, 512), F32), ("wqkv", (512, 1536), BF16),
    ("bqkv", (1536,), F32), ("wo", (512, 512), BF16), ("fp", (16, 512), BF16), ("kernel", (7, 7, 256), F32),
    ("cbias", (1, 256), F32), ("fenc", (16, 256), F32), ("ogain", (1, 256), F32), ("w1", (256, 1024), BF16),
    ("w2", (1024, 256), BF16), ("scale", (1, 256), F32),
)
SCALARS = ("owner", "block", "count")
SCRATCH = (
    ("proj8", (8, 256), F32), ("enc8", (8, 512), F32), ("msg", (16, 128), F32), ("msgs", (4, 16, 128), F32),
    ("side", (64, 512), BF16), ("east", (64, 512), BF16), ("south", (4, 24, 512), BF16), ("corner", (16, 512), BF16),
    ("sst", (8, 128), F32), ("under", (8, 128), F32), ("table", (16, 8, 128), F32), ("bias", (128, 8, 64), F32),
    ("last", (512, 64), F32), ("mixed", (16, 24, 512), F32), ("norm", (6, 8, 8, 512), F32), ("q", (192, 512), BF16),
    ("k", (192, 512), BF16), ("v", (192, 512), BF16), ("att", (192, 512), BF16), ("above", (3, 32, 256), BF16),
    ("below", (3, 32, 256), BF16), ("leave", (2, 88, 256), BF16), ("cols", (2, 88, 256), BF16),
    ("pad", (2, 22, 48, 128), F32), ("pe", (64, 512), BF16), ("flux", (16, 384), BF16),
    ("fluxes", (8, 16, 384), BF16), ("conv", (16, 32, 256), F32), ("pre", (512, 256), F32), ("rate", (512, 256), F32),
)
RESULTS = (
    ("cyc", (16, 24, 512), BF16), ("west", (64, 512), BF16), ("north", (4, 24, 512), BF16), ("nw", (16, 512), BF16),
    ("out", (16, 32, 256), BF16),
)


def pick_flux(x, codes):
    lane = iota((16, 128), 1)
    right = lane >= 64
    picked = [jnp.zeros((16, 128), F32)] * 3
    for j in range(3):
        patch = lane + 128 * j
        east = column_of(patch) < 4
        south = patch < 96
        at = slice(128 * j, 128 * j + 128)
        for side in range(3):
            here = jnp.where(east, x.fluxes[side, :, at].astype(F32), x.fluxes[side + 1, :, at].astype(F32))
            under = jnp.where(east, x.fluxes[4 + side, :, at].astype(F32), x.fluxes[5 + side, :, at].astype(F32))
            tile = jnp.where(south, under, here)
            target = jnp.where(right, side * 8 + 2 * j + 1, side * 8 + 2 * j)
            for k in range(3):
                picked[k] += jnp.where(target == codes[k], tile, 0.0)
    picked = [y + pltpu.roll(y, 64, 1) for y in picked]
    return jnp.concatenate([jnp.where(right, picked[1], picked[0]), picked[2][:, 0:64]], axis=1)


def slot_codes(x):
    lo = lax.axis_index("lon")
    nlo = lax.axis_size("lon")
    codes = []
    for k in range(3):
        side = lax.rem(x.owner[0, k] - lo + 1 + nlo, nlo)
        codes.append(jnp.where(k < x.count[0, 0], side * 8 + x.block[0, k], -1))
    return codes


def ocean_rate(x):
    mask = jnp.broadcast_to(mask_row(x.mask[...]), (16, 512)).astype(BF16)
    parts = [jnp.broadcast_to(y, (16, 256)) for y in split3(x.scale[...])]
    row = iota((16, 256), 0)
    scale = jnp.where(row == 0, parts[0], jnp.where(row == 1, parts[1], jnp.where(row == 2, parts[2], 0.0)))
    x.rate[...] = dot(mask, scale.astype(BF16), TN)


def ocean_update(x):
    forcing = dot(pick_flux(x, slot_codes(x)).astype(BF16), x.overlay[...].reshape(192, 512), NN)
    f_hi, f_lo = split2(forcing)
    e_hi, e_lo = split2(x.fenc[...])
    x.pre[...] = x.conv[...].reshape(512, 256) + dot(
        jnp.concatenate([f_hi, f_lo, f_hi], axis=0).astype(BF16),
        jnp.concatenate([e_hi, e_hi, e_lo], axis=0).astype(BF16),
        TN,
    )

    def cells(i, carry):
        at = pl.ds(pl.multiple_of(i * 128, 128), 128)
        normed = layer_norm(x.pre[at], x.ogain[...], 1e-06).astype(BF16)
        update = jnp.zeros((128, 256), F32)
        for c in range(4):
            cols = slice(256 * c, 256 * c + 256)
            y = dot(normed, x.w1[:, cols], NN)
            hidden = (0.5 * y * (1.0 + lax.erf(y * (0.5**0.5)))).astype(BF16)
            update = update + dot(hidden, x.w2[cols], NN)
        rows = pl.ds(i * 4, 4)
        state = x.ocean[rows].astype(F32).reshape(128, 256)
        x.out[rows] = (state + x.rate[at] * update).astype(BF16).reshape(4, 32, 256)
        return carry

    lax.fori_loop(0, 4, cells, 0)


def assemble(g, x):
    low = low_half((4, 8, 512))
    rows = slice(4 * g, 4 * g + 4)
    body, side = (x.north, x.nw[...]) if g == 0 else (x.cyc.at[rows], x.west[16 * g : 16 * g + 16])
    body = body[...].astype(F32)
    side = unpack(side.astype(F32).reshape(2, 8, 512), False)
    head = jnp.where(low, side, body[:, 0:8])
    x.atm[rows] = jnp.concatenate([head, body[:, 8:24]], axis=1).astype(BF16)


def step_kernel(*refs):
    n = len(OPERANDS)
    given = dict(zip([o[0] for o in OPERANDS], refs[:n]))
    names = [o[0] for o in (*RESULTS, *OPERANDS, *SCRATCH)]
    x = types.SimpleNamespace(**dict(zip(names, refs[n:])))
    load_sem, send_sem, recv_sem = refs[n + len(names) :]

    at = place()
    la = lax.axis_index("lat")
    nla = lax.axis_size("lat")
    wait_barrier = greet([at(*o) for o in PARTNERS])
    loads = {}
    for i, (name, *_) in enumerate(OPERANDS):
        loads[name] = pltpu.make_async_copy(given[name], getattr(x, name), load_sem.at[i])
        loads[name].start()

    def loaded(*names):
        for name in names:
            loads[name].wait()

    copies = []

    def send(src, dst, offset):
        i = len(copies)
        copy = pltpu.make_async_remote_copy(
            src_ref=src, dst_ref=dst, send_sem=send_sem.at[i], recv_sem=recv_sem.at[i],
            device_id=at(*offset), device_id_type=MESH,
        )
        copies.append(copy)
        copy.start()
        return copy

    loaded("ocean", "proj", "mask", "overlay", "owner", "block", "count")
    for half in range(2):
        x.proj8[4 * half : 4 * half + 4] = x.proj[...]
    surface_message(x.owner, x.block, x.count, x.ocean, x.mask, x.overlay, x.proj8, x.msg)
    loaded("tok")
    x.side[...] = pack(x.tok[:, 0:8, :].astype(F32), False).reshape(64, 512).astype(BF16)

    with jax.named_scope("w_barrier"):
        wait_barrier()
    messages = [send(x.msg, x.msgs.at[dj + 1], (0, -dj)) for dj in (2, 1, -1)]
    x.msgs[1] = x.msg[...]
    east_top = send(x.side.at[pl.ds(0, 16)], x.east.at[pl.ds(0, 16)], (0, -1))
    east = send(x.side.at[pl.ds(16, 48)], x.east.at[pl.ds(16, 48)], (0, -1))
    south = send(x.tok.at[pl.ds(0, 4)], x.south, (-1, 0))

    loaded("grid", "enc", "gain")
    for half in range(2):
        x.enc8[4 * half : 4 * half + 4] = x.enc[...]
    bias_table(x.grid, x.table, x.bias)
    edge = la == nla - 1
    a_row = (iota((512, 64), 0) % 64) >= 32
    b_row = iota((512, 64), 1) >= 32
    x.last[...] = jnp.where(edge, jnp.where(a_row != b_row, -1e9, 0.0), 0.0)

    with jax.named_scope("w_messages"):
        for copy in messages:
            copy.wait_recv()
    sst = gather_surface(x.msgs)
    x.sst[...] = sst[0]
    under = send(x.sst, x.under, (-1, 0))
    with jax.named_scope("w_top"):
        east_top.wait_recv()
    corner = send(x.east.at[pl.ds(0, 16)], x.corner, (-1, 0))
    below = send(x.ocean.at[pl.ds(0, 3)], x.below, (-1, 0))
    above = send(x.ocean.at[pl.ds(13, 3)], x.above, (1, 0))
    x.mixed[...] = add_surface(jnp.concatenate(sst, axis=1), x.enc8).reshape(16, 24, 512)
    gain = x.gain[...].reshape(1, 1, 512)
    with jax.named_scope("w_east"):
        east.wait_recv()
    for g in (1, 2, 3):
        normalise(g, x.tok[4 * g : 4 * g + 4], x.east[16 * g : 16 * g + 16], gain, x.mixed, x.norm)
    loaded("wqkv", "bqkv", "wo")
    windows = (x.norm, x.wqkv, x.bqkv, x.wo, x.bias, x.last, x.q, x.k, x.v, x.att)
    attend(0, *windows)
    for g in (1, 2):
        finish(g, x.norm, x.mixed, x.cyc, x.pe.at[pl.ds(16 * g, 16)])
    pieces = [send(x.pe.at[pl.ds(16, 32)], x.west.at[pl.ds(16, 32)], (0, 1))]

    def put(rows, cols, values):
        for h in range(2):
            x.pad[h, rows, cols, :] = values[:, :, 128 * h : 128 * h + 128]

    with jax.named_scope("w_rows"):
        below.wait_recv()
        above.wait_recv()
    put(slice(3, 19), slice(8, 40), x.ocean[...].astype(F32))
    put(slice(0, 3), slice(8, 40), x.above[...].astype(F32) * (la > 0).astype(F32))
    put(slice(19, 22), slice(8, 40), x.below[...].astype(F32) * (la < nla - 1).astype(F32))
    for h in range(2):
        lanes = slice(128 * h, 128 * h + 128)
        x.leave[0, :, lanes] = pack(x.pad[h, :, 32:40, :], True).reshape(88, 128).astype(BF16)
        x.leave[1, :, lanes] = pack(x.pad[h, :, 8:16, :], False).reshape(88, 128).astype(BF16)
    sides = [send(x.leave.at[0], x.cols.at[0], (0, 1)), send(x.leave.at[1], x.cols.at[1], (0, -1))]
    loaded("scale")
    ocean_rate(x)

    with jax.named_scope("w_under"):
        under.wait_recv()
    with jax.named_scope("w_south"):
        south.wait_recv()
        corner.wait_recv()
    x.mixed[0:4] = add_surface(x.under[...], x.enc8)[0:96].reshape(4, 24, 512)
    normalise(0, x.south[...], x.corner[...], gain, x.mixed, x.norm)
    attend(1, *windows)
    for g in (3, 0):
        finish(g, x.norm, x.mixed, x.cyc, x.pe.at[pl.ds(16 * g, 16)])
    loaded("fp")
    x.flux[...] = dot(x.fp[...], x.mixed[...].reshape(384, 512).astype(BF16), NT).astype(BF16)
    fluxes = [
        send(x.flux, x.fluxes.at[down * 4 + dj + 2], (down, -dj))
        for down in (1, 0) for dj in (1, -2, -1, 0) if (down, dj) != (0, 0)
    ]
    pieces += [
        send(x.pe.at[pl.ds(48, 16)], x.west.at[pl.ds(48, 16)], (0, 1)),
        send(x.pe.at[pl.ds(0, 16)], x.nw, (1, 1)),
        send(x.cyc.at[pl.ds(0, 4)], x.north, (1, 0)),
    ]
    x.fluxes[2] = x.flux[...]

    with jax.named_scope("w_sides"):
        for copy in sides:
            copy.wait_recv()
    for side, high in ((0, True), (1, False)):
        values = unpack(x.cols[side].astype(F32).reshape(11, 8, 256), high)
        put(slice(0, 22), slice(40 * side, 40 * side + 8), values)
    loaded("kernel", "cbias")
    convolve(x.pad, x.kernel, x.cbias, x.conv)

    loaded("fenc", "ogain", "w1", "w2")
    with jax.named_scope("w_flux"):
        for copy in fluxes:
            copy.wait_recv()
    ocean_update(x)
    with jax.named_scope("w_pieces"):
        for copy in pieces:
            copy.wait_recv()
        for copy in copies:
            copy.wait_send()


def last_kernel(cyc_ref, west_ref, north_ref, nw_ref, out_ref, atm_to, out_to, atm_s, store_sem):
    stores = [pltpu.make_async_copy(out_ref, out_to, store_sem.at[0])]
    stores[0].start()
    x = types.SimpleNamespace(cyc=cyc_ref, west=west_ref, north=north_ref, nw=nw_ref, atm=atm_s)
    for g in range(4):
        assemble(g, x)
        rows = pl.ds(4 * g, 4)
        stores.append(pltpu.make_async_copy(atm_s.at[rows], atm_to.at[rows], store_sem.at[g + 1]))
        stores[-1].start()
    for copy in stores:
        copy.wait()


def last(*results):
    shapes = [((16, 24, 512), BF16), ((16, 32, 256), BF16)]
    return pl.pallas_call(
        last_kernel,
        out_shape=[jax.ShapeDtypeStruct(*s) for s in shapes],
        in_specs=vmem(len(results)),
        out_specs=anywhere(len(shapes)),
        scratch_shapes=[pltpu.VMEM((16, 24, 512), BF16), pltpu.SemaphoreType.DMA((5,))],
        compiler_params=pltpu.CompilerParams(vmem_limit_bytes=24 << 20),
        name="last",
    )(*results)


def step(*operands):
    def copy_of(name, shape, kind):
        return pltpu.SMEM(shape, kind) if name in SCALARS else pltpu.VMEM(shape, kind)

    return pl.pallas_call(
        step_kernel,
        out_shape=[pltpu.VMEM(shape, kind) for _, shape, kind in RESULTS],
        in_specs=[pl.BlockSpec(memory_space=pltpu.HBM)] * len(OPERANDS),
        out_specs=vmem(len(RESULTS)),
        scratch_shapes=[
            *[copy_of(*o) for o in (*OPERANDS, *SCRATCH)],
            pltpu.SemaphoreType.DMA((len(OPERANDS),)), pltpu.SemaphoreType.DMA((COPIES,)), pltpu.SemaphoreType.DMA((COPIES,)),
        ],
        compiler_params=pltpu.CompilerParams(collective_id=0, has_side_effects=True),
        name="step",
    )(*operands)


def local(
    atmos_patch_tokens,
    atmos_norm_gain,
    query_key_value_weight,
    query_key_value_bias,
    relative_bias_grid,
    attention_output_weight,
    flux_projector,
    surface_encoder,
    ocean_cell_state,
    land_sea_mask,
    depthwise_conv_kernel,
    depthwise_conv_bias,
    ocean_norm_gain,
    pointwise_expand,
    pointwise_contract,
    layer_update_scale,
    forcing_encoder,
    surface_projector,
    overlay_area_weight,
    owners,
    owner_tile_blocks,
    counts,
):
    owners = owners.reshape(1, 3)
    blocks = owner_tile_blocks.reshape(1, 3)
    overlay = overlay_area_weight.reshape(3, 64, 512)
    results = step(
        ocean_cell_state, surface_projector.T, land_sea_mask, overlay, owners, blocks, counts, atmos_patch_tokens,
        relative_bias_grid, surface_encoder, atmos_norm_gain.reshape(1, 512), query_key_value_weight, query_key_value_bias,
        attention_output_weight, flux_projector.T, depthwise_conv_kernel, depthwise_conv_bias.reshape(1, 256), forcing_encoder,
        ocean_norm_gain.reshape(1, 256), pointwise_expand, pointwise_contract, layer_update_scale.reshape(1, 256),
    )
    return last(*results)


def solution(mesh):
    rep = P()
    placed = (
        P("lat", "lon", None), rep, rep, rep, rep, rep, rep, rep, P("lat", "lon", None), P("lat", "lon"),
        rep, rep, rep, rep, rep, rep, rep, rep, P("lat", "lon", None, None, None),
        P("lat", "lon", None), P("lat", "lon", None), P("lat", "lon"),
    )
    return jax.shard_map(
        local,
        mesh=mesh,
        in_specs=placed,
        out_specs=(P("lat", "lon", None), P("lat", "lon", None)),
        check_vma=False,
    )
```

```python
import types

import jax
import jax.numpy as jnp
from jax import lax
from jax.experimental import pallas as pl
from jax.experimental.pallas import tpu as pltpu
from jax.sharding import PartitionSpec as P

F32 = jnp.float32
BF16 = jnp.bfloat16
MESH = pl.DeviceIdType.MESH
HEADS = 16
HALF = 8
WIN = 8
NT = (((1,), (1,)), ((), ()))
TN = (((0,), (0,)), ((), ()))
NN = (((1,), (0,)), ((), ()))


def dot(a, b, dims):
    return lax.dot_general(a, b, dims, preferred_element_type=F32)


def iota(shape, dim):
    return lax.broadcasted_iota(jnp.int32, shape, dim)


def low_half(shape):
    return iota(shape, len(shape) - 2) % 8 < 4


def turn(x):
    return pltpu.roll(x, 4, x.ndim - 2)


def pack(x, high):
    n, _, lanes = x.shape
    x = x.reshape(n // 2, 2, 8, lanes)
    even, odd = x[:, 0], x[:, 1]
    if high:
        even = turn(even)
    else:
        odd = turn(odd)
    return jnp.where(low_half(even.shape), even, odd)


def unpack(x, high):
    n, _, lanes = x.shape
    other = turn(x)
    pair = (other, x) if high else (x, other)
    return jnp.stack(pair, axis=1).reshape(2 * n, 8, lanes)


def split2(x):
    top = x.astype(BF16).astype(F32)
    return top, x - top


def split3(x):
    top, rest = split2(x)
    middle, last = split2(rest)
    return top, middle, last


def greet(partners):
    barrier = pltpu.get_barrier_semaphore()
    for device in partners:
        pl.semaphore_signal(barrier, inc=1, device_id=device, device_id_type=MESH)
    return lambda: pl.semaphore_wait(barrier, len(partners))


def place():
    la, lo = lax.axis_index("lat"), lax.axis_index("lon")
    nla, nlo = lax.axis_size("lat"), lax.axis_size("lon")
    return lambda di, dj: (lax.rem(la + di + nla, nla), lax.rem(lo + dj + nlo, nlo))


def vmem(n):
    return [pl.BlockSpec(memory_space=pltpu.VMEM)] * n


def smem(n):
    return [pl.BlockSpec(memory_space=pltpu.SMEM)] * n


def anywhere(n):
    return [pl.BlockSpec(memory_space=pl.ANY)] * n


def layer_norm(x, gain, epsilon):
    average = jnp.mean(x, axis=-1, keepdims=True)
    centred = x - average
    spread = jnp.mean(centred * centred, axis=-1, keepdims=True)
    return centred * lax.rsqrt(spread + epsilon) * gain


def column_of(patch):
    p = patch.astype(F32)
    return p - 24.0 * jnp.floor((p + 0.5) * (1.0 / 24.0))


def mask_row(mask):
    wide = jnp.concatenate([mask.astype(F32), jnp.zeros((16, 96), F32)], axis=1)
    moved = [wide if q == 0 else pltpu.roll(wide, 32 * q, 1) for q in range(4)]
    parts = [sum(moved[q][4 * j + q : 4 * j + q + 1] for q in range(4)) for j in range(4)]
    return jnp.concatenate(parts, axis=1)


PARTNERS = [(0, 1), (0, -1), (0, 2), (0, -2), (1, 0), (-1, 0)]
COPIES = 32


def surface_message(owner_ref, block_ref, count_ref, ocean_ref, mask_ref, overlay_ref, proj_s, msg_s):
    lo = lax.axis_index("lon")
    nlo = lax.axis_size("lon")
    parts = jnp.concatenate(split3(proj_s[...]), axis=0).astype(BF16)
    surf = dot(parts, ocean_ref[...].reshape(512, 256), NT)
    surf = ((surf[0:8] + surf[8:16] + surf[16:24]) * mask_row(mask_ref[...])).astype(BF16)
    row = iota((8, 128), 0)
    twice = []
    codes = jnp.full((8, 128), -1.0, F32)
    for k in range(3):
        block = overlay_ref[k]
        twice.append(dot(surf, jnp.concatenate([block, block], axis=0), NT))
        side = lax.rem(owner_ref[0, k] - lo + 1 + nlo, nlo)
        code = jnp.where(k < count_ref[0, 0], side * 8 + block_ref[0, k], -1).astype(F32)
        codes = jnp.where(row == 4 + k, code, codes)
    msg_s[0:8] = jnp.where(row < 4, twice[0], twice[1])
    msg_s[8:16] = jnp.where(row < 4, twice[2], codes)


def gather_surface(msgs_ref):
    upper = iota((8, 128), 0) < 4
    right = iota((8, 128), 1) >= 64
    tiles = []
    for tile in range(2):
        sums = [jnp.zeros((8, 128), F32)] * 3
        for side in range(3):
            slot = tile - side + 2
            a = msgs_ref[slot, 0:8, :]
            b = msgs_ref[slot, 8:16, :]
            code_a = jnp.where(upper, b[4:5], b[5:6])
            code_b = jnp.where(upper, b[6:7], -1.0)
            for j in range(3):
                target = jnp.where(right, side * 8.0 + 2 * j + 1, side * 8.0 + 2 * j)
                sums[j] += jnp.where(code_a == target, a, 0.0) + jnp.where(code_b == target, b, 0.0)
        tiles.append(sums)
    return [
        jnp.where(column_of(iota((8, 128), 1) + 128 * j) < 4, tiles[1][j], tiles[0][j]) for j in range(3)
    ]


def bias_table(grid_ref, table_s, rows_s, bias_s):
    grid = jnp.concatenate([grid_ref[...], jnp.zeros((16, 31), F32)], axis=1)
    for ra in range(8):
        rolled = grid if ra == 0 else pltpu.roll(grid, 256 - 15 * ra, 1)
        table_s[:, ra, :] = rolled[:, 0:128]
    parts = [x.astype(BF16) for x in split3(table_s[...].reshape(128, 128))]
    entry = iota((128, 64), 0)
    lane = iota((128, 64), 1)
    for ca in range(8):
        chosen = (entry == (7 - lane // 8) * 15 + ca - lane % 8 + 7).astype(BF16)
        found = (dot(parts[0], chosen, NN) + dot(parts[1], chosen, NN)) + dot(parts[2], chosen, NN)
        rows_s[:, ca, :] = found
    for part in range(8):
        rows = rows_s[16 * part : 16 * part + 16].reshape(128, 64)
        bias_s[:, 128 * part : 128 * part + 128] = rows.T


def add_surface(sst, enc_s):
    s_hi, s_lo = split2(sst)
    e_hi, e_lo = split2(enc_s[...])
    left = jnp.concatenate([s_hi, s_lo, s_hi], axis=0).astype(BF16)
    right = jnp.concatenate([e_hi, e_hi, e_lo], axis=0).astype(BF16)
    return dot(left, right, TN)


def normalise(g, tokens, side, gain, mixed_s, norm_s):
    low = low_half((4, 8, 512))
    rows = slice(4 * g, 4 * g + 4)
    tokens = tokens.astype(F32)
    side = unpack(side.astype(F32).reshape(2, 8, 512), False)
    head = jnp.where(low, side, tokens[:, 0:8])
    tokens = jnp.concatenate([head, tokens[:, 8:24]], axis=1)
    mixed = (tokens + mixed_s[rows]).astype(BF16).astype(F32)
    mixed_s[rows] = mixed
    normed = layer_norm(mixed, gain, 1e-05)
    turned = [turn(normed[:, 8 * b : 8 * b + 8]) for b in range(3)]
    w_row, w_start = WINDOW_OF[g]
    for b in range(3):
        norm_s[w_row * 3 + b, w_start : w_start + 4] = jnp.where(low, turned[b], turned[(b + 1) % 3])


WINDOW_OF = ((1, 4), (0, 0), (0, 4), (1, 0))


def attend(w_row, norm_s, wqkv_s, bqkv_ref, wo_s, bias_s, last_s, q_s, k_s, v_s, att_s):
    rows = norm_s[3 * w_row : 3 * w_row + 3].reshape(192, 512).astype(BF16)
    for part, ref in enumerate((q_s, k_s, v_s)):
        cols = slice(512 * part, 512 * part + 512)
        value = dot(rows, wqkv_s[:, cols], NN) + bqkv_ref[cols].reshape(1, 512)
        if part == 0:
            value = value * 32 ** (-0.5)
        ref[...] = value.astype(BF16)
    own = (iota((8, 1, 256), 2) // 32) == iota((8, 1, 256), 0)
    first_head = iota((64, 128), 0) < 32
    for w in range(3):
        at = slice(64 * w, 64 * w + 64)
        for g in range(2):
            lanes = slice(256 * g, 256 * g + 256)
            queries = jnp.where(own, q_s[at, lanes][None], jnp.zeros((), BF16)).reshape(512, 256)
            scores = dot(k_s[at, lanes], queries, NT) + bias_s[:, 512 * g : 512 * g + 512]
            if w_row == 1:
                scores = scores + last_s[...]
            scores = jnp.exp(scores - jnp.max(scores, axis=0, keepdims=True))
            weights = (scores * (1.0 / jnp.sum(scores, axis=0, keepdims=True))).astype(BF16)
            values = v_s[at, lanes].astype(F32).T.astype(BF16)
            found = []
            for pair in range(4):
                both = dot(values[64 * pair : 64 * pair + 64], weights[:, 128 * pair : 128 * pair + 128], NN)
                found.append(jnp.where(first_head, both, pltpu.roll(both, 64, 1)))
            att_s[at, lanes] = jnp.concatenate(found, axis=0).T[0:64].astype(BF16)
    projected = dot(att_s[...], wo_s[...], NN).astype(BF16).astype(F32)
    norm_s[3 * w_row : 3 * w_row + 3] = projected.reshape(3, 8, 8, 512)


def finish(g, norm_s, mixed_s, cyc_ref, side_ref):
    w_row, w_start = WINDOW_OF[g]
    turned = [turn(norm_s[w_row * 3 + b, w_start : w_start + 4]) for b in range(3)]
    low = low_half((4, 8, 512))
    back = jnp.concatenate([jnp.where(low, turned[b - 1], turned[b]) for b in range(3)], axis=1)
    rows = slice(4 * g, 4 * g + 4)
    result = (mixed_s[rows] + back).astype(BF16)
    mixed_s[rows] = result.astype(F32)
    cyc_ref[rows] = result
    side_ref[...] = pack(result.astype(F32)[:, 0:8], False).reshape(16, 512).astype(BF16)


def convolve(pad_s, kernel_ref, cbias_ref, conv_ref):
    def band(i, carry):
        start = i * 8
        for h in range(2):
            lanes = slice(128 * h, 128 * h + 128)
            first_term = jnp.broadcast_to(cbias_ref[:, lanes], (8, 128))
            for b in range(4):
                sums = [first_term] * 8
                for v in range(7):
                    col = 8 * b + v + 5
                    cells = [pad_s[h, start + r, col : col + 8, :] for r in range(14)]
                    for u in range(7):
                        tap = kernel_ref[u, v : v + 1, lanes]
                        for r in range(8):
                            sums[r] = sums[r] + tap * cells[r + u]
                for r in range(8):
                    conv_ref[start + r, 8 * b : 8 * b + 8, lanes] = sums[r]
        return carry

    lax.fori_loop(0, 2, band, 0)


OPERANDS = (
    ("ocean", (16, 32, 256), BF16), ("proj", (4, 256), F32), ("mask", (16, 32), jnp.int32), ("overlay", (3, 64, 512), BF16),
    ("owner", (1, 3), jnp.int32), ("block", (1, 3), jnp.int32), ("count", (1, 1), jnp.int32), ("tok", (16, 24, 512), BF16),
    ("grid", (16, 225), F32), ("enc", (4, 512), F32), ("gain", (1, 512), F32), ("wqkv", (512, 1536), BF16),
    ("bqkv", (1536,), F32), ("wo", (512, 512), BF16), ("fp", (16, 512), BF16), ("kernel", (7, 7, 256), F32),
    ("cbias", (1, 256), F32), ("fenc", (16, 256), F32), ("ogain", (1, 256), F32), ("w1", (256, 1024), BF16),
    ("w2", (1024, 256), BF16), ("scale", (1, 256), F32),
)
SCALARS = ("owner", "block", "count")
SCRATCH = (
    ("proj8", (8, 256), F32), ("enc8", (8, 512), F32), ("msg", (16, 128), F32), ("msgs", (4, 16, 128), F32),
    ("side", (64, 512), BF16), ("east", (64, 512), BF16), ("south", (4, 24, 512), BF16), ("corner", (16, 512), BF16),
    ("sst", (8, 128), F32), ("under", (8, 128), F32), ("table", (16, 8, 128), F32), ("rows", (128, 8, 64), F32),
    ("bias", (64, 1024), F32), ("last", (64, 512), F32), ("mixed", (16, 24, 512), F32), ("norm", (6, 8, 8, 512), F32), ("q", (192, 512), BF16),
    ("k", (192, 512), BF16), ("v", (192, 512), BF16), ("att", (192, 512), BF16), ("above", (3, 32, 256), BF16),
    ("below", (3, 32, 256), BF16), ("leave", (2, 88, 256), BF16), ("cols", (2, 88, 256), BF16),
    ("pad", (2, 22, 48, 128), F32), ("pe", (64, 512), BF16), ("flux", (16, 384), BF16),
    ("near", (2, 16, 384), BF16), ("top", (16, 128), BF16), ("rim", (16, 128), BF16),
    ("tops", (3, 16, 128), BF16), ("edge", (2, 16, 128), BF16), ("spread", (64, 384), BF16), ("conv", (16, 32, 256), F32), ("pre", (512, 256), F32), ("rate", (512, 256), F32),
)
RESULTS = (
    ("cyc", (16, 24, 512), BF16), ("west", (64, 512), BF16), ("north", (4, 24, 512), BF16), ("nw", (16, 512), BF16),
    ("out", (16, 32, 256), BF16),
)


def spread(x):
    patch = iota((64, 384), 0)
    x.spread[...] = (iota((64, 384), 1) == 24 * (patch // 4) + patch % 4).astype(BF16)


def pick_flux(x, codes):
    lane = iota((16, 128), 1)
    right = lane >= 64
    edge = dot(x.edge[...].reshape(32, 128)[:, 0:64], x.spread[...], NN)
    west, own, east = x.near[0].astype(F32), x.flux[...].astype(F32), x.near[1].astype(F32)
    heads, bodies = (edge[0:16], west, own), (west, own, east)
    tops = [x.tops[n].astype(F32) for n in range(3)]
    top_heads = (edge[16:32, 0:128], tops[0], tops[1])
    picked = [jnp.zeros((16, 128), F32)] * 3
    for j in range(3):
        patch = lane + 128 * j
        head = column_of(patch) < 4
        at = slice(128 * j, 128 * j + 128)
        for side in range(3):
            tile = jnp.where(head, heads[side][:, at], bodies[side][:, at])
            if j == 0:
                tile = jnp.where(patch < 96, jnp.where(head, top_heads[side], tops[side]), tile)
            target = jnp.where(right, side * 8 + 2 * j + 1, side * 8 + 2 * j)
            for k in range(3):
                picked[k] += jnp.where(target == codes[k], tile, 0.0)
    picked = [y + pltpu.roll(y, 64, 1) for y in picked]
    return jnp.concatenate([jnp.where(right, picked[1], picked[0]), picked[2][:, 0:64]], axis=1)


def slot_codes(x):
    lo = lax.axis_index("lon")
    nlo = lax.axis_size("lon")
    codes = []
    for k in range(3):
        side = lax.rem(x.owner[0, k] - lo + 1 + nlo, nlo)
        codes.append(jnp.where(k < x.count[0, 0], side * 8 + x.block[0, k], -1))
    return codes


def ocean_rate(x):
    mask = jnp.broadcast_to(mask_row(x.mask[...]), (16, 512)).astype(BF16)
    parts = [jnp.broadcast_to(y, (16, 256)) for y in split3(x.scale[...])]
    row = iota((16, 256), 0)
    scale = jnp.where(row == 0, parts[0], jnp.where(row == 1, parts[1], jnp.where(row == 2, parts[2], 0.0)))
    x.rate[...] = dot(mask, scale.astype(BF16), TN)


def ocean_update(x):
    forcing = dot(pick_flux(x, slot_codes(x)).astype(BF16), x.overlay[...].reshape(192, 512), NN)
    f_hi, f_lo = split2(forcing)
    e_hi, e_lo = split2(x.fenc[...])
    x.pre[...] = x.conv[...].reshape(512, 256) + dot(
        jnp.concatenate([f_hi, f_lo, f_hi], axis=0).astype(BF16),
        jnp.concatenate([e_hi, e_hi, e_lo], axis=0).astype(BF16),
        TN,
    )

    def cells(i, carry):
        at = pl.ds(pl.multiple_of(i * 128, 128), 128)
        normed = layer_norm(x.pre[at], x.ogain[...], 1e-06).astype(BF16)
        update = jnp.zeros((128, 256), F32)
        for c in range(4):
            cols = slice(256 * c, 256 * c + 256)
            y = dot(normed, x.w1[:, cols], NN)
            hidden = (0.5 * y * (1.0 + lax.erf(y * (0.5**0.5)))).astype(BF16)
            update = update + dot(hidden, x.w2[cols], NN)
        rows = pl.ds(i * 4, 4)
        state = x.ocean[rows].astype(F32).reshape(128, 256)
        x.out[rows] = (state + x.rate[at] * update).astype(BF16).reshape(4, 32, 256)
        return carry

    lax.fori_loop(0, 4, cells, 0)


def assemble(g, x):
    low = low_half((4, 8, 512))
    rows = slice(4 * g, 4 * g + 4)
    body, side = (x.north, x.nw[...]) if g == 0 else (x.cyc.at[rows], x.west[16 * g : 16 * g + 16])
    body = body[...].astype(F32)
    side = unpack(side.astype(F32).reshape(2, 8, 512), False)
    head = jnp.where(low, side, body[:, 0:8])
    x.atm[rows] = jnp.concatenate([head, body[:, 8:24]], axis=1).astype(BF16)


def step_kernel(*refs):
    n = len(OPERANDS)
    given = dict(zip([o[0] for o in OPERANDS], refs[:n]))
    names = [o[0] for o in (*RESULTS, *OPERANDS, *SCRATCH)]
    x = types.SimpleNamespace(**dict(zip(names, refs[n:])))
    load_sem, send_sem, recv_sem = refs[n + len(names) :]

    at = place()
    la = lax.axis_index("lat")
    nla = lax.axis_size("lat")
    wait_barrier = greet([at(*o) for o in PARTNERS])
    loads = {}
    for i, (name, *_) in enumerate(OPERANDS):
        loads[name] = pltpu.make_async_copy(given[name], getattr(x, name), load_sem.at[i])
        loads[name].start()

    def loaded(*names):
        for name in names:
            loads[name].wait()

    copies = []

    def send(src, dst, offset):
        i = len(copies)
        copy = pltpu.make_async_remote_copy(
            src_ref=src, dst_ref=dst, send_sem=send_sem.at[i], recv_sem=recv_sem.at[i],
            device_id=at(*offset), device_id_type=MESH,
        )
        copies.append(copy)
        copy.start()
        return copy

    loaded("ocean", "proj", "mask", "overlay", "owner", "block", "count")
    for half in range(2):
        x.proj8[4 * half : 4 * half + 4] = x.proj[...]
    surface_message(x.owner, x.block, x.count, x.ocean, x.mask, x.overlay, x.proj8, x.msg)
    loaded("tok")
    x.side[...] = pack(x.tok[:, 0:8, :].astype(F32), False).reshape(64, 512).astype(BF16)

    wait_barrier()
    messages = [send(x.msg, x.msgs.at[dj + 1], (0, -dj)) for dj in (2, 1, -1)]
    x.msgs[1] = x.msg[...]
    east_top = send(x.side.at[pl.ds(0, 16)], x.east.at[pl.ds(0, 16)], (0, -1))
    east = send(x.side.at[pl.ds(16, 48)], x.east.at[pl.ds(16, 48)], (0, -1))
    south = send(x.tok.at[pl.ds(0, 4)], x.south, (-1, 0))

    loaded("grid", "enc", "gain")
    for half in range(2):
        x.enc8[4 * half : 4 * half + 4] = x.enc[...]
    bias_table(x.grid, x.table, x.rows, x.bias)
    edge = la == nla - 1
    a_row = (iota((64, 512), 1) % 64) >= 32
    b_row = iota((64, 512), 0) >= 32
    x.last[...] = jnp.where(edge, jnp.where(a_row != b_row, -1e9, 0.0), 0.0)

    for copy in messages:
        copy.wait_recv()
    sst = gather_surface(x.msgs)
    x.sst[...] = sst[0]
    under = send(x.sst, x.under, (-1, 0))
    east_top.wait_recv()
    corner = send(x.east.at[pl.ds(0, 16)], x.corner, (-1, 0))
    below = send(x.ocean.at[pl.ds(0, 3)], x.below, (-1, 0))
    above = send(x.ocean.at[pl.ds(13, 3)], x.above, (1, 0))
    x.mixed[...] = add_surface(jnp.concatenate(sst, axis=1), x.enc8).reshape(16, 24, 512)
    gain = x.gain[...].reshape(1, 1, 512)
    east.wait_recv()
    for g in (1, 2, 3):
        normalise(g, x.tok[4 * g : 4 * g + 4], x.east[16 * g : 16 * g + 16], gain, x.mixed, x.norm)
    loaded("wqkv", "bqkv", "wo")
    windows = (x.norm, x.wqkv, x.bqkv, x.wo, x.bias, x.last, x.q, x.k, x.v, x.att)
    attend(0, *windows)
    for g in (1, 2):
        finish(g, x.norm, x.mixed, x.cyc, x.pe.at[pl.ds(16 * g, 16)])
    pieces = [send(x.pe.at[pl.ds(16, 32)], x.west.at[pl.ds(16, 32)], (0, 1))]

    def put(rows, cols, values):
        for h in range(2):
            x.pad[h, rows, cols, :] = values[:, :, 128 * h : 128 * h + 128]

    below.wait_recv()
    above.wait_recv()
    put(slice(3, 19), slice(8, 40), x.ocean[...].astype(F32))
    put(slice(0, 3), slice(8, 40), x.above[...].astype(F32) * (la > 0).astype(F32))
    put(slice(19, 22), slice(8, 40), x.below[...].astype(F32) * (la < nla - 1).astype(F32))
    for h in range(2):
        lanes = slice(128 * h, 128 * h + 128)
        x.leave[0, :, lanes] = pack(x.pad[h, :, 32:40, :], True).reshape(88, 128).astype(BF16)
        x.leave[1, :, lanes] = pack(x.pad[h, :, 8:16, :], False).reshape(88, 128).astype(BF16)
    sides = [send(x.leave.at[0], x.cols.at[0], (0, 1)), send(x.leave.at[1], x.cols.at[1], (0, -1))]
    loaded("scale")
    ocean_rate(x)
    spread(x)

    under.wait_recv()
    south.wait_recv()
    corner.wait_recv()
    x.mixed[0:4] = add_surface(x.under[...], x.enc8)[0:96].reshape(4, 24, 512)
    normalise(0, x.south[...], x.corner[...], gain, x.mixed, x.norm)
    attend(1, *windows)
    for g in (3, 0):
        finish(g, x.norm, x.mixed, x.cyc, x.pe.at[pl.ds(16 * g, 16)])
    loaded("fp")
    flux = dot(x.fp[...], x.mixed[...].reshape(384, 512).astype(BF16), NT).astype(BF16)
    x.flux[...] = flux
    x.top[...] = flux[:, 0:128]
    edge = dot(x.fp[...], x.pe[...], NT)
    x.rim[...] = jnp.concatenate([edge, jnp.zeros((16, 64), F32)], axis=1).astype(BF16)
    fluxes = [
        send(x.top, x.tops.at[2], (1, -1)),
        send(x.rim, x.edge.at[1], (1, 2)),
        send(x.rim, x.edge.at[0], (0, 2)),
        send(x.top, x.tops.at[0], (1, 1)),
        send(x.top, x.tops.at[1], (1, 0)),
        send(x.flux, x.near.at[1], (0, -1)),
        send(x.flux, x.near.at[0], (0, 1)),
    ]
    pieces += [
        send(x.pe.at[pl.ds(48, 16)], x.west.at[pl.ds(48, 16)], (0, 1)),
        send(x.pe.at[pl.ds(0, 16)], x.nw, (1, 1)),
        send(x.cyc.at[pl.ds(0, 4)], x.north, (1, 0)),
    ]

    for copy in sides:
        copy.wait_recv()
    for side, high in ((0, True), (1, False)):
        values = unpack(x.cols[side].astype(F32).reshape(11, 8, 256), high)
        put(slice(0, 22), slice(40 * side, 40 * side + 8), values)
    loaded("kernel", "cbias")
    convolve(x.pad, x.kernel, x.cbias, x.conv)

    loaded("fenc", "ogain", "w1", "w2")
    for copy in fluxes:
        copy.wait_recv()
    ocean_update(x)
    for copy in pieces:
        copy.wait_recv()
    for copy in copies:
        copy.wait_send()


def last_kernel(cyc_ref, west_ref, north_ref, nw_ref, out_ref, atm_to, out_to, atm_s, store_sem):
    stores = [pltpu.make_async_copy(out_ref, out_to, store_sem.at[0])]
    stores[0].start()
    x = types.SimpleNamespace(cyc=cyc_ref, west=west_ref, north=north_ref, nw=nw_ref, atm=atm_s)
    for g in range(4):
        assemble(g, x)
        rows = pl.ds(4 * g, 4)
        stores.append(pltpu.make_async_copy(atm_s.at[rows], atm_to.at[rows], store_sem.at[g + 1]))
        stores[-1].start()
    for copy in stores:
        copy.wait()


def last(*results):
    shapes = [((16, 24, 512), BF16), ((16, 32, 256), BF16)]
    return pl.pallas_call(
        last_kernel,
        out_shape=[jax.ShapeDtypeStruct(*s) for s in shapes],
        in_specs=vmem(len(results)),
        out_specs=anywhere(len(shapes)),
        scratch_shapes=[pltpu.VMEM((16, 24, 512), BF16), pltpu.SemaphoreType.DMA((5,))],
        compiler_params=pltpu.CompilerParams(vmem_limit_bytes=24 << 20),
        name="last",
    )(*results)


def step(*operands):
    def copy_of(name, shape, kind):
        return pltpu.SMEM(shape, kind) if name in SCALARS else pltpu.VMEM(shape, kind)

    return pl.pallas_call(
        step_kernel,
        out_shape=[pltpu.VMEM(shape, kind) for _, shape, kind in RESULTS],
        in_specs=[pl.BlockSpec(memory_space=pltpu.HBM)] * len(OPERANDS),
        out_specs=vmem(len(RESULTS)),
        scratch_shapes=[
            *[copy_of(*o) for o in (*OPERANDS, *SCRATCH)],
            pltpu.SemaphoreType.DMA((len(OPERANDS),)), pltpu.SemaphoreType.DMA((COPIES,)), pltpu.SemaphoreType.DMA((COPIES,)),
        ],
        compiler_params=pltpu.CompilerParams(collective_id=0, has_side_effects=True),
        name="step",
    )(*operands)


def local(
    atmos_patch_tokens,
    atmos_norm_gain,
    query_key_value_weight,
    query_key_value_bias,
    relative_bias_grid,
    attention_output_weight,
    flux_projector,
    surface_encoder,
    ocean_cell_state,
    land_sea_mask,
    depthwise_conv_kernel,
    depthwise_conv_bias,
    ocean_norm_gain,
    pointwise_expand,
    pointwise_contract,
    layer_update_scale,
    forcing_encoder,
    surface_projector,
    overlay_area_weight,
    owners,
    owner_tile_blocks,
    counts,
):
    owners = owners.reshape(1, 3)
    blocks = owner_tile_blocks.reshape(1, 3)
    overlay = overlay_area_weight.reshape(3, 64, 512)
    results = step(
        ocean_cell_state, surface_projector.T, land_sea_mask, overlay, owners, blocks, counts, atmos_patch_tokens,
        relative_bias_grid, surface_encoder, atmos_norm_gain.reshape(1, 512), query_key_value_weight, query_key_value_bias,
        attention_output_weight, flux_projector.T, depthwise_conv_kernel, depthwise_conv_bias.reshape(1, 256), forcing_encoder,
        ocean_norm_gain.reshape(1, 256), pointwise_expand, pointwise_contract, layer_update_scale.reshape(1, 256),
    )
    return last(*results)


def solution(mesh):
    rep = P()
    placed = (
        P("lat", "lon", None), rep, rep, rep, rep, rep, rep, rep, P("lat", "lon", None), P("lat", "lon"),
        rep, rep, rep, rep, rep, rep, rep, rep, P("lat", "lon", None, None, None),
        P("lat", "lon", None), P("lat", "lon", None), P("lat", "lon"),
    )
    return jax.shard_map(
        local,
        mesh=mesh,
        in_specs=placed,
        out_specs=(P("lat", "lon", None), P("lat", "lon", None)),
        check_vma=False,
    )
```

```python
import types

import jax
import jax.numpy as jnp
from jax import lax
from jax.experimental import pallas as pl
from jax.experimental.pallas import tpu as pltpu
from jax.sharding import PartitionSpec as P

F32 = jnp.float32
BF16 = jnp.bfloat16
MESH = pl.DeviceIdType.MESH
HEADS = 16
HALF = 8
WIN = 8
NT = (((1,), (1,)), ((), ()))
TN = (((0,), (0,)), ((), ()))
NN = (((1,), (0,)), ((), ()))


def dot(a, b, dims):
    return lax.dot_general(a, b, dims, preferred_element_type=F32)


def iota(shape, dim):
    return lax.broadcasted_iota(jnp.int32, shape, dim)


def low_half(shape):
    return iota(shape, len(shape) - 2) % 8 < 4


def turn(x):
    return pltpu.roll(x, 4, x.ndim - 2)


def pack(x, high):
    n, _, lanes = x.shape
    x = x.reshape(n // 2, 2, 8, lanes)
    even, odd = x[:, 0], x[:, 1]
    if high:
        even = turn(even)
    else:
        odd = turn(odd)
    return jnp.where(low_half(even.shape), even, odd)


def unpack(x, high):
    n, _, lanes = x.shape
    other = turn(x)
    pair = (other, x) if high else (x, other)
    return jnp.stack(pair, axis=1).reshape(2 * n, 8, lanes)


def split2(x):
    top = x.astype(BF16).astype(F32)
    return top, x - top


def split3(x):
    top, rest = split2(x)
    middle, last = split2(rest)
    return top, middle, last


def greet(partners):
    barrier = pltpu.get_barrier_semaphore()
    for device in partners:
        pl.semaphore_signal(barrier, inc=1, device_id=device, device_id_type=MESH)
    return lambda: pl.semaphore_wait(barrier, len(partners))


def place():
    la, lo = lax.axis_index("lat"), lax.axis_index("lon")
    nla, nlo = lax.axis_size("lat"), lax.axis_size("lon")
    return lambda di, dj: (lax.rem(la + di + nla, nla), lax.rem(lo + dj + nlo, nlo))


def vmem(n):
    return [pl.BlockSpec(memory_space=pltpu.VMEM)] * n


def smem(n):
    return [pl.BlockSpec(memory_space=pltpu.SMEM)] * n


def anywhere(n):
    return [pl.BlockSpec(memory_space=pl.ANY)] * n


def layer_norm(x, gain, epsilon):
    average = jnp.mean(x, axis=-1, keepdims=True)
    centred = x - average
    spread = jnp.mean(centred * centred, axis=-1, keepdims=True)
    return centred * lax.rsqrt(spread + epsilon) * gain


def column_of(patch):
    p = patch.astype(F32)
    return p - 24.0 * jnp.floor((p + 0.5) * (1.0 / 24.0))


def mask_row(mask):
    wide = jnp.concatenate([mask.astype(F32), jnp.zeros((16, 96), F32)], axis=1)
    moved = [wide if q == 0 else pltpu.roll(wide, 32 * q, 1) for q in range(4)]
    parts = [sum(moved[q][4 * j + q : 4 * j + q + 1] for q in range(4)) for j in range(4)]
    return jnp.concatenate(parts, axis=1)


PARTNERS = [(0, 1), (0, -1), (0, 2), (0, -2), (1, 0), (-1, 0)]
COPIES = 32


def surface_message(owner_ref, block_ref, count_ref, ocean_ref, mask_ref, overlay_ref, proj_s, msg_s):
    lo = lax.axis_index("lon")
    nlo = lax.axis_size("lon")
    parts = jnp.concatenate(split3(proj_s[...]), axis=0).astype(BF16)
    surf = dot(parts, ocean_ref[...].reshape(512, 256), NT)
    surf = ((surf[0:8] + surf[8:16] + surf[16:24]) * mask_row(mask_ref[...])).astype(BF16)
    row = iota((8, 128), 0)
    twice = []
    codes = jnp.full((8, 128), -1.0, F32)
    for k in range(3):
        block = overlay_ref[k]
        twice.append(dot(surf, jnp.concatenate([block, block], axis=0), NT))
        side = lax.rem(owner_ref[0, k] - lo + 1 + nlo, nlo)
        code = jnp.where(k < count_ref[0, 0], side * 8 + block_ref[0, k], -1).astype(F32)
        codes = jnp.where(row == 4 + k, code, codes)
    msg_s[0:8] = jnp.where(row < 4, twice[0], twice[1])
    msg_s[8:16] = jnp.where(row < 4, twice[2], codes)


def gather_surface(msgs_ref):
    upper = iota((8, 128), 0) < 4
    right = iota((8, 128), 1) >= 64
    tiles = []
    for tile in range(2):
        sums = [jnp.zeros((8, 128), F32)] * 3
        for side in range(3):
            slot = tile - side + 2
            a = msgs_ref[slot, 0:8, :]
            b = msgs_ref[slot, 8:16, :]
            code_a = jnp.where(upper, b[4:5], b[5:6])
            code_b = jnp.where(upper, b[6:7], -1.0)
            for j in range(3):
                target = jnp.where(right, side * 8.0 + 2 * j + 1, side * 8.0 + 2 * j)
                sums[j] += jnp.where(code_a == target, a, 0.0) + jnp.where(code_b == target, b, 0.0)
        tiles.append(sums)
    return [
        jnp.where(column_of(iota((8, 128), 1) + 128 * j) < 4, tiles[1][j], tiles[0][j]) for j in range(3)
    ]


def bias_table(grid_ref, table_s, rows_s, bias_s):
    grid = jnp.concatenate([grid_ref[...], jnp.zeros((16, 31), F32)], axis=1)
    for ra in range(8):
        rolled = grid if ra == 0 else pltpu.roll(grid, 256 - 15 * ra, 1)
        table_s[:, ra, :] = rolled[:, 0:128]
    parts = [x.astype(BF16) for x in split3(table_s[...].reshape(128, 128))]
    entry = iota((128, 64), 0)
    lane = iota((128, 64), 1)
    for ca in range(8):
        chosen = (entry == (7 - lane // 8) * 15 + ca - lane % 8 + 7).astype(BF16)
        found = (dot(parts[0], chosen, NN) + dot(parts[1], chosen, NN)) + dot(parts[2], chosen, NN)
        rows_s[:, ca, :] = found
    for part in range(8):
        rows = rows_s[16 * part : 16 * part + 16].reshape(128, 64)
        bias_s[:, 128 * part : 128 * part + 128] = rows.T


def add_surface(sst, enc_s):
    s_hi, s_lo = split2(sst)
    e_hi, e_lo = split2(enc_s[...])
    left = jnp.concatenate([s_hi, s_lo, s_hi], axis=0).astype(BF16)
    right = jnp.concatenate([e_hi, e_hi, e_lo], axis=0).astype(BF16)
    return dot(left, right, TN)


def normalise(g, tokens, side, gain, mixed_s, norm_s):
    low = low_half((4, 8, 512))
    rows = slice(4 * g, 4 * g + 4)
    tokens = tokens.astype(F32)
    side = unpack(side.astype(F32).reshape(2, 8, 512), False)
    head = jnp.where(low, side, tokens[:, 0:8])
    tokens = jnp.concatenate([head, tokens[:, 8:24]], axis=1)
    mixed = (tokens + mixed_s[rows]).astype(BF16).astype(F32)
    mixed_s[rows] = mixed
    normed = layer_norm(mixed, gain, 1e-05)
    turned = [turn(normed[:, 8 * b : 8 * b + 8]) for b in range(3)]
    w_row, w_start = WINDOW_OF[g]
    for b in range(3):
        norm_s[w_row * 3 + b, w_start : w_start + 4] = jnp.where(low, turned[b], turned[(b + 1) % 3])


WINDOW_OF = ((1, 4), (0, 0), (0, 4), (1, 0))


def attend(w_row, norm_s, wqkv_s, bqkv_ref, wo_s, bias_s, last_s, q_s, k_s, v_s, att_s):
    rows = norm_s[3 * w_row : 3 * w_row + 3].reshape(192, 512).astype(BF16)
    for part, ref in enumerate((q_s, k_s, v_s)):
        cols = slice(512 * part, 512 * part + 512)
        value = dot(rows, wqkv_s[:, cols], NN) + bqkv_ref[cols].reshape(1, 512)
        if part == 0:
            value = value * 32 ** (-0.5)
        ref[...] = value.astype(BF16)
    own = (iota((8, 1, 256), 2) // 32) == iota((8, 1, 256), 0)
    first_head = iota((64, 128), 0) < 32
    for w in range(3):
        at = slice(64 * w, 64 * w + 64)
        for g in range(2):
            lanes = slice(256 * g, 256 * g + 256)
            queries = jnp.where(own, q_s[at, lanes][None], jnp.zeros((), BF16)).reshape(512, 256)
            scores = dot(k_s[at, lanes], queries, NT) + bias_s[:, 512 * g : 512 * g + 512]
            if w_row == 1:
                scores = scores + last_s[...]
            scores = jnp.exp(scores - jnp.max(scores, axis=0, keepdims=True))
            weights = (scores * (1.0 / jnp.sum(scores, axis=0, keepdims=True))).astype(BF16)
            values = v_s[at, lanes].astype(F32).T.astype(BF16)
            found = []
            for pair in range(4):
                both = dot(values[64 * pair : 64 * pair + 64], weights[:, 128 * pair : 128 * pair + 128], NN)
                found.append(jnp.where(first_head, both, pltpu.roll(both, 64, 1)))
            att_s[at, lanes] = jnp.concatenate(found, axis=0).T[0:64].astype(BF16)
    projected = dot(att_s[...], wo_s[...], NN).astype(BF16).astype(F32)
    norm_s[3 * w_row : 3 * w_row + 3] = projected.reshape(3, 8, 8, 512)


def finish(g, norm_s, mixed_s, cyc_ref, side_ref):
    w_row, w_start = WINDOW_OF[g]
    turned = [turn(norm_s[w_row * 3 + b, w_start : w_start + 4]) for b in range(3)]
    low = low_half((4, 8, 512))
    back = jnp.concatenate([jnp.where(low, turned[b - 1], turned[b]) for b in range(3)], axis=1)
    rows = slice(4 * g, 4 * g + 4)
    result = (mixed_s[rows] + back).astype(BF16)
    mixed_s[rows] = result.astype(F32)
    cyc_ref[rows] = result
    side_ref[...] = pack(result.astype(F32)[:, 0:8], False).reshape(16, 512).astype(BF16)


def convolve(pad_s, kernel_ref, cbias_ref, conv_ref):
    def band(i, carry):
        start = i * 8
        for h in range(2):
            lanes = slice(128 * h, 128 * h + 128)
            first_term = jnp.broadcast_to(cbias_ref[:, lanes], (8, 128))
            for b in range(4):
                sums = [first_term] * 8
                for v in range(7):
                    col = 8 * b + v + 5
                    cells = [pad_s[h, start + r, col : col + 8, :] for r in range(14)]
                    for u in range(7):
                        tap = kernel_ref[u, v : v + 1, lanes]
                        for r in range(8):
                            sums[r] = sums[r] + tap * cells[r + u]
                for r in range(8):
                    conv_ref[start + r, 8 * b : 8 * b + 8, lanes] = sums[r]
        return carry

    lax.fori_loop(0, 2, band, 0)


OPERANDS = (
    ("ocean", (16, 32, 256), BF16), ("proj", (4, 256), F32), ("mask", (16, 32), jnp.int32), ("overlay", (3, 64, 512), BF16),
    ("owner", (1, 3), jnp.int32), ("block", (1, 3), jnp.int32), ("count", (1, 1), jnp.int32), ("tok", (16, 24, 512), BF16),
    ("grid", (16, 225), F32), ("enc", (4, 512), F32), ("gain", (1, 512), F32), ("wqkv", (512, 1536), BF16),
    ("bqkv", (1536,), F32), ("wo", (512, 512), BF16), ("fp", (16, 512), BF16), ("kernel", (7, 7, 256), F32),
    ("cbias", (1, 256), F32), ("fenc", (16, 256), F32), ("ogain", (1, 256), F32), ("w1", (256, 1024), BF16),
    ("w2", (1024, 256), BF16), ("scale", (1, 256), F32),
)
SCALARS = ("owner", "block", "count")
SCRATCH = (
    ("proj8", (8, 256), F32), ("enc8", (8, 512), F32), ("msg", (16, 128), F32), ("msgs", (4, 16, 128), F32),
    ("side", (64, 512), BF16), ("east", (64, 512), BF16), ("upper", (4, 24, 512), BF16), ("corner", (16, 512), BF16),
    ("sst", (8, 128), F32), ("over", (8, 128), F32), ("table", (16, 8, 128), F32), ("rows", (128, 8, 64), F32),
    ("bias", (64, 1024), F32), ("last", (64, 512), F32), ("mixed", (16, 24, 512), F32), ("norm", (6, 8, 8, 512), F32), ("q", (192, 512), BF16),
    ("k", (192, 512), BF16), ("v", (192, 512), BF16), ("att", (192, 512), BF16), ("above", (3, 32, 256), BF16),
    ("below", (3, 32, 256), BF16), ("leave", (2, 88, 256), BF16), ("cols", (2, 88, 256), BF16),
    ("pad", (2, 22, 48, 128), F32), ("pe", (64, 512), BF16), ("flux", (16, 384), BF16),
    ("near", (2, 16, 384), BF16), ("top", (16, 128), BF16), ("rim", (16, 128), BF16),
    ("tops", (3, 16, 128), BF16), ("edge", (2, 16, 128), BF16), ("spread", (64, 384), BF16), ("conv", (16, 32, 256), F32), ("pre", (512, 256), F32), ("rate", (512, 256), F32),
)
RESULTS = (
    ("cyc", (16, 24, 512), BF16), ("west", (64, 512), BF16), ("south", (4, 24, 512), BF16), ("sw", (16, 512), BF16),
    ("out", (16, 32, 256), BF16),
)


def spread(x):
    patch = iota((64, 384), 0)
    x.spread[...] = (iota((64, 384), 1) == 24 * (patch // 4) + patch % 4).astype(BF16)


def pick_flux(x, codes):
    lane = iota((16, 128), 1)
    right = lane >= 64
    edge = dot(x.edge[...].reshape(32, 128)[:, 0:64], x.spread[...], NN)
    west, own, east = x.near[0].astype(F32), x.flux[...].astype(F32), x.near[1].astype(F32)
    heads, bodies = (edge[0:16], west, own), (west, own, east)
    tops = [x.tops[n].astype(F32) for n in range(3)]
    top_heads = (edge[16:32, 256:384], tops[0], tops[1])
    picked = [jnp.zeros((16, 128), F32)] * 3
    for j in range(3):
        patch = lane + 128 * j
        head = column_of(patch) < 4
        at = slice(128 * j, 128 * j + 128)
        for side in range(3):
            tile = jnp.where(head, heads[side][:, at], bodies[side][:, at])
            if j == 2:
                tile = jnp.where(patch >= 288, jnp.where(head, top_heads[side], tops[side]), tile)
            target = jnp.where(right, side * 8 + 2 * j + 1, side * 8 + 2 * j)
            for k in range(3):
                picked[k] += jnp.where(target == codes[k], tile, 0.0)
    picked = [y + pltpu.roll(y, 64, 1) for y in picked]
    return jnp.concatenate([jnp.where(right, picked[1], picked[0]), picked[2][:, 0:64]], axis=1)


def slot_codes(x):
    lo = lax.axis_index("lon")
    nlo = lax.axis_size("lon")
    codes = []
    for k in range(3):
        side = lax.rem(x.owner[0, k] - lo + 1 + nlo, nlo)
        codes.append(jnp.where(k < x.count[0, 0], side * 8 + x.block[0, k], -1))
    return codes


def ocean_rate(x):
    mask = jnp.broadcast_to(mask_row(x.mask[...]), (16, 512)).astype(BF16)
    parts = [jnp.broadcast_to(y, (16, 256)) for y in split3(x.scale[...])]
    row = iota((16, 256), 0)
    scale = jnp.where(row == 0, parts[0], jnp.where(row == 1, parts[1], jnp.where(row == 2, parts[2], 0.0)))
    x.rate[...] = dot(mask, scale.astype(BF16), TN)


def ocean_update(x):
    forcing = dot(pick_flux(x, slot_codes(x)).astype(BF16), x.overlay[...].reshape(192, 512), NN)
    f_hi, f_lo = split2(forcing)
    e_hi, e_lo = split2(x.fenc[...])
    x.pre[...] = x.conv[...].reshape(512, 256) + dot(
        jnp.concatenate([f_hi, f_lo, f_hi], axis=0).astype(BF16),
        jnp.concatenate([e_hi, e_hi, e_lo], axis=0).astype(BF16),
        TN,
    )

    for i in range(4):
        at = slice(128 * i, 128 * i + 128)
        normed = layer_norm(x.pre[at], x.ogain[...], 1e-06).astype(BF16)
        update = jnp.zeros((128, 256), F32)
        for c in range(4):
            cols = slice(256 * c, 256 * c + 256)
            y = dot(normed, x.w1[:, cols], NN)
            hidden = (0.5 * y * (1.0 + lax.erf(y * (0.5**0.5)))).astype(BF16)
            update = update + dot(hidden, x.w2[cols], NN)
        rows = slice(4 * i, 4 * i + 4)
        state = x.ocean[rows].astype(F32).reshape(128, 256)
        x.out[rows] = (state + x.rate[at] * update).astype(BF16).reshape(4, 32, 256)


def assemble(g, x):
    low = low_half((4, 8, 512))
    rows = slice(4 * g, 4 * g + 4)
    body, side = (x.south, x.sw[...]) if g == 3 else (x.cyc.at[rows], x.west[16 * g : 16 * g + 16])
    body = body[...].astype(F32)
    side = unpack(side.astype(F32).reshape(2, 8, 512), False)
    head = jnp.where(low, side, body[:, 0:8])
    x.atm[rows] = jnp.concatenate([head, body[:, 8:24]], axis=1).astype(BF16)


def step_kernel(*refs):
    n = len(OPERANDS)
    given = dict(zip([o[0] for o in OPERANDS], refs[:n]))
    names = [o[0] for o in (*RESULTS, *OPERANDS, *SCRATCH)]
    x = types.SimpleNamespace(**dict(zip(names, refs[n:])))
    load_sem, send_sem, recv_sem = refs[n + len(names) :]

    at = place()
    la = lax.axis_index("lat")
    nla = lax.axis_size("lat")
    wait_barrier = greet([at(*o) for o in PARTNERS])
    loads = {}
    for i, (name, *_) in enumerate(OPERANDS):
        loads[name] = pltpu.make_async_copy(given[name], getattr(x, name), load_sem.at[i])
        loads[name].start()

    def loaded(*names):
        for name in names:
            loads[name].wait()

    copies = []

    def send(src, dst, offset):
        i = len(copies)
        copy = pltpu.make_async_remote_copy(
            src_ref=src, dst_ref=dst, send_sem=send_sem.at[i], recv_sem=recv_sem.at[i],
            device_id=at(*offset), device_id_type=MESH,
        )
        copies.append(copy)
        copy.start()
        return copy

    loaded("ocean", "proj", "mask", "overlay", "owner", "block", "count")
    for half in range(2):
        x.proj8[4 * half : 4 * half + 4] = x.proj[...]
    surface_message(x.owner, x.block, x.count, x.ocean, x.mask, x.overlay, x.proj8, x.msg)
    loaded("tok")
    x.side[...] = pack(x.tok[:, 0:8, :].astype(F32), False).reshape(64, 512).astype(BF16)

    wait_barrier()
    messages = [send(x.msg, x.msgs.at[dj + 1], (0, -dj)) for dj in (2, 1, -1)]
    x.msgs[1] = x.msg[...]
    east_end = send(x.side.at[pl.ds(48, 16)], x.east.at[pl.ds(48, 16)], (0, -1))
    east = send(x.side.at[pl.ds(0, 48)], x.east.at[pl.ds(0, 48)], (0, -1))
    upper = send(x.tok.at[pl.ds(12, 4)], x.upper, (1, 0))

    loaded("grid", "enc", "gain")
    for half in range(2):
        x.enc8[4 * half : 4 * half + 4] = x.enc[...]
    bias_table(x.grid, x.table, x.rows, x.bias)
    edge = la == 0
    a_row = (iota((64, 512), 1) % 64) >= 32
    b_row = iota((64, 512), 0) >= 32
    x.last[...] = jnp.where(edge, jnp.where(a_row != b_row, -1e9, 0.0), 0.0)

    for copy in messages:
        copy.wait_recv()
    sst = gather_surface(x.msgs)
    x.sst[...] = sst[2]
    over = send(x.sst, x.over, (1, 0))
    east_end.wait_recv()
    corner = send(x.east.at[pl.ds(48, 16)], x.corner, (1, 0))
    below = send(x.ocean.at[pl.ds(0, 3)], x.below, (-1, 0))
    above = send(x.ocean.at[pl.ds(13, 3)], x.above, (1, 0))
    x.mixed[...] = add_surface(jnp.concatenate(sst, axis=1), x.enc8).reshape(16, 24, 512)
    gain = x.gain[...].reshape(1, 1, 512)
    east.wait_recv()
    for g in (1, 2, 0):
        normalise(g, x.tok[4 * g : 4 * g + 4], x.east[16 * g : 16 * g + 16], gain, x.mixed, x.norm)
    loaded("wqkv", "bqkv", "wo")
    windows = (x.norm, x.wqkv, x.bqkv, x.wo, x.bias, x.last, x.q, x.k, x.v, x.att)
    attend(0, *windows)
    for g in (1, 2):
        finish(g, x.norm, x.mixed, x.cyc, x.pe.at[pl.ds(16 * g, 16)])
    pieces = [send(x.pe.at[pl.ds(16, 32)], x.west.at[pl.ds(16, 32)], (0, 1))]

    def put(rows, cols, values):
        for h in range(2):
            x.pad[h, rows, cols, :] = values[:, :, 128 * h : 128 * h + 128]

    below.wait_recv()
    above.wait_recv()
    put(slice(3, 19), slice(8, 40), x.ocean[...].astype(F32))
    put(slice(0, 3), slice(8, 40), x.above[...].astype(F32) * (la > 0).astype(F32))
    put(slice(19, 22), slice(8, 40), x.below[...].astype(F32) * (la < nla - 1).astype(F32))
    for h in range(2):
        lanes = slice(128 * h, 128 * h + 128)
        x.leave[0, :, lanes] = pack(x.pad[h, :, 32:40, :], True).reshape(88, 128).astype(BF16)
        x.leave[1, :, lanes] = pack(x.pad[h, :, 8:16, :], False).reshape(88, 128).astype(BF16)
    sides = [send(x.leave.at[0], x.cols.at[0], (0, 1)), send(x.leave.at[1], x.cols.at[1], (0, -1))]
    loaded("scale")
    ocean_rate(x)
    spread(x)

    for copy in (over, upper, corner):
        copy.wait_recv()
    x.mixed[12:16] = add_surface(x.over[...], x.enc8)[32:128].reshape(4, 24, 512)
    normalise(3, x.upper[...], x.corner[...], gain, x.mixed, x.norm)
    attend(1, *windows)
    for g in (3, 0):
        finish(g, x.norm, x.mixed, x.cyc, x.pe.at[pl.ds(16 * g, 16)])
    loaded("fp")
    flux = dot(x.fp[...], x.mixed[...].reshape(384, 512).astype(BF16), NT).astype(BF16)
    x.flux[...] = flux
    x.top[...] = flux[:, 256:384]
    edge = dot(x.fp[...], x.pe[...], NT)
    x.rim[...] = jnp.concatenate([edge, jnp.zeros((16, 64), F32)], axis=1).astype(BF16)
    fluxes = [
        send(x.top, x.tops.at[0], (-1, 1)),
        send(x.rim, x.edge.at[1], (-1, 2)),
        send(x.rim, x.edge.at[0], (0, 2)),
        send(x.top, x.tops.at[2], (-1, -1)),
        send(x.top, x.tops.at[1], (-1, 0)),
        send(x.flux, x.near.at[1], (0, -1)),
        send(x.flux, x.near.at[0], (0, 1)),
    ]
    pieces += [
        send(x.pe.at[pl.ds(0, 16)], x.west.at[pl.ds(0, 16)], (0, 1)),
        send(x.pe.at[pl.ds(48, 16)], x.sw, (-1, 1)),
        send(x.cyc.at[pl.ds(12, 4)], x.south, (-1, 0)),
    ]

    for copy in sides:
        copy.wait_recv()
    for side, high in ((0, True), (1, False)):
        values = unpack(x.cols[side].astype(F32).reshape(11, 8, 256), high)
        put(slice(0, 22), slice(40 * side, 40 * side + 8), values)
    loaded("kernel", "cbias")
    convolve(x.pad, x.kernel, x.cbias, x.conv)

    loaded("fenc", "ogain", "w1", "w2")
    for copy in fluxes:
        copy.wait_recv()
    ocean_update(x)
    for copy in pieces:
        copy.wait_recv()
    for copy in copies:
        copy.wait_send()


def last_kernel(cyc_ref, west_ref, south_ref, sw_ref, out_ref, atm_to, out_to, atm_s, store_sem):
    stores = [pltpu.make_async_copy(out_ref, out_to, store_sem.at[0])]
    stores[0].start()
    x = types.SimpleNamespace(cyc=cyc_ref, west=west_ref, south=south_ref, sw=sw_ref, atm=atm_s)
    for g in range(4):
        assemble(g, x)
        rows = pl.ds(4 * g, 4)
        stores.append(pltpu.make_async_copy(atm_s.at[rows], atm_to.at[rows], store_sem.at[g + 1]))
        stores[-1].start()
    for copy in stores:
        copy.wait()


def last(*results):
    shapes = [((16, 24, 512), BF16), ((16, 32, 256), BF16)]
    return pl.pallas_call(
        last_kernel,
        out_shape=[jax.ShapeDtypeStruct(*s) for s in shapes],
        in_specs=vmem(len(results)),
        out_specs=anywhere(len(shapes)),
        scratch_shapes=[pltpu.VMEM((16, 24, 512), BF16), pltpu.SemaphoreType.DMA((5,))],
        compiler_params=pltpu.CompilerParams(vmem_limit_bytes=24 << 20),
        name="last",
    )(*results)


def step(*operands):
    def copy_of(name, shape, kind):
        return pltpu.SMEM(shape, kind) if name in SCALARS else pltpu.VMEM(shape, kind)

    return pl.pallas_call(
        step_kernel,
        out_shape=[pltpu.VMEM(shape, kind) for _, shape, kind in RESULTS],
        in_specs=[pl.BlockSpec(memory_space=pltpu.HBM)] * len(OPERANDS),
        out_specs=vmem(len(RESULTS)),
        scratch_shapes=[
            *[copy_of(*o) for o in (*OPERANDS, *SCRATCH)],
            pltpu.SemaphoreType.DMA((len(OPERANDS),)), pltpu.SemaphoreType.DMA((COPIES,)), pltpu.SemaphoreType.DMA((COPIES,)),
        ],
        compiler_params=pltpu.CompilerParams(collective_id=0, has_side_effects=True),
        name="step",
    )(*operands)


def local(
    atmos_patch_tokens,
    atmos_norm_gain,
    query_key_value_weight,
    query_key_value_bias,
    relative_bias_grid,
    attention_output_weight,
    flux_projector,
    surface_encoder,
    ocean_cell_state,
    land_sea_mask,
    depthwise_conv_kernel,
    depthwise_conv_bias,
    ocean_norm_gain,
    pointwise_expand,
    pointwise_contract,
    layer_update_scale,
    forcing_encoder,
    surface_projector,
    overlay_area_weight,
    owners,
    owner_tile_blocks,
    counts,
):
    owners = owners.reshape(1, 3)
    blocks = owner_tile_blocks.reshape(1, 3)
    overlay = overlay_area_weight.reshape(3, 64, 512)
    results = step(
        ocean_cell_state, surface_projector.T, land_sea_mask, overlay, owners, blocks, counts, atmos_patch_tokens,
        relative_bias_grid, surface_encoder, atmos_norm_gain.reshape(1, 512), query_key_value_weight, query_key_value_bias,
        attention_output_weight, flux_projector.T, depthwise_conv_kernel, depthwise_conv_bias.reshape(1, 256), forcing_encoder,
        ocean_norm_gain.reshape(1, 256), pointwise_expand, pointwise_contract, layer_update_scale.reshape(1, 256),
    )
    return last(*results)


def solution(mesh):
    rep = P()
    placed = (
        P("lat", "lon", None), rep, rep, rep, rep, rep, rep, rep, P("lat", "lon", None), P("lat", "lon"),
        rep, rep, rep, rep, rep, rep, rep, rep, P("lat", "lon", None, None, None),
        P("lat", "lon", None), P("lat", "lon", None), P("lat", "lon"),
    )
    return jax.shard_map(
        local,
        mesh=mesh,
        in_specs=placed,
        out_specs=(P("lat", "lon", None), P("lat", "lon", None)),
        check_vma=False,
    )
```

```python
import types

import jax
import jax.numpy as jnp
from jax import lax
from jax.experimental import pallas as pl
from jax.experimental.pallas import tpu as pltpu
from jax.sharding import PartitionSpec as P

F32 = jnp.float32
BF16 = jnp.bfloat16
MESH = pl.DeviceIdType.MESH
HEADS = 16
HALF = 8
WIN = 8
NT = (((1,), (1,)), ((), ()))
TN = (((0,), (0,)), ((), ()))
NN = (((1,), (0,)), ((), ()))


def dot(a, b, dims):
    return lax.dot_general(a, b, dims, preferred_element_type=F32)


def iota(shape, dim):
    return lax.broadcasted_iota(jnp.int32, shape, dim)


def low_half(shape):
    return iota(shape, len(shape) - 2) % 8 < 4


def turn(x):
    return pltpu.roll(x, 4, x.ndim - 2)


def pack(x, high):
    n, _, lanes = x.shape
    x = x.reshape(n // 2, 2, 8, lanes)
    even, odd = x[:, 0], x[:, 1]
    if high:
        even = turn(even)
    else:
        odd = turn(odd)
    return jnp.where(low_half(even.shape), even, odd)


def unpack(x, high):
    n, _, lanes = x.shape
    other = turn(x)
    pair = (other, x) if high else (x, other)
    return jnp.stack(pair, axis=1).reshape(2 * n, 8, lanes)


def split2(x):
    top = x.astype(BF16).astype(F32)
    return top, x - top


def split3(x):
    top, rest = split2(x)
    middle, last = split2(rest)
    return top, middle, last


def greet(partners):
    barrier = pltpu.get_barrier_semaphore()
    for device in partners:
        pl.semaphore_signal(barrier, inc=1, device_id=device, device_id_type=MESH)
    return lambda: pl.semaphore_wait(barrier, len(partners))


def place():
    la, lo = lax.axis_index("lat"), lax.axis_index("lon")
    nla, nlo = lax.axis_size("lat"), lax.axis_size("lon")
    return lambda di, dj: (lax.rem(la + di + nla, nla), lax.rem(lo + dj + nlo, nlo))


def vmem(n):
    return [pl.BlockSpec(memory_space=pltpu.VMEM)] * n


def smem(n):
    return [pl.BlockSpec(memory_space=pltpu.SMEM)] * n


def anywhere(n):
    return [pl.BlockSpec(memory_space=pl.ANY)] * n


def layer_norm(x, gain, epsilon):
    average = jnp.mean(x, axis=-1, keepdims=True)
    centred = x - average
    spread = jnp.mean(centred * centred, axis=-1, keepdims=True)
    return centred * lax.rsqrt(spread + epsilon) * gain


def column_of(patch):
    p = patch.astype(F32)
    return p - 24.0 * jnp.floor((p + 0.5) * (1.0 / 24.0))


def mask_row(mask):
    wide = jnp.concatenate([mask.astype(F32), jnp.zeros((16, 96), F32)], axis=1)
    moved = [wide if q == 0 else pltpu.roll(wide, 32 * q, 1) for q in range(4)]
    parts = [sum(moved[q][4 * j + q : 4 * j + q + 1] for q in range(4)) for j in range(4)]
    return jnp.concatenate(parts, axis=1)


PARTNERS = [(0, 1), (0, -1), (0, 2), (0, -2), (1, 0), (-1, 0)]
COPIES = 32


def surface_message(owner_ref, block_ref, count_ref, ocean_ref, mask_ref, overlay_ref, proj_s, msg_s):
    lo = lax.axis_index("lon")
    nlo = lax.axis_size("lon")
    parts = jnp.concatenate(split3(proj_s[...]), axis=0).astype(BF16)
    surf = dot(parts, ocean_ref[...].reshape(512, 256), NT)
    surf = ((surf[0:8] + surf[8:16] + surf[16:24]) * mask_row(mask_ref[...])).astype(BF16)
    row = iota((8, 128), 0)
    twice = []
    codes = jnp.full((8, 128), -1.0, F32)
    for k in range(3):
        block = overlay_ref[k]
        twice.append(dot(surf, jnp.concatenate([block, block], axis=0), NT))
        side = lax.rem(owner_ref[0, k] - lo + 1 + nlo, nlo)
        code = jnp.where(k < count_ref[0, 0], side * 8 + block_ref[0, k], -1).astype(F32)
        codes = jnp.where(row == 4 + k, code, codes)
    msg_s[0:8] = jnp.where(row < 4, twice[0], twice[1])
    msg_s[8:16] = jnp.where(row < 4, twice[2], codes)


def gather_surface(msgs_ref):
    upper = iota((8, 128), 0) < 4
    right = iota((8, 128), 1) >= 64
    tiles = []
    for tile in range(2):
        sums = [jnp.zeros((8, 128), F32)] * 3
        for side in range(3):
            slot = tile - side + 2
            a = msgs_ref[slot, 0:8, :]
            b = msgs_ref[slot, 8:16, :]
            code_a = jnp.where(upper, b[4:5], b[5:6])
            code_b = jnp.where(upper, b[6:7], -1.0)
            for j in range(3):
                target = jnp.where(right, side * 8.0 + 2 * j + 1, side * 8.0 + 2 * j)
                sums[j] += jnp.where(code_a == target, a, 0.0) + jnp.where(code_b == target, b, 0.0)
        tiles.append(sums)
    return [
        jnp.where(column_of(iota((8, 128), 1) + 128 * j) < 4, tiles[1][j], tiles[0][j]) for j in range(3)
    ]


def bias_table(grid_ref, table_s, rows_s, bias_s):
    grid = jnp.concatenate([grid_ref[...], jnp.zeros((16, 31), F32)], axis=1)
    for ra in range(8):
        rolled = grid if ra == 0 else pltpu.roll(grid, 256 - 15 * ra, 1)
        table_s[:, ra, :] = rolled[:, 0:128]
    parts = [x.astype(BF16) for x in split3(table_s[...].reshape(128, 128))]
    entry = iota((128, 64), 0)
    lane = iota((128, 64), 1)
    for ca in range(8):
        chosen = (entry == (7 - lane // 8) * 15 + ca - lane % 8 + 7).astype(BF16)
        found = (dot(parts[0], chosen, NN) + dot(parts[1], chosen, NN)) + dot(parts[2], chosen, NN)
        rows_s[:, ca, :] = found
    for part in range(8):
        rows = rows_s[16 * part : 16 * part + 16].reshape(128, 64)
        bias_s[:, 128 * part : 128 * part + 128] = rows.T


def add_surface(sst, enc_s):
    s_hi, s_lo = split2(sst)
    e_hi, e_lo = split2(enc_s[...])
    left = jnp.concatenate([s_hi, s_lo, s_hi], axis=0).astype(BF16)
    right = jnp.concatenate([e_hi, e_hi, e_lo], axis=0).astype(BF16)
    return dot(left, right, TN)


def normalise(g, tokens, side, gain, mixed_s, norm_s):
    low = low_half((4, 8, 512))
    rows = slice(4 * g, 4 * g + 4)
    tokens = tokens.astype(F32)
    side = unpack(side.astype(F32).reshape(2, 8, 512), False)
    head = jnp.where(low, side, tokens[:, 0:8])
    tokens = jnp.concatenate([head, tokens[:, 8:24]], axis=1)
    mixed = (tokens + mixed_s[rows]).astype(BF16).astype(F32)
    mixed_s[rows] = mixed
    normed = layer_norm(mixed, gain, 1e-05)
    turned = [turn(normed[:, 8 * b : 8 * b + 8]) for b in range(3)]
    w_row, w_start = WINDOW_OF[g]
    for b in range(3):
        norm_s[w_row * 3 + b, w_start : w_start + 4] = jnp.where(low, turned[b], turned[(b + 1) % 3])


WINDOW_OF = ((1, 4), (0, 0), (0, 4), (1, 0))


def attend(w_row, norm_s, wqkv_s, bqkv_ref, wo_s, bias_s, last_s, q_s, k_s, v_s, att_s):
    rows = norm_s[3 * w_row : 3 * w_row + 3].reshape(192, 512).astype(BF16)
    for part, ref in enumerate((q_s, k_s, v_s)):
        cols = slice(512 * part, 512 * part + 512)
        value = dot(rows, wqkv_s[:, cols], NN) + bqkv_ref[cols].reshape(1, 512)
        if part == 0:
            value = value * 32 ** (-0.5)
        ref[...] = value.astype(BF16)
    own = (iota((8, 1, 256), 2) // 32) == iota((8, 1, 256), 0)
    first_head = iota((64, 128), 0) < 32
    for w in range(3):
        at = slice(64 * w, 64 * w + 64)
        for g in range(2):
            lanes = slice(256 * g, 256 * g + 256)
            queries = jnp.where(own, q_s[at, lanes][None], jnp.zeros((), BF16)).reshape(512, 256)
            scores = dot(k_s[at, lanes], queries, NT) + bias_s[:, 512 * g : 512 * g + 512]
            if w_row == 1:
                scores = scores + last_s[...]
            scores = jnp.exp(scores - jnp.max(scores, axis=0, keepdims=True))
            weights = (scores * (1.0 / jnp.sum(scores, axis=0, keepdims=True))).astype(BF16)
            values = v_s[at, lanes].astype(F32).T.astype(BF16)
            found = []
            for pair in range(4):
                both = dot(values[64 * pair : 64 * pair + 64], weights[:, 128 * pair : 128 * pair + 128], NN)
                found.append(jnp.where(first_head, both, pltpu.roll(both, 64, 1)))
            att_s[at, lanes] = jnp.concatenate(found, axis=0).T[0:64].astype(BF16)
    projected = dot(att_s[...], wo_s[...], NN).astype(BF16).astype(F32)
    norm_s[3 * w_row : 3 * w_row + 3] = projected.reshape(3, 8, 8, 512)


def finish(g, norm_s, mixed_s, cyc_ref, side_ref):
    w_row, w_start = WINDOW_OF[g]
    turned = [turn(norm_s[w_row * 3 + b, w_start : w_start + 4]) for b in range(3)]
    low = low_half((4, 8, 512))
    back = jnp.concatenate([jnp.where(low, turned[b - 1], turned[b]) for b in range(3)], axis=1)
    rows = slice(4 * g, 4 * g + 4)
    result = (mixed_s[rows] + back).astype(BF16)
    mixed_s[rows] = result.astype(F32)
    cyc_ref[rows] = result
    side_ref[...] = pack(result.astype(F32)[:, 0:8], False).reshape(16, 512).astype(BF16)


def convolve(pad_s, kernel_ref, cbias_ref, conv_ref):
    def band(i, carry):
        start = i * 8
        for h in range(2):
            lanes = slice(128 * h, 128 * h + 128)
            first_term = jnp.broadcast_to(cbias_ref[:, lanes], (8, 128))
            for b in range(4):
                sums = [first_term] * 8
                for v in range(7):
                    col = 8 * b + v + 5
                    cells = [pad_s[h, start + r, col : col + 8, :] for r in range(14)]
                    for u in range(7):
                        tap = kernel_ref[u, v : v + 1, lanes]
                        for r in range(8):
                            sums[r] = sums[r] + tap * cells[r + u]
                for r in range(8):
                    conv_ref[start + r, 8 * b : 8 * b + 8, lanes] = sums[r]
        return carry

    lax.fori_loop(0, 2, band, 0)


OPERANDS = (
    ("ocean", (16, 32, 256), BF16), ("proj", (4, 256), F32), ("mask", (16, 32), jnp.int32), ("overlay", (3, 64, 512), BF16),
    ("owner", (1, 3), jnp.int32), ("block", (1, 3), jnp.int32), ("count", (1, 1), jnp.int32), ("tok", (16, 24, 512), BF16),
    ("grid", (16, 225), F32), ("enc", (4, 512), F32), ("gain", (1, 512), F32), ("wqkv", (512, 1536), BF16),
    ("bqkv", (1536,), F32), ("wo", (512, 512), BF16), ("fp", (16, 512), BF16), ("kernel", (7, 7, 256), F32),
    ("cbias", (1, 256), F32), ("fenc", (16, 256), F32), ("ogain", (1, 256), F32), ("w1", (256, 1024), BF16),
    ("w2", (1024, 256), BF16), ("scale", (1, 256), F32),
)
SCALARS = ("owner", "block", "count")
SCRATCH = (
    ("proj8", (8, 256), F32), ("enc8", (8, 512), F32), ("msg", (16, 128), F32), ("msgs", (4, 16, 128), F32),
    ("side", (64, 512), BF16), ("east", (64, 512), BF16), ("upper", (4, 24, 512), BF16), ("corner", (16, 512), BF16),
    ("sst", (8, 128), F32), ("over", (8, 128), F32), ("table", (16, 8, 128), F32), ("rows", (128, 8, 64), F32),
    ("bias", (64, 1024), F32), ("last", (64, 512), F32), ("mixed", (16, 24, 512), F32), ("norm", (6, 8, 8, 512), F32), ("q", (192, 512), BF16),
    ("k", (192, 512), BF16), ("v", (192, 512), BF16), ("att", (192, 512), BF16), ("above", (3, 32, 256), BF16),
    ("below", (3, 32, 256), BF16), ("leave", (2, 88, 256), BF16), ("cols", (2, 88, 256), BF16),
    ("pad", (2, 22, 48, 128), F32), ("pe", (64, 512), BF16), ("flux", (16, 384), BF16),
    ("near", (2, 16, 384), BF16), ("top", (16, 128), BF16), ("rim", (16, 128), BF16),
    ("tops", (3, 16, 128), BF16), ("edge", (2, 16, 128), BF16), ("spread", (64, 384), BF16), ("conv", (16, 32, 256), F32), ("pre", (512, 256), F32), ("rate", (512, 256), F32),
)
RESULTS = (
    ("cyc", (16, 24, 512), BF16), ("west", (64, 512), BF16), ("south", (4, 24, 512), BF16), ("sw", (16, 512), BF16),
    ("out", (16, 32, 256), BF16),
)


def spread(x):
    patch = iota((64, 384), 0)
    x.spread[...] = (iota((64, 384), 1) == 24 * (patch // 4) + patch % 4).astype(BF16)


def pick_flux(x, codes):
    lane = iota((16, 128), 1)
    right = lane >= 64
    edge = dot(x.edge[...].reshape(32, 128)[:, 0:64], x.spread[...], NN)
    west, own, east = x.near[0].astype(F32), x.flux[...].astype(F32), x.near[1].astype(F32)
    heads, bodies = (edge[0:16], west, own), (west, own, east)
    tops = [x.tops[n].astype(F32) for n in range(3)]
    top_heads = (edge[16:32, 256:384], tops[0], tops[1])
    picked = [jnp.zeros((16, 128), F32)] * 3
    for j in range(3):
        patch = lane + 128 * j
        head = column_of(patch) < 4
        at = slice(128 * j, 128 * j + 128)
        for side in range(3):
            tile = jnp.where(head, heads[side][:, at], bodies[side][:, at])
            if j == 2:
                tile = jnp.where(patch >= 288, jnp.where(head, top_heads[side], tops[side]), tile)
            target = jnp.where(right, side * 8 + 2 * j + 1, side * 8 + 2 * j)
            for k in range(3):
                picked[k] += jnp.where(target == codes[k], tile, 0.0)
    picked = [y + pltpu.roll(y, 64, 1) for y in picked]
    return jnp.concatenate([jnp.where(right, picked[1], picked[0]), picked[2][:, 0:64]], axis=1)


def slot_codes(x):
    lo = lax.axis_index("lon")
    nlo = lax.axis_size("lon")
    codes = []
    for k in range(3):
        side = lax.rem(x.owner[0, k] - lo + 1 + nlo, nlo)
        codes.append(jnp.where(k < x.count[0, 0], side * 8 + x.block[0, k], -1))
    return codes


def ocean_rate(x):
    mask = jnp.broadcast_to(mask_row(x.mask[...]), (16, 512)).astype(BF16)
    parts = [jnp.broadcast_to(y, (16, 256)) for y in split3(x.scale[...])]
    row = iota((16, 256), 0)
    scale = jnp.where(row == 0, parts[0], jnp.where(row == 1, parts[1], jnp.where(row == 2, parts[2], 0.0)))
    x.rate[...] = dot(mask, scale.astype(BF16), TN)


def ocean_update(x):
    forcing = dot(pick_flux(x, slot_codes(x)).astype(BF16), x.overlay[...].reshape(192, 512), NN)
    f_hi, f_lo = split2(forcing)
    e_hi, e_lo = split2(x.fenc[...])
    x.pre[...] = x.conv[...].reshape(512, 256) + dot(
        jnp.concatenate([f_hi, f_lo, f_hi], axis=0).astype(BF16),
        jnp.concatenate([e_hi, e_hi, e_lo], axis=0).astype(BF16),
        TN,
    )

    for i in range(4):
        at = slice(128 * i, 128 * i + 128)
        normed = layer_norm(x.pre[at], x.ogain[...], 1e-06).astype(BF16)
        update = jnp.zeros((128, 256), F32)
        for c in range(4):
            cols = slice(256 * c, 256 * c + 256)
            y = dot(normed, x.w1[:, cols], NN)
            hidden = (0.5 * y * (1.0 + lax.erf(y * (0.5**0.5)))).astype(BF16)
            update = update + dot(hidden, x.w2[cols], NN)
        rows = slice(4 * i, 4 * i + 4)
        state = x.ocean[rows].astype(F32).reshape(128, 256)
        x.out[rows] = (state + x.rate[at] * update).astype(BF16).reshape(4, 32, 256)


def assemble(g, x):
    low = low_half((4, 8, 512))
    rows = slice(4 * g, 4 * g + 4)
    body, side = (x.south, x.sw[...]) if g == 3 else (x.cyc.at[rows], x.west[16 * g : 16 * g + 16])
    body = body[...].astype(F32)
    side = unpack(side.astype(F32).reshape(2, 8, 512), False)
    head = jnp.where(low, side, body[:, 0:8])
    x.atm[rows] = jnp.concatenate([head, body[:, 8:24]], axis=1).astype(BF16)


def step_kernel(*refs):
    n = len(OPERANDS)
    given = dict(zip([o[0] for o in OPERANDS], refs[:n]))
    names = [o[0] for o in (*RESULTS, *OPERANDS, *SCRATCH)]
    x = types.SimpleNamespace(**dict(zip(names, refs[n:])))
    load_sem, send_sem, recv_sem = refs[n + len(names) :]

    at = place()
    la = lax.axis_index("lat")
    nla = lax.axis_size("lat")
    wait_barrier = greet([at(*o) for o in PARTNERS])
    loads = {}
    for i, (name, *_) in enumerate(OPERANDS):
        loads[name] = pltpu.make_async_copy(given[name], getattr(x, name), load_sem.at[i])
        loads[name].start()

    def loaded(*names):
        for name in names:
            loads[name].wait()

    copies = []

    def send(src, dst, offset):
        i = len(copies)
        copy = pltpu.make_async_remote_copy(
            src_ref=src, dst_ref=dst, send_sem=send_sem.at[i], recv_sem=recv_sem.at[i],
            device_id=at(*offset), device_id_type=MESH,
        )
        copies.append(copy)
        copy.start()
        return copy

    loaded("ocean", "proj", "mask", "overlay", "owner", "block", "count")
    for half in range(2):
        x.proj8[4 * half : 4 * half + 4] = x.proj[...]
    surface_message(x.owner, x.block, x.count, x.ocean, x.mask, x.overlay, x.proj8, x.msg)
    loaded("tok")
    x.side[...] = pack(x.tok[:, 0:8, :].astype(F32), False).reshape(64, 512).astype(BF16)

    wait_barrier()
    messages = [send(x.msg, x.msgs.at[dj + 1], (0, -dj)) for dj in (2, 1, -1)]
    x.msgs[1] = x.msg[...]
    east_end = send(x.side.at[pl.ds(48, 16)], x.east.at[pl.ds(48, 16)], (0, -1))
    east = send(x.side.at[pl.ds(0, 48)], x.east.at[pl.ds(0, 48)], (0, -1))
    upper = send(x.tok.at[pl.ds(12, 4)], x.upper, (1, 0))
    above = send(x.ocean.at[pl.ds(13, 3)], x.above, (1, 0))
    below = send(x.ocean.at[pl.ds(0, 3)], x.below, (-1, 0))

    loaded("grid", "enc", "gain")
    for half in range(2):
        x.enc8[4 * half : 4 * half + 4] = x.enc[...]
    bias_table(x.grid, x.table, x.rows, x.bias)
    edge = la == 0
    a_row = (iota((64, 512), 1) % 64) >= 32
    b_row = iota((64, 512), 0) >= 32
    x.last[...] = jnp.where(edge, jnp.where(a_row != b_row, -1e9, 0.0), 0.0)

    for copy in messages:
        copy.wait_recv()
    sst = gather_surface(x.msgs)
    x.sst[...] = sst[2]
    over = send(x.sst, x.over, (1, 0))
    east_end.wait_recv()
    corner = send(x.east.at[pl.ds(48, 16)], x.corner, (1, 0))
    x.mixed[...] = add_surface(jnp.concatenate(sst, axis=1), x.enc8).reshape(16, 24, 512)
    gain = x.gain[...].reshape(1, 1, 512)
    east.wait_recv()
    for g in (1, 2, 0):
        normalise(g, x.tok[4 * g : 4 * g + 4], x.east[16 * g : 16 * g + 16], gain, x.mixed, x.norm)
    loaded("wqkv", "bqkv", "wo")
    windows = (x.norm, x.wqkv, x.bqkv, x.wo, x.bias, x.last, x.q, x.k, x.v, x.att)
    attend(0, *windows)
    for g in (1, 2):
        finish(g, x.norm, x.mixed, x.cyc, x.pe.at[pl.ds(16 * g, 16)])

    def put(rows, cols, values):
        for h in range(2):
            x.pad[h, rows, cols, :] = values[:, :, 128 * h : 128 * h + 128]

    below.wait_recv()
    above.wait_recv()
    put(slice(3, 19), slice(8, 40), x.ocean[...].astype(F32))
    put(slice(0, 3), slice(8, 40), x.above[...].astype(F32) * (la > 0).astype(F32))
    put(slice(19, 22), slice(8, 40), x.below[...].astype(F32) * (la < nla - 1).astype(F32))
    for h in range(2):
        lanes = slice(128 * h, 128 * h + 128)
        x.leave[0, :, lanes] = pack(x.pad[h, :, 32:40, :], True).reshape(88, 128).astype(BF16)
        x.leave[1, :, lanes] = pack(x.pad[h, :, 8:16, :], False).reshape(88, 128).astype(BF16)
    sides = [send(x.leave.at[0], x.cols.at[0], (0, 1)), send(x.leave.at[1], x.cols.at[1], (0, -1))]
    loaded("scale")
    ocean_rate(x)
    spread(x)

    for copy in (over, upper, corner):
        copy.wait_recv()
    x.mixed[12:16] = add_surface(x.over[...], x.enc8)[32:128].reshape(4, 24, 512)
    normalise(3, x.upper[...], x.corner[...], gain, x.mixed, x.norm)
    attend(1, *windows)
    for g in (3, 0):
        finish(g, x.norm, x.mixed, x.cyc, x.pe.at[pl.ds(16 * g, 16)])
    loaded("fp")
    flux = dot(x.fp[...], x.mixed[...].reshape(384, 512).astype(BF16), NT).astype(BF16)
    x.flux[...] = flux
    x.top[...] = flux[:, 256:384]
    edge = dot(x.fp[...], x.pe[...], NT)
    x.rim[...] = jnp.concatenate([edge, jnp.zeros((16, 64), F32)], axis=1).astype(BF16)
    fluxes = [
        send(x.top, x.tops.at[0], (-1, 1)),
        send(x.rim, x.edge.at[1], (-1, 2)),
        send(x.rim, x.edge.at[0], (0, 2)),
        send(x.top, x.tops.at[2], (-1, -1)),
        send(x.top, x.tops.at[1], (-1, 0)),
        send(x.flux, x.near.at[1], (0, -1)),
        send(x.flux, x.near.at[0], (0, 1)),
    ]
    pieces = [
        send(x.pe.at[pl.ds(0, 48)], x.west.at[pl.ds(0, 48)], (0, 1)),
        send(x.pe.at[pl.ds(48, 16)], x.sw, (-1, 1)),
        send(x.cyc.at[pl.ds(12, 4)], x.south, (-1, 0)),
    ]

    for copy in sides:
        copy.wait_recv()
    for side, high in ((0, True), (1, False)):
        values = unpack(x.cols[side].astype(F32).reshape(11, 8, 256), high)
        put(slice(0, 22), slice(40 * side, 40 * side + 8), values)
    loaded("kernel", "cbias")
    convolve(x.pad, x.kernel, x.cbias, x.conv)

    loaded("fenc", "ogain", "w1", "w2")
    for copy in fluxes:
        copy.wait_recv()
    ocean_update(x)
    for copy in pieces:
        copy.wait_recv()
    for copy in copies:
        copy.wait_send()


def last_kernel(cyc_ref, west_ref, south_ref, sw_ref, out_ref, atm_to, out_to, atm_s, store_sem):
    stores = [pltpu.make_async_copy(out_ref, out_to, store_sem.at[0])]
    stores[0].start()
    x = types.SimpleNamespace(cyc=cyc_ref, west=west_ref, south=south_ref, sw=sw_ref, atm=atm_s)
    for g in range(4):
        assemble(g, x)
        rows = pl.ds(4 * g, 4)
        stores.append(pltpu.make_async_copy(atm_s.at[rows], atm_to.at[rows], store_sem.at[g + 1]))
        stores[-1].start()
    for copy in stores:
        copy.wait()


def last(*results):
    shapes = [((16, 24, 512), BF16), ((16, 32, 256), BF16)]
    return pl.pallas_call(
        last_kernel,
        out_shape=[jax.ShapeDtypeStruct(*s) for s in shapes],
        in_specs=vmem(len(results)),
        out_specs=anywhere(len(shapes)),
        scratch_shapes=[pltpu.VMEM((16, 24, 512), BF16), pltpu.SemaphoreType.DMA((5,))],
        compiler_params=pltpu.CompilerParams(vmem_limit_bytes=24 << 20),
        name="last",
    )(*results)


def step(*operands):
    def copy_of(name, shape, kind):
        return pltpu.SMEM(shape, kind) if name in SCALARS else pltpu.VMEM(shape, kind)

    return pl.pallas_call(
        step_kernel,
        out_shape=[pltpu.VMEM(shape, kind) for _, shape, kind in RESULTS],
        in_specs=[pl.BlockSpec(memory_space=pltpu.HBM)] * len(OPERANDS),
        out_specs=vmem(len(RESULTS)),
        scratch_shapes=[
            *[copy_of(*o) for o in (*OPERANDS, *SCRATCH)],
            pltpu.SemaphoreType.DMA((len(OPERANDS),)), pltpu.SemaphoreType.DMA((COPIES,)), pltpu.SemaphoreType.DMA((COPIES,)),
        ],
        compiler_params=pltpu.CompilerParams(collective_id=0, has_side_effects=True),
        name="step",
    )(*operands)


def local(
    atmos_patch_tokens,
    atmos_norm_gain,
    query_key_value_weight,
    query_key_value_bias,
    relative_bias_grid,
    attention_output_weight,
    flux_projector,
    surface_encoder,
    ocean_cell_state,
    land_sea_mask,
    depthwise_conv_kernel,
    depthwise_conv_bias,
    ocean_norm_gain,
    pointwise_expand,
    pointwise_contract,
    layer_update_scale,
    forcing_encoder,
    surface_projector,
    overlay_area_weight,
    owners,
    owner_tile_blocks,
    counts,
):
    owners = owners.reshape(1, 3)
    blocks = owner_tile_blocks.reshape(1, 3)
    overlay = overlay_area_weight.reshape(3, 64, 512)
    results = step(
        ocean_cell_state, surface_projector.T, land_sea_mask, overlay, owners, blocks, counts, atmos_patch_tokens,
        relative_bias_grid, surface_encoder, atmos_norm_gain.reshape(1, 512), query_key_value_weight, query_key_value_bias,
        attention_output_weight, flux_projector.T, depthwise_conv_kernel, depthwise_conv_bias.reshape(1, 256), forcing_encoder,
        ocean_norm_gain.reshape(1, 256), pointwise_expand, pointwise_contract, layer_update_scale.reshape(1, 256),
    )
    return last(*results)


def solution(mesh):
    rep = P()
    placed = (
        P("lat", "lon", None), rep, rep, rep, rep, rep, rep, rep, P("lat", "lon", None), P("lat", "lon"),
        rep, rep, rep, rep, rep, rep, rep, rep, P("lat", "lon", None, None, None),
        P("lat", "lon", None), P("lat", "lon", None), P("lat", "lon"),
    )
    return jax.shard_map(
        local,
        mesh=mesh,
        in_specs=placed,
        out_specs=(P("lat", "lon", None), P("lat", "lon", None)),
        check_vma=False,
    )
```

```python
import types

import jax
import jax.numpy as jnp
from jax import lax
from jax.experimental import pallas as pl
from jax.experimental.pallas import tpu as pltpu
from jax.sharding import PartitionSpec as P

F32 = jnp.float32
BF16 = jnp.bfloat16
MESH = pl.DeviceIdType.MESH
HEADS = 16
HALF = 8
WIN = 8
NT = (((1,), (1,)), ((), ()))
TN = (((0,), (0,)), ((), ()))
NN = (((1,), (0,)), ((), ()))


def dot(a, b, dims):
    return lax.dot_general(a, b, dims, preferred_element_type=F32)


def iota(shape, dim):
    return lax.broadcasted_iota(jnp.int32, shape, dim)


def low_half(shape):
    return iota(shape, len(shape) - 2) % 8 < 4


def turn(x):
    return pltpu.roll(x, 4, x.ndim - 2)


def pack(x, high):
    n, _, lanes = x.shape
    x = x.reshape(n // 2, 2, 8, lanes)
    even, odd = x[:, 0], x[:, 1]
    if high:
        even = turn(even)
    else:
        odd = turn(odd)
    return jnp.where(low_half(even.shape), even, odd)


def unpack(x, high):
    n, _, lanes = x.shape
    other = turn(x)
    pair = (other, x) if high else (x, other)
    return jnp.stack(pair, axis=1).reshape(2 * n, 8, lanes)


def split2(x):
    top = x.astype(BF16).astype(F32)
    return top, x - top


def split3(x):
    top, rest = split2(x)
    middle, last = split2(rest)
    return top, middle, last


def greet(partners):
    barrier = pltpu.get_barrier_semaphore()
    for device in partners:
        pl.semaphore_signal(barrier, inc=1, device_id=device, device_id_type=MESH)
    return lambda: pl.semaphore_wait(barrier, len(partners))


def place():
    la, lo = lax.axis_index("lat"), lax.axis_index("lon")
    nla, nlo = lax.axis_size("lat"), lax.axis_size("lon")
    return lambda di, dj: (lax.rem(la + di + nla, nla), lax.rem(lo + dj + nlo, nlo))


def vmem(n):
    return [pl.BlockSpec(memory_space=pltpu.VMEM)] * n


def smem(n):
    return [pl.BlockSpec(memory_space=pltpu.SMEM)] * n


def anywhere(n):
    return [pl.BlockSpec(memory_space=pl.ANY)] * n


def layer_norm(x, gain, epsilon):
    average = jnp.mean(x, axis=-1, keepdims=True)
    centred = x - average
    spread = jnp.mean(centred * centred, axis=-1, keepdims=True)
    return centred * lax.rsqrt(spread + epsilon) * gain


def column_of(patch):
    p = patch.astype(F32)
    return p - 24.0 * jnp.floor((p + 0.5) * (1.0 / 24.0))


def mask_row(mask):
    wide = jnp.concatenate([mask.astype(F32), jnp.zeros((16, 96), F32)], axis=1)
    moved = [wide if q == 0 else pltpu.roll(wide, 32 * q, 1) for q in range(4)]
    parts = [sum(moved[q][4 * j + q : 4 * j + q + 1] for q in range(4)) for j in range(4)]
    return jnp.concatenate(parts, axis=1)


PARTNERS = [(0, 1), (0, -1), (0, 2), (0, -2), (1, 0), (-1, 0)]
COPIES = 32


def surface_message(owner_ref, block_ref, count_ref, ocean_ref, mask_ref, overlay_ref, proj_s, msg_s):
    lo = lax.axis_index("lon")
    nlo = lax.axis_size("lon")
    parts = jnp.concatenate(split3(proj_s[...]), axis=0).astype(BF16)
    surf = dot(parts, ocean_ref[...].reshape(512, 256), NT)
    surf = ((surf[0:8] + surf[8:16] + surf[16:24]) * mask_row(mask_ref[...])).astype(BF16)
    row = iota((8, 128), 0)
    twice = []
    codes = jnp.full((8, 128), -1.0, F32)
    for k in range(3):
        block = overlay_ref[k]
        twice.append(dot(surf, jnp.concatenate([block, block], axis=0), NT))
        side = lax.rem(owner_ref[0, k] - lo + 1 + nlo, nlo)
        code = jnp.where(k < count_ref[0, 0], side * 8 + block_ref[0, k], -1).astype(F32)
        codes = jnp.where(row == 4 + k, code, codes)
    msg_s[0:8] = jnp.where(row < 4, twice[0], twice[1])
    msg_s[8:16] = jnp.where(row < 4, twice[2], codes)


def gather_surface(msgs_ref):
    upper = iota((8, 128), 0) < 4
    right = iota((8, 128), 1) >= 64
    tiles = []
    for tile in range(2):
        sums = [jnp.zeros((8, 128), F32)] * 3
        for side in range(3):
            slot = tile - side + 2
            a = msgs_ref[slot, 0:8, :]
            b = msgs_ref[slot, 8:16, :]
            code_a = jnp.where(upper, b[4:5], b[5:6])
            code_b = jnp.where(upper, b[6:7], -1.0)
            for j in range(3):
                target = jnp.where(right, side * 8.0 + 2 * j + 1, side * 8.0 + 2 * j)
                sums[j] += jnp.where(code_a == target, a, 0.0) + jnp.where(code_b == target, b, 0.0)
        tiles.append(sums)
    return [
        jnp.where(column_of(iota((8, 128), 1) + 128 * j) < 4, tiles[1][j], tiles[0][j]) for j in range(3)
    ]


def bias_table(grid_ref, table_s, rows_s, bias_s):
    grid = jnp.concatenate([grid_ref[...], jnp.zeros((16, 31), F32)], axis=1)
    for ra in range(8):
        rolled = grid if ra == 0 else pltpu.roll(grid, 256 - 15 * ra, 1)
        table_s[:, ra, :] = rolled[:, 0:128]
    parts = [x.astype(BF16) for x in split3(table_s[...].reshape(128, 128))]
    entry = iota((128, 64), 0)
    lane = iota((128, 64), 1)
    for ca in range(8):
        chosen = (entry == (7 - lane // 8) * 15 + ca - lane % 8 + 7).astype(BF16)
        found = (dot(parts[0], chosen, NN) + dot(parts[1], chosen, NN)) + dot(parts[2], chosen, NN)
        rows_s[:, ca, :] = found
    for part in range(8):
        rows = rows_s[16 * part : 16 * part + 16].reshape(128, 64)
        bias_s[:, 128 * part : 128 * part + 128] = rows.T


def add_surface(sst, enc_s):
    s_hi, s_lo = split2(sst)
    e_hi, e_lo = split2(enc_s[...])
    left = jnp.concatenate([s_hi, s_lo, s_hi], axis=0).astype(BF16)
    right = jnp.concatenate([e_hi, e_hi, e_lo], axis=0).astype(BF16)
    return dot(left, right, TN)


def normalise(g, tokens, side, gain, mixed_s, norm_s):
    low = low_half((4, 8, 512))
    rows = slice(4 * g, 4 * g + 4)
    tokens = tokens.astype(F32)
    side = unpack(side.astype(F32).reshape(2, 8, 512), False)
    head = jnp.where(low, side, tokens[:, 0:8])
    tokens = jnp.concatenate([head, tokens[:, 8:24]], axis=1)
    mixed = (tokens + mixed_s[rows]).astype(BF16).astype(F32)
    mixed_s[rows] = mixed
    normed = layer_norm(mixed, gain, 1e-05)
    turned = [turn(normed[:, 8 * b : 8 * b + 8]) for b in range(3)]
    w_row, w_start = WINDOW_OF[g]
    for b in range(3):
        norm_s[w_row * 3 + b, w_start : w_start + 4] = jnp.where(low, turned[b], turned[(b + 1) % 3])


WINDOW_OF = ((1, 4), (0, 0), (0, 4), (1, 0))


def attend(w_row, norm_s, wqkv_s, bqkv_ref, wo_s, bias_s, last_s, q_s, k_s, v_s, att_s):
    rows = norm_s[3 * w_row : 3 * w_row + 3].reshape(192, 512).astype(BF16)
    for part, ref in enumerate((q_s, k_s, v_s)):
        cols = slice(512 * part, 512 * part + 512)
        value = dot(rows, wqkv_s[:, cols], NN) + bqkv_ref[cols].reshape(1, 512)
        if part == 0:
            value = value * 32 ** (-0.5)
        ref[...] = value.astype(BF16)
    own = (iota((8, 1, 256), 2) // 32) == iota((8, 1, 256), 0)
    first_head = iota((64, 128), 0) < 32
    for w in range(3):
        at = slice(64 * w, 64 * w + 64)
        for g in range(2):
            lanes = slice(256 * g, 256 * g + 256)
            queries = jnp.where(own, q_s[at, lanes][None], jnp.zeros((), BF16)).reshape(512, 256)
            scores = dot(k_s[at, lanes], queries, NT) + bias_s[:, 512 * g : 512 * g + 512]
            if w_row == 1:
                scores = scores + last_s[...]
            scores = jnp.exp(scores - jnp.max(scores, axis=0, keepdims=True))
            weights = (scores * (1.0 / jnp.sum(scores, axis=0, keepdims=True))).astype(BF16)
            values = v_s[at, lanes].astype(F32).T.astype(BF16)
            found = []
            for pair in range(4):
                both = dot(values[64 * pair : 64 * pair + 64], weights[:, 128 * pair : 128 * pair + 128], NN)
                found.append(jnp.where(first_head, both, pltpu.roll(both, 64, 1)))
            att_s[at, lanes] = jnp.concatenate(found, axis=0).T[0:64].astype(BF16)
    projected = dot(att_s[...], wo_s[...], NN).astype(BF16).astype(F32)
    norm_s[3 * w_row : 3 * w_row + 3] = projected.reshape(3, 8, 8, 512)


def finish(g, norm_s, mixed_s, cyc_ref, side_ref):
    w_row, w_start = WINDOW_OF[g]
    turned = [turn(norm_s[w_row * 3 + b, w_start : w_start + 4]) for b in range(3)]
    low = low_half((4, 8, 512))
    back = jnp.concatenate([jnp.where(low, turned[b - 1], turned[b]) for b in range(3)], axis=1)
    rows = slice(4 * g, 4 * g + 4)
    result = (mixed_s[rows] + back).astype(BF16)
    mixed_s[rows] = result.astype(F32)
    cyc_ref[rows] = result
    side_ref[...] = pack(result.astype(F32)[:, 0:8], False).reshape(16, 512).astype(BF16)


def convolve(pad_s, kernel_ref, cbias_ref, conv_ref):
    def band(i, carry):
        start = i * 8
        for h in range(2):
            lanes = slice(128 * h, 128 * h + 128)
            first_term = jnp.broadcast_to(cbias_ref[:, lanes], (8, 128))
            for b in range(4):
                sums = [first_term] * 8
                for v in range(7):
                    col = 8 * b + v + 5
                    cells = [pad_s[h, start + r, col : col + 8, :] for r in range(14)]
                    for u in range(7):
                        tap = kernel_ref[u, v : v + 1, lanes]
                        for r in range(8):
                            sums[r] = sums[r] + tap * cells[r + u]
                for r in range(8):
                    conv_ref[start + r, 8 * b : 8 * b + 8, lanes] = sums[r]
        return carry

    lax.fori_loop(0, 2, band, 0)


OPERANDS = (
    ("ocean", (16, 32, 256), BF16), ("proj", (4, 256), F32), ("mask", (16, 32), jnp.int32), ("overlay", (3, 64, 512), BF16),
    ("owner", (1, 3), jnp.int32), ("block", (1, 3), jnp.int32), ("count", (1, 1), jnp.int32), ("tok", (16, 24, 512), BF16),
    ("grid", (16, 225), F32), ("enc", (4, 512), F32), ("gain", (1, 512), F32), ("wqkv", (512, 1536), BF16),
    ("bqkv", (1536,), F32), ("wo", (512, 512), BF16), ("fp", (16, 512), BF16), ("kernel", (7, 7, 256), F32),
    ("cbias", (1, 256), F32), ("fenc", (16, 256), F32), ("ogain", (1, 256), F32), ("w1", (256, 1024), BF16),
    ("w2", (1024, 256), BF16), ("scale", (1, 256), F32),
)
SCALARS = ("owner", "block", "count")
SCRATCH = (
    ("proj8", (8, 256), F32), ("enc8", (8, 512), F32), ("msg", (16, 128), F32), ("msgs", (4, 16, 128), F32),
    ("side", (64, 512), BF16), ("east", (64, 512), BF16), ("upper", (4, 24, 512), BF16), ("corner", (16, 512), BF16),
    ("sst", (8, 128), F32), ("over", (8, 128), F32), ("table", (16, 8, 128), F32), ("rows", (128, 8, 64), F32),
    ("bias", (64, 1024), F32), ("last", (64, 512), F32), ("mixed", (16, 24, 512), F32), ("norm", (6, 8, 8, 512), F32), ("q", (192, 512), BF16),
    ("k", (192, 512), BF16), ("v", (192, 512), BF16), ("att", (192, 512), BF16), ("above", (3, 32, 256), BF16),
    ("below", (3, 32, 256), BF16), ("leave", (2, 88, 256), BF16), ("cols", (2, 88, 256), BF16),
    ("pad", (2, 22, 48, 128), F32), ("pe", (64, 512), BF16), ("flux", (16, 384), BF16),
    ("near", (2, 16, 384), BF16), ("top", (16, 128), BF16), ("rim", (16, 128), BF16),
    ("tops", (3, 16, 128), BF16), ("edge", (2, 16, 128), BF16), ("spread", (64, 384), BF16), ("conv", (16, 32, 256), F32), ("pre", (512, 256), F32), ("rate", (512, 256), F32),
)
RESULTS = (
    ("cyc", (16, 24, 512), BF16), ("west", (64, 512), BF16), ("south", (4, 24, 512), BF16), ("sw", (16, 512), BF16),
    ("out", (16, 32, 256), BF16),
)


def spread(x):
    patch = iota((64, 384), 0)
    x.spread[...] = (iota((64, 384), 1) == 24 * (patch // 4) + patch % 4).astype(BF16)


def pick_flux(x, codes):
    lane = iota((16, 128), 1)
    right = lane >= 64
    edge = dot(x.edge[...].reshape(32, 128)[:, 0:64], x.spread[...], NN)
    west, own, east = x.near[0].astype(F32), x.flux[...].astype(F32), x.near[1].astype(F32)
    heads, bodies = (edge[0:16], west, own), (west, own, east)
    tops = [x.tops[n].astype(F32) for n in range(3)]
    top_heads = (edge[16:32, 256:384], tops[0], tops[1])
    picked = [jnp.zeros((16, 128), F32)] * 3
    for j in range(3):
        patch = lane + 128 * j
        head = column_of(patch) < 4
        at = slice(128 * j, 128 * j + 128)
        for side in range(3):
            tile = jnp.where(head, heads[side][:, at], bodies[side][:, at])
            if j == 2:
                tile = jnp.where(patch >= 288, jnp.where(head, top_heads[side], tops[side]), tile)
            target = jnp.where(right, side * 8 + 2 * j + 1, side * 8 + 2 * j)
            for k in range(3):
                picked[k] += jnp.where(target == codes[k], tile, 0.0)
    picked = [y + pltpu.roll(y, 64, 1) for y in picked]
    return jnp.concatenate([jnp.where(right, picked[1], picked[0]), picked[2][:, 0:64]], axis=1)


def slot_codes(x):
    lo = lax.axis_index("lon")
    nlo = lax.axis_size("lon")
    codes = []
    for k in range(3):
        side = lax.rem(x.owner[0, k] - lo + 1 + nlo, nlo)
        codes.append(jnp.where(k < x.count[0, 0], side * 8 + x.block[0, k], -1))
    return codes


def ocean_rate(x):
    mask = jnp.broadcast_to(mask_row(x.mask[...]), (16, 512)).astype(BF16)
    parts = [jnp.broadcast_to(y, (16, 256)) for y in split3(x.scale[...])]
    row = iota((16, 256), 0)
    scale = jnp.where(row == 0, parts[0], jnp.where(row == 1, parts[1], jnp.where(row == 2, parts[2], 0.0)))
    x.rate[...] = dot(mask, scale.astype(BF16), TN)


def ocean_update(x):
    forcing = dot(pick_flux(x, slot_codes(x)).astype(BF16), x.overlay[...].reshape(192, 512), NN)
    f_hi, f_lo = split2(forcing)
    e_hi, e_lo = split2(x.fenc[...])
    x.pre[...] = x.conv[...].reshape(512, 256) + dot(
        jnp.concatenate([f_hi, f_lo, f_hi], axis=0).astype(BF16),
        jnp.concatenate([e_hi, e_hi, e_lo], axis=0).astype(BF16),
        TN,
    )

    for i in range(4):
        at = slice(128 * i, 128 * i + 128)
        normed = layer_norm(x.pre[at], x.ogain[...], 1e-06).astype(BF16)
        update = jnp.zeros((128, 256), F32)
        for c in range(4):
            cols = slice(256 * c, 256 * c + 256)
            y = dot(normed, x.w1[:, cols], NN)
            hidden = (0.5 * y * (1.0 + lax.erf(y * (0.5**0.5)))).astype(BF16)
            update = update + dot(hidden, x.w2[cols], NN)
        rows = slice(4 * i, 4 * i + 4)
        state = x.ocean[rows].astype(F32).reshape(128, 256)
        x.out[rows] = (state + x.rate[at] * update).astype(BF16).reshape(4, 32, 256)


def assemble(g, x):
    low = low_half((4, 8, 512))
    rows = slice(4 * g, 4 * g + 4)
    body, side = (x.south, x.sw[...]) if g == 3 else (x.cyc.at[rows], x.west[16 * g : 16 * g + 16])
    body = body[...].astype(F32)
    side = unpack(side.astype(F32).reshape(2, 8, 512), False)
    head = jnp.where(low, side, body[:, 0:8])
    x.atm[rows] = jnp.concatenate([head, body[:, 8:24]], axis=1).astype(BF16)


def step_kernel(*refs):
    n = len(OPERANDS)
    given = dict(zip([o[0] for o in OPERANDS], refs[:n]))
    names = [o[0] for o in (*RESULTS, *OPERANDS, *SCRATCH)]
    x = types.SimpleNamespace(**dict(zip(names, refs[n:])))
    load_sem, send_sem, recv_sem = refs[n + len(names) :]

    at = place()
    la = lax.axis_index("lat")
    nla = lax.axis_size("lat")
    wait_barrier = greet([at(*o) for o in PARTNERS])
    loads = {}
    for i, (name, *_) in enumerate(OPERANDS):
        loads[name] = pltpu.make_async_copy(given[name], getattr(x, name), load_sem.at[i])
        loads[name].start()

    def loaded(*names):
        for name in names:
            loads[name].wait()

    copies = []

    def send(src, dst, offset):
        i = len(copies)
        copy = pltpu.make_async_remote_copy(
            src_ref=src, dst_ref=dst, send_sem=send_sem.at[i], recv_sem=recv_sem.at[i],
            device_id=at(*offset), device_id_type=MESH,
        )
        copies.append(copy)
        copy.start()
        return copy

    loaded("ocean", "proj", "mask", "overlay", "owner", "block", "count")
    for half in range(2):
        x.proj8[4 * half : 4 * half + 4] = x.proj[...]
    surface_message(x.owner, x.block, x.count, x.ocean, x.mask, x.overlay, x.proj8, x.msg)
    loaded("tok")
    x.side[...] = pack(x.tok[:, 0:8, :].astype(F32), False).reshape(64, 512).astype(BF16)

    wait_barrier()
    messages = [send(x.msg, x.msgs.at[dj + 1], (0, -dj)) for dj in (2, 1, -1)]
    x.msgs[1] = x.msg[...]
    east_end = send(x.side.at[pl.ds(48, 16)], x.east.at[pl.ds(48, 16)], (0, -1))
    east = send(x.side.at[pl.ds(0, 48)], x.east.at[pl.ds(0, 48)], (0, -1))
    upper = send(x.tok.at[pl.ds(12, 4)], x.upper, (1, 0))
    above = send(x.ocean.at[pl.ds(13, 3)], x.above, (1, 0))
    below = send(x.ocean.at[pl.ds(0, 3)], x.below, (-1, 0))

    loaded("grid", "enc", "gain")
    for half in range(2):
        x.enc8[4 * half : 4 * half + 4] = x.enc[...]
    bias_table(x.grid, x.table, x.rows, x.bias)
    edge = la == 0
    a_row = (iota((64, 512), 1) % 64) >= 32
    b_row = iota((64, 512), 0) >= 32
    x.last[...] = jnp.where(edge, jnp.where(a_row != b_row, -1e9, 0.0), 0.0)

    loaded("scale")
    ocean_rate(x)
    spread(x)
    for copy in messages:
        copy.wait_recv()
    sst = gather_surface(x.msgs)
    x.sst[...] = sst[2]
    over = send(x.sst, x.over, (1, 0))
    east_end.wait_recv()
    corner = send(x.east.at[pl.ds(48, 16)], x.corner, (1, 0))
    x.mixed[...] = add_surface(jnp.concatenate(sst, axis=1), x.enc8).reshape(16, 24, 512)
    gain = x.gain[...].reshape(1, 1, 512)
    east.wait_recv()
    for g in (1, 2):
        normalise(g, x.tok[4 * g : 4 * g + 4], x.east[16 * g : 16 * g + 16], gain, x.mixed, x.norm)
    loaded("wqkv", "bqkv", "wo")
    windows = (x.norm, x.wqkv, x.bqkv, x.wo, x.bias, x.last, x.q, x.k, x.v, x.att)
    attend(0, *windows)
    for g in (1, 2):
        finish(g, x.norm, x.mixed, x.cyc, x.pe.at[pl.ds(16 * g, 16)])

    def put(rows, cols, values):
        for h in range(2):
            x.pad[h, rows, cols, :] = values[:, :, 128 * h : 128 * h + 128]

    below.wait_recv()
    above.wait_recv()
    put(slice(3, 19), slice(8, 40), x.ocean[...].astype(F32))
    put(slice(0, 3), slice(8, 40), x.above[...].astype(F32) * (la > 0).astype(F32))
    put(slice(19, 22), slice(8, 40), x.below[...].astype(F32) * (la < nla - 1).astype(F32))
    for h in range(2):
        lanes = slice(128 * h, 128 * h + 128)
        x.leave[0, :, lanes] = pack(x.pad[h, :, 32:40, :], True).reshape(88, 128).astype(BF16)
        x.leave[1, :, lanes] = pack(x.pad[h, :, 8:16, :], False).reshape(88, 128).astype(BF16)
    sides = [send(x.leave.at[0], x.cols.at[0], (0, 1)), send(x.leave.at[1], x.cols.at[1], (0, -1))]
    pieces = [send(x.pe.at[pl.ds(16, 32)], x.west.at[pl.ds(16, 32)], (0, 1))]
    normalise(0, x.tok[0:4], x.east[0:16], gain, x.mixed, x.norm)

    for copy in (over, upper, corner):
        copy.wait_recv()
    x.mixed[12:16] = add_surface(x.over[...], x.enc8)[32:128].reshape(4, 24, 512)
    normalise(3, x.upper[...], x.corner[...], gain, x.mixed, x.norm)
    attend(1, *windows)
    for g in (3, 0):
        finish(g, x.norm, x.mixed, x.cyc, x.pe.at[pl.ds(16 * g, 16)])
    loaded("fp")
    flux = dot(x.fp[...], x.mixed[...].reshape(384, 512).astype(BF16), NT).astype(BF16)
    x.flux[...] = flux
    x.top[...] = flux[:, 256:384]
    edge = dot(x.fp[...], x.pe[...], NT)
    x.rim[...] = jnp.concatenate([edge, jnp.zeros((16, 64), F32)], axis=1).astype(BF16)
    fluxes = [
        send(x.top, x.tops.at[0], (-1, 1)),
        send(x.rim, x.edge.at[1], (-1, 2)),
        send(x.rim, x.edge.at[0], (0, 2)),
        send(x.top, x.tops.at[2], (-1, -1)),
        send(x.top, x.tops.at[1], (-1, 0)),
        send(x.flux, x.near.at[1], (0, -1)),
        send(x.flux, x.near.at[0], (0, 1)),
    ]
    pieces += [
        send(x.pe.at[pl.ds(0, 16)], x.west.at[pl.ds(0, 16)], (0, 1)),
        send(x.pe.at[pl.ds(48, 16)], x.sw, (-1, 1)),
        send(x.cyc.at[pl.ds(12, 4)], x.south, (-1, 0)),
    ]

    for copy in sides:
        copy.wait_recv()
    for side, high in ((0, True), (1, False)):
        values = unpack(x.cols[side].astype(F32).reshape(11, 8, 256), high)
        put(slice(0, 22), slice(40 * side, 40 * side + 8), values)
    loaded("kernel", "cbias")
    convolve(x.pad, x.kernel, x.cbias, x.conv)

    loaded("fenc", "ogain", "w1", "w2")
    for copy in fluxes:
        copy.wait_recv()
    ocean_update(x)
    for copy in pieces:
        copy.wait_recv()
    for copy in copies:
        copy.wait_send()


def last_kernel(cyc_ref, west_ref, south_ref, sw_ref, out_ref, atm_to, out_to, atm_s, store_sem):
    stores = [pltpu.make_async_copy(out_ref, out_to, store_sem.at[0])]
    stores[0].start()
    x = types.SimpleNamespace(cyc=cyc_ref, west=west_ref, south=south_ref, sw=sw_ref, atm=atm_s)
    for g in range(4):
        assemble(g, x)
        rows = pl.ds(4 * g, 4)
        stores.append(pltpu.make_async_copy(atm_s.at[rows], atm_to.at[rows], store_sem.at[g + 1]))
        stores[-1].start()
    for copy in stores:
        copy.wait()


def last(*results):
    shapes = [((16, 24, 512), BF16), ((16, 32, 256), BF16)]
    return pl.pallas_call(
        last_kernel,
        out_shape=[jax.ShapeDtypeStruct(*s) for s in shapes],
        in_specs=vmem(len(results)),
        out_specs=anywhere(len(shapes)),
        scratch_shapes=[pltpu.VMEM((16, 24, 512), BF16), pltpu.SemaphoreType.DMA((5,))],
        compiler_params=pltpu.CompilerParams(vmem_limit_bytes=24 << 20),
        name="last",
    )(*results)


def step(*operands):
    def copy_of(name, shape, kind):
        return pltpu.SMEM(shape, kind) if name in SCALARS else pltpu.VMEM(shape, kind)

    return pl.pallas_call(
        step_kernel,
        out_shape=[pltpu.VMEM(shape, kind) for _, shape, kind in RESULTS],
        in_specs=[pl.BlockSpec(memory_space=pltpu.HBM)] * len(OPERANDS),
        out_specs=vmem(len(RESULTS)),
        scratch_shapes=[
            *[copy_of(*o) for o in (*OPERANDS, *SCRATCH)],
            pltpu.SemaphoreType.DMA((len(OPERANDS),)), pltpu.SemaphoreType.DMA((COPIES,)), pltpu.SemaphoreType.DMA((COPIES,)),
        ],
        compiler_params=pltpu.CompilerParams(collective_id=0, has_side_effects=True),
        name="step",
    )(*operands)


def local(
    atmos_patch_tokens,
    atmos_norm_gain,
    query_key_value_weight,
    query_key_value_bias,
    relative_bias_grid,
    attention_output_weight,
    flux_projector,
    surface_encoder,
    ocean_cell_state,
    land_sea_mask,
    depthwise_conv_kernel,
    depthwise_conv_bias,
    ocean_norm_gain,
    pointwise_expand,
    pointwise_contract,
    layer_update_scale,
    forcing_encoder,
    surface_projector,
    overlay_area_weight,
    owners,
    owner_tile_blocks,
    counts,
):
    owners = owners.reshape(1, 3)
    blocks = owner_tile_blocks.reshape(1, 3)
    overlay = overlay_area_weight.reshape(3, 64, 512)
    results = step(
        ocean_cell_state, surface_projector.T, land_sea_mask, overlay, owners, blocks, counts, atmos_patch_tokens,
        relative_bias_grid, surface_encoder, atmos_norm_gain.reshape(1, 512), query_key_value_weight, query_key_value_bias,
        attention_output_weight, flux_projector.T, depthwise_conv_kernel, depthwise_conv_bias.reshape(1, 256), forcing_encoder,
        ocean_norm_gain.reshape(1, 256), pointwise_expand, pointwise_contract, layer_update_scale.reshape(1, 256),
    )
    return last(*results)


def solution(mesh):
    rep = P()
    placed = (
        P("lat", "lon", None), rep, rep, rep, rep, rep, rep, rep, P("lat", "lon", None), P("lat", "lon"),
        rep, rep, rep, rep, rep, rep, rep, rep, P("lat", "lon", None, None, None),
        P("lat", "lon", None), P("lat", "lon", None), P("lat", "lon"),
    )
    return jax.shard_map(
        local,
        mesh=mesh,
        in_specs=placed,
        out_specs=(P("lat", "lon", None), P("lat", "lon", None)),
        check_vma=False,
    )
```

```python
import types

import jax
import jax.numpy as jnp
from jax import lax
from jax.experimental import pallas as pl
from jax.experimental.pallas import tpu as pltpu
from jax.sharding import PartitionSpec as P

F32 = jnp.float32
BF16 = jnp.bfloat16
MESH = pl.DeviceIdType.MESH
HEADS = 16
HALF = 8
WIN = 8
NT = (((1,), (1,)), ((), ()))
TN = (((0,), (0,)), ((), ()))
NN = (((1,), (0,)), ((), ()))


def dot(a, b, dims):
    return lax.dot_general(a, b, dims, preferred_element_type=F32)


def iota(shape, dim):
    return lax.broadcasted_iota(jnp.int32, shape, dim)


def low_half(shape):
    return iota(shape, len(shape) - 2) % 8 < 4


def turn(x):
    return pltpu.roll(x, 4, x.ndim - 2)


def pack(x, high):
    n, _, lanes = x.shape
    x = x.reshape(n // 2, 2, 8, lanes)
    even, odd = x[:, 0], x[:, 1]
    if high:
        even = turn(even)
    else:
        odd = turn(odd)
    return jnp.where(low_half(even.shape), even, odd)


def unpack(x, high):
    n, _, lanes = x.shape
    other = turn(x)
    pair = (other, x) if high else (x, other)
    return jnp.stack(pair, axis=1).reshape(2 * n, 8, lanes)


def split2(x):
    top = x.astype(BF16).astype(F32)
    return top, x - top


def split3(x):
    top, rest = split2(x)
    middle, last = split2(rest)
    return top, middle, last


def greet(partners):
    barrier = pltpu.get_barrier_semaphore()
    for device in partners:
        pl.semaphore_signal(barrier, inc=1, device_id=device, device_id_type=MESH)
    return lambda: pl.semaphore_wait(barrier, len(partners))


def place():
    la, lo = lax.axis_index("lat"), lax.axis_index("lon")
    nla, nlo = lax.axis_size("lat"), lax.axis_size("lon")
    return lambda di, dj: (lax.rem(la + di + nla, nla), lax.rem(lo + dj + nlo, nlo))


def vmem(n):
    return [pl.BlockSpec(memory_space=pltpu.VMEM)] * n


def smem(n):
    return [pl.BlockSpec(memory_space=pltpu.SMEM)] * n


def anywhere(n):
    return [pl.BlockSpec(memory_space=pl.ANY)] * n


def layer_norm(x, gain, epsilon):
    average = jnp.mean(x, axis=-1, keepdims=True)
    centred = x - average
    spread = jnp.mean(centred * centred, axis=-1, keepdims=True)
    return centred * lax.rsqrt(spread + epsilon) * gain


def column_of(patch):
    p = patch.astype(F32)
    return p - 24.0 * jnp.floor((p + 0.5) * (1.0 / 24.0))


def mask_row(mask):
    wide = jnp.concatenate([mask.astype(F32), jnp.zeros((16, 96), F32)], axis=1)
    moved = [wide if q == 0 else pltpu.roll(wide, 32 * q, 1) for q in range(4)]
    parts = [sum(moved[q][4 * j + q : 4 * j + q + 1] for q in range(4)) for j in range(4)]
    return jnp.concatenate(parts, axis=1)


PARTNERS = [(0, 1), (0, -1), (0, 2), (0, -2), (1, 0), (-1, 0)]
COPIES = 32


def surface_message(owner_ref, block_ref, count_ref, ocean_ref, mask_ref, overlay_ref, proj_s, msg_s):
    lo = lax.axis_index("lon")
    nlo = lax.axis_size("lon")
    parts = jnp.concatenate(split3(proj_s[...]), axis=0).astype(BF16)
    surf = dot(parts, ocean_ref[...].reshape(512, 256), NT)
    surf = ((surf[0:8] + surf[8:16] + surf[16:24]) * mask_row(mask_ref[...])).astype(BF16)
    row = iota((8, 128), 0)
    twice = []
    codes = jnp.full((8, 128), -1.0, F32)
    for k in range(3):
        block = overlay_ref[k]
        twice.append(dot(surf, jnp.concatenate([block, block], axis=0), NT))
        side = lax.rem(owner_ref[0, k] - lo + 1 + nlo, nlo)
        code = jnp.where(k < count_ref[0, 0], side * 8 + block_ref[0, k], -1).astype(F32)
        codes = jnp.where(row == 4 + k, code, codes)
    msg_s[0:8] = jnp.where(row < 4, twice[0], twice[1])
    msg_s[8:16] = jnp.where(row < 4, twice[2], codes)


def gather_surface(msgs_ref):
    upper = iota((8, 128), 0) < 4
    right = iota((8, 128), 1) >= 64
    tiles = []
    for tile in range(2):
        sums = [jnp.zeros((8, 128), F32)] * 3
        for side in range(3):
            slot = tile - side + 2
            a = msgs_ref[slot, 0:8, :]
            b = msgs_ref[slot, 8:16, :]
            code_a = jnp.where(upper, b[4:5], b[5:6])
            code_b = jnp.where(upper, b[6:7], -1.0)
            for j in range(3):
                target = jnp.where(right, side * 8.0 + 2 * j + 1, side * 8.0 + 2 * j)
                sums[j] += jnp.where(code_a == target, a, 0.0) + jnp.where(code_b == target, b, 0.0)
        tiles.append(sums)
    return [
        jnp.where(column_of(iota((8, 128), 1) + 128 * j) < 4, tiles[1][j], tiles[0][j]) for j in range(3)
    ]


def bias_table(grid_ref, table_s, rows_s, bias_s):
    grid = jnp.concatenate([grid_ref[...], jnp.zeros((16, 31), F32)], axis=1)
    for ra in range(8):
        rolled = grid if ra == 0 else pltpu.roll(grid, 256 - 15 * ra, 1)
        table_s[:, ra, :] = rolled[:, 0:128]
    parts = [x.astype(BF16) for x in split3(table_s[...].reshape(128, 128))]
    entry = iota((128, 64), 0)
    lane = iota((128, 64), 1)
    for ca in range(8):
        chosen = (entry == (7 - lane // 8) * 15 + ca - lane % 8 + 7).astype(BF16)
        found = (dot(parts[0], chosen, NN) + dot(parts[1], chosen, NN)) + dot(parts[2], chosen, NN)
        rows_s[:, ca, :] = found
    for part in range(8):
        rows = rows_s[16 * part : 16 * part + 16].reshape(128, 64)
        bias_s[:, 128 * part : 128 * part + 128] = rows.T


def add_surface(sst, enc_s):
    s_hi, s_lo = split2(sst)
    e_hi, e_lo = split2(enc_s[...])
    left = jnp.concatenate([s_hi, s_lo, s_hi], axis=0).astype(BF16)
    right = jnp.concatenate([e_hi, e_hi, e_lo], axis=0).astype(BF16)
    return dot(left, right, TN)


def normalise(g, tokens, side, gain, mixed_s, norm_s):
    low = low_half((4, 8, 512))
    rows = slice(4 * g, 4 * g + 4)
    tokens = tokens.astype(F32)
    side = unpack(side.astype(F32).reshape(2, 8, 512), False)
    head = jnp.where(low, side, tokens[:, 0:8])
    tokens = jnp.concatenate([head, tokens[:, 8:24]], axis=1)
    mixed = (tokens + mixed_s[rows]).astype(BF16).astype(F32)
    mixed_s[rows] = mixed
    normed = layer_norm(mixed, gain, 1e-05)
    turned = [turn(normed[:, 8 * b : 8 * b + 8]) for b in range(3)]
    w_row, w_start = WINDOW_OF[g]
    for b in range(3):
        norm_s[w_row * 3 + b, w_start : w_start + 4] = jnp.where(low, turned[b], turned[(b + 1) % 3])


WINDOW_OF = ((1, 4), (0, 0), (0, 4), (1, 0))


def attend(w_row, norm_s, wqkv_s, bqkv_ref, wo_s, bias_s, last_s, q_s, k_s, v_s, att_s):
    rows = norm_s[3 * w_row : 3 * w_row + 3].reshape(192, 512).astype(BF16)
    for part, ref in enumerate((q_s, k_s, v_s)):
        cols = slice(512 * part, 512 * part + 512)
        value = dot(rows, wqkv_s[:, cols], NN) + bqkv_ref[cols].reshape(1, 512)
        if part == 0:
            value = value * 32 ** (-0.5)
        ref[...] = value.astype(BF16)
    own = (iota((8, 1, 256), 2) // 32) == iota((8, 1, 256), 0)
    first_head = iota((64, 128), 0) < 32
    for w in range(3):
        at = slice(64 * w, 64 * w + 64)
        for g in range(2):
            lanes = slice(256 * g, 256 * g + 256)
            queries = jnp.where(own, q_s[at, lanes][None], jnp.zeros((), BF16)).reshape(512, 256)
            scores = dot(k_s[at, lanes], queries, NT) + bias_s[:, 512 * g : 512 * g + 512]
            if w_row == 1:
                scores = scores + last_s[...]
            scores = jnp.exp(scores - jnp.max(scores, axis=0, keepdims=True))
            weights = (scores * (1.0 / jnp.sum(scores, axis=0, keepdims=True))).astype(BF16)
            values = v_s[at, lanes].astype(F32).T.astype(BF16)
            found = []
            for pair in range(4):
                both = dot(values[64 * pair : 64 * pair + 64], weights[:, 128 * pair : 128 * pair + 128], NN)
                found.append(jnp.where(first_head, both, pltpu.roll(both, 64, 1)))
            att_s[at, lanes] = jnp.concatenate(found, axis=0).T[0:64].astype(BF16)
    projected = dot(att_s[...], wo_s[...], NN).astype(BF16).astype(F32)
    norm_s[3 * w_row : 3 * w_row + 3] = projected.reshape(3, 8, 8, 512)


def finish(g, norm_s, mixed_s, cyc_ref, side_ref):
    w_row, w_start = WINDOW_OF[g]
    turned = [turn(norm_s[w_row * 3 + b, w_start : w_start + 4]) for b in range(3)]
    low = low_half((4, 8, 512))
    back = jnp.concatenate([jnp.where(low, turned[b - 1], turned[b]) for b in range(3)], axis=1)
    rows = slice(4 * g, 4 * g + 4)
    result = (mixed_s[rows] + back).astype(BF16)
    mixed_s[rows] = result.astype(F32)
    cyc_ref[rows] = result
    side_ref[...] = pack(result.astype(F32)[:, 0:8], False).reshape(16, 512).astype(BF16)


def convolve(pad_s, kernel_ref, cbias_ref, conv_ref):
    def band(i, carry):
        start = i * 8
        for h in range(2):
            lanes = slice(128 * h, 128 * h + 128)
            first_term = jnp.broadcast_to(cbias_ref[:, lanes], (8, 128))
            for b in range(4):
                sums = [first_term] * 8
                for v in range(7):
                    col = 8 * b + v + 5
                    cells = [pad_s[h, start + r, col : col + 8, :] for r in range(14)]
                    for u in range(7):
                        tap = kernel_ref[u, v : v + 1, lanes]
                        for r in range(8):
                            sums[r] = sums[r] + tap * cells[r + u]
                for r in range(8):
                    conv_ref[start + r, 8 * b : 8 * b + 8, lanes] = sums[r]
        return carry

    lax.fori_loop(0, 2, band, 0)


OPERANDS = (
    ("ocean", (16, 32, 256), BF16), ("proj", (4, 256), F32), ("mask", (16, 32), jnp.int32), ("overlay", (3, 64, 512), BF16),
    ("owner", (1, 3), jnp.int32), ("block", (1, 3), jnp.int32), ("count", (1, 1), jnp.int32), ("tok", (16, 24, 512), BF16),
    ("grid", (16, 225), F32), ("enc", (4, 512), F32), ("gain", (1, 512), F32), ("wqkv", (512, 1536), BF16),
    ("bqkv", (1536,), F32), ("wo", (512, 512), BF16), ("fp", (16, 512), BF16), ("kernel", (7, 7, 256), F32),
    ("cbias", (1, 256), F32), ("fenc", (16, 256), F32), ("ogain", (1, 256), F32), ("w1", (256, 1024), BF16),
    ("w2", (1024, 256), BF16), ("scale", (1, 256), F32),
)
SCALARS = ("owner", "block", "count")
SCRATCH = (
    ("proj8", (8, 256), F32), ("enc8", (8, 512), F32), ("msg", (16, 128), F32), ("msgs", (4, 16, 128), F32),
    ("side", (64, 512), BF16), ("east", (64, 512), BF16), ("upper", (4, 24, 512), BF16), ("corner", (16, 512), BF16),
    ("sst", (8, 128), F32), ("over", (8, 128), F32), ("table", (16, 8, 128), F32), ("rows", (128, 8, 64), F32),
    ("bias", (64, 1024), F32), ("last", (64, 512), F32), ("mixed", (16, 24, 512), F32), ("norm", (6, 8, 8, 512), F32), ("q", (192, 512), BF16),
    ("k", (192, 512), BF16), ("v", (192, 512), BF16), ("att", (192, 512), BF16), ("above", (3, 32, 256), BF16),
    ("below", (3, 32, 256), BF16), ("leave", (2, 88, 256), BF16), ("cols", (2, 88, 256), BF16),
    ("pad", (2, 22, 48, 128), F32), ("pe", (64, 512), BF16), ("flux", (16, 384), BF16),
    ("near", (2, 16, 384), BF16), ("top", (16, 128), BF16), ("rim", (16, 128), BF16),
    ("tops", (3, 16, 128), BF16), ("edge", (2, 16, 128), BF16), ("spread", (64, 384), BF16), ("conv", (16, 32, 256), F32), ("pre", (512, 256), F32), ("rate", (512, 256), F32),
)
RESULTS = (
    ("cyc", (16, 24, 512), BF16), ("west", (64, 512), BF16), ("south", (4, 24, 512), BF16), ("sw", (16, 512), BF16),
    ("out", (16, 32, 256), BF16),
)


def spread(x):
    patch = iota((64, 384), 0)
    x.spread[...] = (iota((64, 384), 1) == 24 * (patch // 4) + patch % 4).astype(BF16)


def pick_flux(x, codes):
    lane = iota((16, 128), 1)
    right = lane >= 64
    edge = dot(x.edge[...].reshape(32, 128)[:, 0:64], x.spread[...], NN)
    west, own, east = x.near[0].astype(F32), x.flux[...].astype(F32), x.near[1].astype(F32)
    heads, bodies = (edge[0:16], west, own), (west, own, east)
    tops = [x.tops[n].astype(F32) for n in range(3)]
    top_heads = (edge[16:32, 256:384], tops[0], tops[1])
    picked = [jnp.zeros((16, 128), F32)] * 3
    for j in range(3):
        patch = lane + 128 * j
        head = column_of(patch) < 4
        at = slice(128 * j, 128 * j + 128)
        for side in range(3):
            tile = jnp.where(head, heads[side][:, at], bodies[side][:, at])
            if j == 2:
                tile = jnp.where(patch >= 288, jnp.where(head, top_heads[side], tops[side]), tile)
            target = jnp.where(right, side * 8 + 2 * j + 1, side * 8 + 2 * j)
            for k in range(3):
                picked[k] += jnp.where(target == codes[k], tile, 0.0)
    picked = [y + pltpu.roll(y, 64, 1) for y in picked]
    return jnp.concatenate([jnp.where(right, picked[1], picked[0]), picked[2][:, 0:64]], axis=1)


def slot_codes(x):
    lo = lax.axis_index("lon")
    nlo = lax.axis_size("lon")
    codes = []
    for k in range(3):
        side = lax.rem(x.owner[0, k] - lo + 1 + nlo, nlo)
        codes.append(jnp.where(k < x.count[0, 0], side * 8 + x.block[0, k], -1))
    return codes


def ocean_rate(x):
    mask = jnp.broadcast_to(mask_row(x.mask[...]), (16, 512)).astype(BF16)
    parts = [jnp.broadcast_to(y, (16, 256)) for y in split3(x.scale[...])]
    row = iota((16, 256), 0)
    scale = jnp.where(row == 0, parts[0], jnp.where(row == 1, parts[1], jnp.where(row == 2, parts[2], 0.0)))
    x.rate[...] = dot(mask, scale.astype(BF16), TN)


def ocean_update(x):
    forcing = dot(pick_flux(x, slot_codes(x)).astype(BF16), x.overlay[...].reshape(192, 512), NN)
    f_hi, f_lo = split2(forcing)
    e_hi, e_lo = split2(x.fenc[...])
    x.pre[...] = x.conv[...].reshape(512, 256) + dot(
        jnp.concatenate([f_hi, f_lo, f_hi], axis=0).astype(BF16),
        jnp.concatenate([e_hi, e_hi, e_lo], axis=0).astype(BF16),
        TN,
    )

    for i in range(4):
        at = slice(128 * i, 128 * i + 128)
        normed = layer_norm(x.pre[at], x.ogain[...], 1e-06).astype(BF16)
        update = jnp.zeros((128, 256), F32)
        for c in range(4):
            cols = slice(256 * c, 256 * c + 256)
            y = dot(normed, x.w1[:, cols], NN)
            hidden = (0.5 * y * (1.0 + lax.erf(y * (0.5**0.5)))).astype(BF16)
            update = update + dot(hidden, x.w2[cols], NN)
        rows = slice(4 * i, 4 * i + 4)
        state = x.ocean[rows].astype(F32).reshape(128, 256)
        x.out[rows] = (state + x.rate[at] * update).astype(BF16).reshape(4, 32, 256)


def assemble(g, x):
    low = low_half((4, 8, 512))
    rows = slice(4 * g, 4 * g + 4)
    body, side = (x.south, x.sw[...]) if g == 3 else (x.cyc.at[rows], x.west[16 * g : 16 * g + 16])
    body = body[...].astype(F32)
    side = unpack(side.astype(F32).reshape(2, 8, 512), False)
    head = jnp.where(low, side, body[:, 0:8])
    x.atm[rows] = jnp.concatenate([head, body[:, 8:24]], axis=1).astype(BF16)


def step_kernel(*refs):
    n = len(OPERANDS)
    given = dict(zip([o[0] for o in OPERANDS], refs[:n]))
    names = [o[0] for o in (*RESULTS, *OPERANDS, *SCRATCH)]
    x = types.SimpleNamespace(**dict(zip(names, refs[n:])))
    load_sem, send_sem, recv_sem = refs[n + len(names) :]

    at = place()
    la = lax.axis_index("lat")
    nla = lax.axis_size("lat")
    wait_barrier = greet([at(*o) for o in PARTNERS])
    loads = {}
    for i, (name, *_) in enumerate(OPERANDS):
        loads[name] = pltpu.make_async_copy(given[name], getattr(x, name), load_sem.at[i])
        loads[name].start()

    def loaded(*names):
        for name in names:
            loads[name].wait()

    copies = []

    def send(src, dst, offset):
        i = len(copies)
        copy = pltpu.make_async_remote_copy(
            src_ref=src, dst_ref=dst, send_sem=send_sem.at[i], recv_sem=recv_sem.at[i],
            device_id=at(*offset), device_id_type=MESH,
        )
        copies.append(copy)
        copy.start()
        return copy

    loaded("ocean", "proj", "mask", "overlay", "owner", "block", "count")
    for half in range(2):
        x.proj8[4 * half : 4 * half + 4] = x.proj[...]
    surface_message(x.owner, x.block, x.count, x.ocean, x.mask, x.overlay, x.proj8, x.msg)
    loaded("tok")
    x.side[...] = pack(x.tok[:, 0:8, :].astype(F32), False).reshape(64, 512).astype(BF16)

    wait_barrier()
    messages = [send(x.msg, x.msgs.at[dj + 1], (0, -dj)) for dj in (2, 1, -1)]
    x.msgs[1] = x.msg[...]
    east_end = send(x.side.at[pl.ds(48, 16)], x.east.at[pl.ds(48, 16)], (0, -1))
    east = send(x.side.at[pl.ds(0, 48)], x.east.at[pl.ds(0, 48)], (0, -1))
    upper = send(x.tok.at[pl.ds(12, 4)], x.upper, (1, 0))
    above = send(x.ocean.at[pl.ds(13, 3)], x.above, (1, 0))
    below = send(x.ocean.at[pl.ds(0, 3)], x.below, (-1, 0))

    loaded("grid", "enc", "gain")
    for half in range(2):
        x.enc8[4 * half : 4 * half + 4] = x.enc[...]
    bias_table(x.grid, x.table, x.rows, x.bias)
    edge = la == 0
    a_row = (iota((64, 512), 1) % 64) >= 32
    b_row = iota((64, 512), 0) >= 32
    x.last[...] = jnp.where(edge, jnp.where(a_row != b_row, -1e9, 0.0), 0.0)

    loaded("scale")
    ocean_rate(x)
    spread(x)
    for copy in messages:
        copy.wait_recv()
    sst = gather_surface(x.msgs)
    x.sst[...] = sst[2]
    over = send(x.sst, x.over, (1, 0))
    east_end.wait_recv()
    corner = send(x.east.at[pl.ds(48, 16)], x.corner, (1, 0))
    def put(rows, cols, values):
        for h in range(2):
            x.pad[h, rows, cols, :] = values[:, :, 128 * h : 128 * h + 128]

    below.wait_recv()
    above.wait_recv()
    put(slice(3, 19), slice(8, 40), x.ocean[...].astype(F32))
    put(slice(0, 3), slice(8, 40), x.above[...].astype(F32) * (la > 0).astype(F32))
    put(slice(19, 22), slice(8, 40), x.below[...].astype(F32) * (la < nla - 1).astype(F32))
    for h in range(2):
        lanes = slice(128 * h, 128 * h + 128)
        x.leave[0, :, lanes] = pack(x.pad[h, :, 32:40, :], True).reshape(88, 128).astype(BF16)
        x.leave[1, :, lanes] = pack(x.pad[h, :, 8:16, :], False).reshape(88, 128).astype(BF16)
    sides = [send(x.leave.at[0], x.cols.at[0], (0, 1)), send(x.leave.at[1], x.cols.at[1], (0, -1))]
    x.mixed[...] = add_surface(jnp.concatenate(sst, axis=1), x.enc8).reshape(16, 24, 512)
    gain = x.gain[...].reshape(1, 1, 512)
    east.wait_recv()
    for g in (1, 2):
        normalise(g, x.tok[4 * g : 4 * g + 4], x.east[16 * g : 16 * g + 16], gain, x.mixed, x.norm)
    loaded("wqkv", "bqkv", "wo")
    windows = (x.norm, x.wqkv, x.bqkv, x.wo, x.bias, x.last, x.q, x.k, x.v, x.att)
    attend(0, *windows)
    for g in (1, 2):
        finish(g, x.norm, x.mixed, x.cyc, x.pe.at[pl.ds(16 * g, 16)])

    pieces = [send(x.pe.at[pl.ds(16, 32)], x.west.at[pl.ds(16, 32)], (0, 1))]
    normalise(0, x.tok[0:4], x.east[0:16], gain, x.mixed, x.norm)

    for copy in (over, upper, corner):
        copy.wait_recv()
    x.mixed[12:16] = add_surface(x.over[...], x.enc8)[32:128].reshape(4, 24, 512)
    normalise(3, x.upper[...], x.corner[...], gain, x.mixed, x.norm)
    attend(1, *windows)
    for g in (3, 0):
        finish(g, x.norm, x.mixed, x.cyc, x.pe.at[pl.ds(16 * g, 16)])
    loaded("fp")
    flux = dot(x.fp[...], x.mixed[...].reshape(384, 512).astype(BF16), NT).astype(BF16)
    x.flux[...] = flux
    x.top[...] = flux[:, 256:384]
    edge = dot(x.fp[...], x.pe[...], NT)
    x.rim[...] = jnp.concatenate([edge, jnp.zeros((16, 64), F32)], axis=1).astype(BF16)
    fluxes = [
        send(x.top, x.tops.at[0], (-1, 1)),
        send(x.rim, x.edge.at[1], (-1, 2)),
        send(x.rim, x.edge.at[0], (0, 2)),
        send(x.top, x.tops.at[2], (-1, -1)),
        send(x.top, x.tops.at[1], (-1, 0)),
        send(x.flux, x.near.at[1], (0, -1)),
        send(x.flux, x.near.at[0], (0, 1)),
    ]
    pieces += [
        send(x.pe.at[pl.ds(0, 16)], x.west.at[pl.ds(0, 16)], (0, 1)),
        send(x.pe.at[pl.ds(48, 16)], x.sw, (-1, 1)),
        send(x.cyc.at[pl.ds(12, 4)], x.south, (-1, 0)),
    ]

    for copy in sides:
        copy.wait_recv()
    for side, high in ((0, True), (1, False)):
        values = unpack(x.cols[side].astype(F32).reshape(11, 8, 256), high)
        put(slice(0, 22), slice(40 * side, 40 * side + 8), values)
    loaded("kernel", "cbias")
    convolve(x.pad, x.kernel, x.cbias, x.conv)

    loaded("fenc", "ogain", "w1", "w2")
    for copy in fluxes:
        copy.wait_recv()
    ocean_update(x)
    for copy in pieces:
        copy.wait_recv()
    for copy in copies:
        copy.wait_send()


def last_kernel(cyc_ref, west_ref, south_ref, sw_ref, out_ref, atm_to, out_to, atm_s, store_sem):
    stores = [pltpu.make_async_copy(out_ref, out_to, store_sem.at[0])]
    stores[0].start()
    x = types.SimpleNamespace(cyc=cyc_ref, west=west_ref, south=south_ref, sw=sw_ref, atm=atm_s)
    for g in range(4):
        assemble(g, x)
        rows = pl.ds(4 * g, 4)
        stores.append(pltpu.make_async_copy(atm_s.at[rows], atm_to.at[rows], store_sem.at[g + 1]))
        stores[-1].start()
    for copy in stores:
        copy.wait()


def last(*results):
    shapes = [((16, 24, 512), BF16), ((16, 32, 256), BF16)]
    return pl.pallas_call(
        last_kernel,
        out_shape=[jax.ShapeDtypeStruct(*s) for s in shapes],
        in_specs=vmem(len(results)),
        out_specs=anywhere(len(shapes)),
        scratch_shapes=[pltpu.VMEM((16, 24, 512), BF16), pltpu.SemaphoreType.DMA((5,))],
        compiler_params=pltpu.CompilerParams(vmem_limit_bytes=24 << 20),
        name="last",
    )(*results)


def step(*operands):
    def copy_of(name, shape, kind):
        return pltpu.SMEM(shape, kind) if name in SCALARS else pltpu.VMEM(shape, kind)

    return pl.pallas_call(
        step_kernel,
        out_shape=[pltpu.VMEM(shape, kind) for _, shape, kind in RESULTS],
        in_specs=[pl.BlockSpec(memory_space=pltpu.HBM)] * len(OPERANDS),
        out_specs=vmem(len(RESULTS)),
        scratch_shapes=[
            *[copy_of(*o) for o in (*OPERANDS, *SCRATCH)],
            pltpu.SemaphoreType.DMA((len(OPERANDS),)), pltpu.SemaphoreType.DMA((COPIES,)), pltpu.SemaphoreType.DMA((COPIES,)),
        ],
        compiler_params=pltpu.CompilerParams(collective_id=0, has_side_effects=True),
        name="step",
    )(*operands)


def local(
    atmos_patch_tokens,
    atmos_norm_gain,
    query_key_value_weight,
    query_key_value_bias,
    relative_bias_grid,
    attention_output_weight,
    flux_projector,
    surface_encoder,
    ocean_cell_state,
    land_sea_mask,
    depthwise_conv_kernel,
    depthwise_conv_bias,
    ocean_norm_gain,
    pointwise_expand,
    pointwise_contract,
    layer_update_scale,
    forcing_encoder,
    surface_projector,
    overlay_area_weight,
    owners,
    owner_tile_blocks,
    counts,
):
    owners = owners.reshape(1, 3)
    blocks = owner_tile_blocks.reshape(1, 3)
    overlay = overlay_area_weight.reshape(3, 64, 512)
    results = step(
        ocean_cell_state, surface_projector.T, land_sea_mask, overlay, owners, blocks, counts, atmos_patch_tokens,
        relative_bias_grid, surface_encoder, atmos_norm_gain.reshape(1, 512), query_key_value_weight, query_key_value_bias,
        attention_output_weight, flux_projector.T, depthwise_conv_kernel, depthwise_conv_bias.reshape(1, 256), forcing_encoder,
        ocean_norm_gain.reshape(1, 256), pointwise_expand, pointwise_contract, layer_update_scale.reshape(1, 256),
    )
    return last(*results)


def solution(mesh):
    rep = P()
    placed = (
        P("lat", "lon", None), rep, rep, rep, rep, rep, rep, rep, P("lat", "lon", None), P("lat", "lon"),
        rep, rep, rep, rep, rep, rep, rep, rep, P("lat", "lon", None, None, None),
        P("lat", "lon", None), P("lat", "lon", None), P("lat", "lon"),
    )
    return jax.shard_map(
        local,
        mesh=mesh,
        in_specs=placed,
        out_specs=(P("lat", "lon", None), P("lat", "lon", None)),
        check_vma=False,
    )
```
